256 devices in a mesh: row: 16 (over z, core), col: 16 (over x, y).
Axes of the slice: x: 4, y: 4, z: 8, core: 2. Of those that a mesh axis runs over, the one named last changes fastest.
Arguments:
- running_cost: float32 [4096, 8192], P('row', 'col'), may hold values from 0.5 to 7.5, as said below
- control_x: float32 [4096, 8192], P('row', 'col'), may hold values from -6 to 6
- control_y: float32 [4096, 8192], P('row', 'col'), may hold values from -6 to 6
- prior_density: float32 [4096, 8192], P('row', 'col'), may hold values from 0.5 to 2
Outputs:
- value_field: float32 [4096, 8192], P('row', 'col')
- density: float32 [4096, 8192], P('row', 'col')
- ergodic: float32 [], replicated
The draws below stay inside these ranges and needn't reach their ends.
Inputs may be any that keep to these rules, and one draw needn't show every extreme that they name: `running_cost`: strictly positive.
All inputs are finite; a program needn't handle non-finite values.
Results may differ from the reference program's by a relative error of at most 0.0003.
Values sent between devices are 32-bit elements; how exact they have to be, the bound alone decides.
A program may use at most 64 MiB of HBM per device.

```python
import jax
import jax.numpy as jnp

ITERS = 3
NX = 4096
NY = 8192


def draw_running_cost(key, part):
    rows = jnp.arange(NX, dtype=jnp.float32)
    ramp = 1.0 + 2.0 * rows / (NX - 1.0)
    rough = jax.random.uniform(key, (NX, NY), jnp.float32, 0.5, 1.5)
    return (ramp[:, None] * rough).astype(jnp.float32)


def shard_levels(key, shape, split, smallest, largest):
    gain, own = 1.0, jax.random.fold_in(key, 6)
    for position, blocks in split:
        draws = jnp.exp(jax.random.uniform(jax.random.fold_in(own, position), (blocks,), jnp.float32, smallest / len(split), largest / len(split)))
        gain = gain * jnp.repeat(draws, shape[position] // blocks).reshape([-1 if axis == position else 1 for axis in range(len(shape))])
    return gain


def scatter_about(stream_key, extent, spread, reach, cuts=(), held_as=jnp.bfloat16):
    entries = jax.random.normal(stream_key, extent, jnp.float32) * spread
    if len(cuts) > 0:
        entries = shard_levels(stream_key, extent, cuts, -0.22, 0.18) * entries
    return jnp.clip(entries, min=-reach, max=reach).astype(held_as)


def setup_inputs(seed: int = 0) -> dict:
    key_list = jax.random.split(jax.random.key(seed), 5)
    running_cost = draw_running_cost(jax.random.fold_in(key_list[4], 71), 0)
    control_x = scatter_about(key_list[1], (NX, NY), 1.0, 6.0, ((0, 16), (1, 16)), jnp.float32)
    control_y = scatter_about(key_list[2], (NX, NY), 1.0, 6.0, ((0, 16), (1, 16)), jnp.float32)
    prior_density = jnp.clip(0.5 + 1.5 * jax.random.uniform(key_list[3], (NX, NY), jnp.float32) ** shard_levels(key_list[3], (NX, NY), ((0, 16), (1, 16)), -0.2, 0.2), 0.5, 2.0)
    return dict(running_cost=running_cost, control_x=control_x, control_y=control_y, prior_density=prior_density)


discount_rate = 0.05
diffusion = 0.25


def interior(padded):
    return padded[1:-1, 1:-1]


def neighbours(padded):
    return (padded[2:, 1:-1], padded[:-2, 1:-1], padded[1:-1, 2:], padded[1:-1, :-2])


def coefficients(conduct, padded_conduct, zeroth):
    weights = tuple(diffusion * 0.5 * (conduct + outside) for outside in neighbours(padded_conduct))
    center = zeroth + ((weights[0] + weights[1]) + (weights[2] + weights[3]))
    return (center,) + weights


def operator_apply(padded, coeffs):
    beside = neighbours(padded)
    inflow = (coeffs[1] * beside[0] + coeffs[2] * beside[1]) + (coeffs[3] * beside[2] + coeffs[4] * beside[3])
    return coeffs[0] * interior(padded) - inflow


def conjugate(coeffs, forcing):
    solution = jnp.zeros_like(forcing)
    residual = forcing
    direction = forcing
    norm_now = jnp.sum(residual * residual)
    for iteration in range(ITERS):
        applied = operator_apply(jnp.pad(direction, 1), coeffs)
        step_size = norm_now / jnp.sum(direction * applied)
        solution = solution + step_size * direction
        residual = residual - step_size * applied
        norm_next = jnp.sum(residual * residual)
        direction = residual + (norm_next / norm_now) * direction
        norm_now = norm_next
    return solution


def reference(running_cost, control_x, control_y, prior_density):
    control_cost = 0.5 * (control_x * control_x + control_y * control_y)
    conduct = 1.0 + control_cost
    padded_conduct = jnp.pad(conduct, 1)
    bellman = coefficients(conduct, padded_conduct, discount_rate)
    value_field = conjugate(bellman, running_cost + control_cost)
    padded_value = jnp.pad(value_field, 1)
    beside = neighbours(padded_value)
    slope_row = 0.5 * (beside[0] - beside[1])
    slope_col = 0.5 * (beside[2] - beside[3])
    congestion = (slope_row * slope_row + slope_col * slope_col) / (2.0 * diffusion)
    planck = coefficients(conduct, padded_conduct, discount_rate + congestion)
    density = conjugate(planck, prior_density)
    weighted = jnp.sum(prior_density * (running_cost + control_cost - discount_rate * value_field))
    ergodic = weighted / jnp.sum(prior_density)
    return value_field, density, ergodic
```

```python
import functools

import jax
import jax.numpy as jnp
from jax import lax
from jax.experimental import pallas as pl
from jax.experimental.pallas import tpu as pltpu
from jax.sharding import PartitionSpec as P

MESH = pl.DeviceIdType.MESH

SCALE = 1.0 / 64.0
FACE = 0.25 * 0.5 * SCALE
DISCOUNT = 0.05

LANE = 128
TOP = 16
HALO = 8
STEP = 16


def solve(nu):
    shift = DISCOUNT * SCALE
    m = [nu[k + 1] + shift * nu[k] for k in range(5)]
    l1 = m[1] / m[0]
    l2 = m[2] / m[0]
    d1 = m[2] - l1 * m[1]
    e = m[3] - l2 * m[1]
    l3 = e / d1
    d2 = (m[4] - l2 * m[2]) - l3 * e
    y0 = nu[0]
    y1 = nu[1] - l1 * y0
    y2 = (nu[2] - l2 * y0) - l3 * y1
    c2 = y2 / d2
    c1 = y1 / d1 - l3 * c2
    c0 = y0 / m[0] - l1 * c1 - l2 * c2
    return c0 * SCALE, c1 * SCALE, c2 * SCALE


def kernel(
    nrow, ncol, rows, tiles,
    rc_hbm, cx_hbm, cy_hbm, pr_hbm,
    val_hbm, den_hbm, erg_ref,
    cx, cy, rc, C, B, Q, WE, WW, WS, CE, V1, V2, X, LP, U1, U2, Y,
    pack_e, pack_w, from_w, from_e, ga, gb, gc, gd,
    in_sem, out_sem, hs_sem, hr_sem, as_sem, ar_sem,
):
    me_r = lax.axis_index("row")
    me_c = lax.axis_index("col")
    up, down = lax.rem(me_r + nrow - 1, nrow), lax.rem(me_r + 1, nrow)
    west, east = lax.rem(me_c + ncol - 1, ncol), lax.rem(me_c + 1, ncol)
    ext = tiles + 1
    END = TOP + rows

    def tile_of(ref, j):
        return ref.at[:, pl.ds(j * LANE, LANE)]

    loads = {}
    for n, (src, dst, top) in enumerate(((cx_hbm, cx, 0), (cy_hbm, cy, 0), (rc_hbm, rc, 0), (pr_hbm, Q, TOP))):
        for j in range(tiles):
            copy = pltpu.make_async_copy(tile_of(src, j), dst.at[j, pl.ds(top, rows), :], in_sem.at[n, j])
            copy.start()
            loads[n, j] = copy

    barrier = pltpu.get_barrier_semaphore()
    met = 0
    for d in range(1, nrow):
        pl.semaphore_signal(barrier, inc=1, device_id=(lax.rem(me_r + d, nrow), me_c), device_id_type=MESH)
        met += 1
    for d in range(1, ncol):
        pl.semaphore_signal(barrier, inc=1, device_id=(me_r, lax.rem(me_c + d, ncol)), device_id_type=MESH)
        met += 1
    for r in (up, down):
        for c in (west, east):
            pl.semaphore_signal(barrier, inc=1, device_id=(r, c), device_id_type=MESH)
            met += 1

    zero = jnp.zeros((8, LANE), jnp.float32)
    for ref in (C, B, Q, WS, V1, V2, X, U1, U2):
        for j in range(ext):
            ref[j, pl.ds(0, 8), :] = zero
            ref[j, pl.ds(END + HALO, 8), :] = zero

    for copy in loads.values():
        copy.wait()

    def first(i, carry):
        r = pl.multiple_of(i * STEP, STEP)
        for j in range(tiles):
            a, b = cx[j, pl.ds(r, STEP), :], cy[j, pl.ds(r, STEP), :]
            cost = 0.5 * (a * a + b * b)
            C[j, pl.ds(TOP + r, STEP), :] = (1.0 + cost) * FACE
            B[j, pl.ds(TOP + r, STEP), :] = rc[j, pl.ds(r, STEP), :] + cost
        return carry

    lax.fori_loop(0, rows // STEP, first, 0)

    parts = LANE // 16
    pile = rows // parts
    lane = lax.broadcasted_iota(jnp.int32, (pile, LANE), 1)
    slot = lane & 15
    is_c, is_b = slot < 6, slot < 11
    acc_e = jnp.zeros((pile, LANE), jnp.float32)
    acc_w = jnp.zeros((pile, LANE), jnp.float32)
    for k in range(parts):
        at = pl.ds(TOP + pile * k, pile)
        here = (lane >> 4) == k
        got = []
        for j, firsts in ((tiles - 1, (122, 123, 125)), (0, (0, 0, 0))):
            rolled = [
                pltpu.roll(f[j, at, :], (16 * k + o - s) % LANE, 1)
                for f, o, s in zip((C, B, Q), (0, 6, 11), firsts)
            ]
            got.append(jnp.where(is_c, rolled[0], jnp.where(is_b, rolled[1], rolled[2])))
        acc_e = jnp.where(here, got[0], acc_e)
        acc_w = jnp.where(here, got[1], acc_w)
    pack_e[...] = acc_e
    pack_w[...] = acc_w

    pl.semaphore_wait(barrier, met)

    sends = []

    def send(src, dst, to):
        n = len(sends)
        copy = pltpu.make_async_remote_copy(
            src_ref=src, dst_ref=dst, send_sem=hs_sem.at[n], recv_sem=hr_sem.at[n],
            device_id=to, device_id_type=MESH,
        )
        copy.start()
        sends.append(copy)

    send(pack_e, from_w.at[pl.ds(0, pile), :], (me_r, east))
    send(pack_w, from_e.at[pl.ds(0, pile), :], (me_r, west))
    low, high = pl.ds(0, 8), pl.ds(pile - 8, 8)
    sw_at, nw_at = pl.ds(pile, 8), pl.ds(pile + 8, 8)
    send(pack_e.at[high, :], from_w.at[nw_at, :], (down, east))
    send(pack_e.at[low, :], from_w.at[sw_at, :], (up, east))
    send(pack_w.at[high, :], from_e.at[nw_at, :], (down, west))
    send(pack_w.at[low, :], from_e.at[sw_at, :], (up, west))
    body = pl.ds(0, tiles)
    for f in (C, B, Q):
        send(f.at[body, pl.ds(TOP, HALO), :], f.at[body, pl.ds(END, HALO), :], (up, me_c))
        send(f.at[body, pl.ds(END - HALO, HALO), :], f.at[body, pl.ds(TOP - HALO, HALO), :], (down, me_c))

    for copy in sends:
        copy.wait_recv()

    one, nil = jnp.float32(1.0), jnp.float32(0.0)
    has_n = jnp.where(me_r > 0, one, nil)
    has_s = jnp.where(me_r < nrow - 1, one, nil)
    has_w = jnp.where(me_c > 0, one, nil)
    has_e = jnp.where(me_c < ncol - 1, one, nil)

    def unpack(at, src, k, n, keep):
        w = from_w[src, :] * (has_w * keep)
        e = from_e[src, :] * (has_e * keep)
        l = lax.broadcasted_iota(jnp.int32, (n, LANE), 1)
        for f, o, s, wide in zip((C, B, Q), (0, 6, 11), (122, 123, 125), (6, 5, 3)):
            rw = pltpu.roll(w, (s - 16 * k - o) % LANE, 1)
            re = pltpu.roll(e, (-16 * k - o) % LANE, 1)
            f[tiles, at, :] = jnp.where(l >= s, rw, jnp.where(l < wide, re, 0.0))

    for k in range(parts):
        unpack(pl.ds(TOP + pile * k, pile), pl.ds(0, pile), k, pile, one)
    unpack(pl.ds(TOP - HALO, HALO), nw_at, parts - 1, HALO, has_n)
    unpack(pl.ds(END, HALO), sw_at, 0, HALO, has_s)

    @pl.when(me_r == 0)
    def _():
        for f in (C, B, Q):
            for j in range(tiles):
                f[j, pl.ds(TOP - HALO, HALO), :] = zero

    @pl.when(me_r == nrow - 1)
    def _():
        for f in (C, B, Q):
            for j in range(tiles):
                f[j, pl.ds(END, HALO), :] = zero

    lane1 = lax.broadcasted_iota(jnp.int32, (1, LANE), 1)
    inside = jnp.where(lane1 < LANE // 2, has_e, has_w)

    def masks(n):
        l = lax.broadcasted_iota(jnp.int32, (n, LANE), 1)
        return l == LANE - 1, l == 0

    def to_east(vs, last):
        r = [pltpu.roll(v, LANE - 1, 1) for v in vs]
        return [jnp.where(last, r[(j + 1) % ext], r[j]) for j in range(ext)]

    def to_west(vs, start):
        r = [pltpu.roll(v, 1, 1) for v in vs]
        return [jnp.where(start, r[(j - 1) % ext], r[j]) for j in range(ext)]

    def rows_of(ref, r, n):
        return [ref[j, pl.ds(r, n), :] for j in range(ext)]

    def keep_in(vs, keep):
        vs = vs[:tiles] + [vs[tiles] * inside]
        return vs if keep is None else [v * keep for v in vs]

    def put(ref, r, n, vs):
        for j, v in enumerate(vs):
            ref[j, pl.ds(r, n), :] = v

    def fold(acc, v):
        for s in range(0, v.shape[0], 8):
            acc = acc + v[s : s + 8, :]
        return acc

    def add(accs, lists):
        out = []
        for acc, (p, q) in zip(accs, lists):
            total = None
            for j in range(tiles):
                t = p[j] if q is None else p[j] * q[j]
                total = t if total is None else total + t
            out.append(fold(acc, total))
        return tuple(out)

    def apply_from(vs, ref, r, n, center, we, ww, ws, wn, keep):
        last, start = masks(n)
        ve, vw = to_east(vs, last), to_west(vs, start)
        vs_, vn = rows_of(ref, r + 1, n), rows_of(ref, r - 1, n)
        return keep_in(
            [
                center[j] * vs[j] - ((ws[j] * vs_[j] + wn[j] * vn[j]) + (we[j] * ve[j] + ww[j] * vw[j]))
                for j in range(ext)
            ],
            keep,
        )

    def over_rows(step, accs):
        step(TOP - HALO, HALO, None, has_n)
        step(END, HALO, None, has_s)

        def loop(i, accs):
            return step(pl.multiple_of(TOP + i * STEP, STEP), STEP, accs, None)

        return lax.fori_loop(0, rows // STEP, loop, accs)

    def blank(k):
        return tuple(zero for _ in range(k))

    def pass1(r, n, accs, keep):
        last, start = masks(n)
        c0 = rows_of(C, r, n)
        cs, cn = rows_of(C, r + 1, n), rows_of(C, r - 1, n)
        ce, cw = to_east(c0, last), to_west(c0, start)
        we = [c0[j] + ce[j] for j in range(ext)]
        ww = [c0[j] + cw[j] for j in range(ext)]
        ws = [c0[j] + cs[j] for j in range(ext)]
        wn = [c0[j] + cn[j] for j in range(ext)]
        center = [(ws[j] + wn[j]) + (we[j] + ww[j]) for j in range(ext)]
        put(WE, r, n, we)
        put(WW, r, n, ww)
        put(WS, r, n, ws)
        put(CE, r, n, center)
        b = rows_of(B, r, n)
        v1 = apply_from(b, B, r, n, center, we, ww, ws, wn, keep)
        put(V1, r, n, v1)
        if accs is None:
            return None
        q = rows_of(Q, r, n)
        return add(accs, ((b, b), (b, v1), (v1, v1), (q, None), (q, b), (q, v1), (q, q)))

    nu0, nu1, nu2, s_q, s_qb, s_q1, mu0 = over_rows(pass1, blank(7))

    def weights_of(r, n):
        return rows_of(WE, r, n), rows_of(WW, r, n), rows_of(WS, r, n), rows_of(WS, r - 1, n)

    def pass2(r, n, accs, keep):
        v1 = rows_of(V1, r, n)
        v2 = apply_from(v1, V1, r, n, rows_of(CE, r, n), *weights_of(r, n), keep)
        put(V2, r, n, v2)
        if accs is None:
            return None
        q = rows_of(Q, r, n)
        return add(accs, ((v1, v2), (v2, v2), (q, v2)))

    nu3, nu4, s_q2 = over_rows(pass2, blank(3))

    def energy(V, center):
        def step(i, acc):
            r = pl.multiple_of(TOP + i * STEP, STEP)
            last, _ = masks(STEP)
            v = rows_of(V, r, STEP)
            ve = to_east(v, last)
            total = None
            for j in range(tiles):
                out = WE[j, pl.ds(r, STEP), :] * ve[j] + WS[j, pl.ds(r, STEP), :] * V[j, pl.ds(r + 1, STEP), :]
                t = v[j] * (center[j, pl.ds(r, STEP), :] * v[j] - (out + out))
                total = t if total is None else total + t
            return fold(acc, total)

        return lax.fori_loop(0, rows // STEP, step, zero)

    nu5 = energy(V2, CE)

    lane8 = lax.broadcasted_iota(jnp.int32, (8, LANE), 1)

    def start_stage(buf, stage, along_col):
        count, mine = (ncol, me_c) if along_col else (nrow, me_r)
        copies = []
        for d in range(1, count):
            to = lax.rem(mine + d, count)
            copy = pltpu.make_async_remote_copy(
                src_ref=buf.at[mine], dst_ref=buf.at[mine],
                send_sem=as_sem.at[stage, d], recv_sem=ar_sem.at[stage, d],
                device_id=(me_r, to) if along_col else (to, me_c), device_id_type=MESH,
            )
            copy.start()
            copies.append(copy)
        return copies

    def finish_stage(buf, copies):
        for copy in copies:
            copy.wait_recv()
        terms = [buf[k] for k in range(buf.shape[0])]
        while len(terms) > 1:
            terms = [terms[k] + terms[k + 1] if k + 1 < len(terms) else terms[k] for k in range(0, len(terms), 2)]
        return terms[0]

    def gather(accs):
        packed = jnp.zeros((8, LANE), jnp.float32)
        for k, acc in enumerate(accs):
            packed = jnp.where(lane8 == k, jnp.sum(acc, axis=1, keepdims=True), packed)
        return jnp.sum(packed, axis=0, keepdims=True)

    def spread(row, k):
        return jnp.broadcast_to(row[:, k : k + 1], (1, LANE))

    ga[me_c] = gather((nu0, nu1, nu2, nu3, nu4, nu5, s_q, s_qb, s_q1, s_q2))
    stage_a = start_stage(ga, 0, True)

    def pass_q(r, n, accs, keep):
        put(LP, r, n, apply_from(rows_of(Q, r, n), Q, r, n, rows_of(CE, r, n), *weights_of(r, n), keep))
        return accs

    over_rows(pass_q, 0)

    gb[me_r] = finish_stage(ga, stage_a)
    stage_b = start_stage(gb, 1, False)
    for copy in sends + stage_a:
        copy.wait_send()
    sums = finish_stage(gb, stage_b)

    c0, c1, c2 = solve([spread(sums, k) for k in range(6)])
    t_q, t_qb, t_q1, t_q2 = [spread(sums, k) for k in range(6, 10)]

    def pass_x(r, n, accs, keep):
        b, v1, v2 = rows_of(B, r, n), rows_of(V1, r, n), rows_of(V2, r, n)
        put(X, r, n, [c0 * b[j] + (c1 * v1[j] + c2 * v2[j]) for j in range(ext)])
        return accs

    over_rows(pass_x, 0)

    stores = []
    for j in range(tiles):
        copy = pltpu.make_async_copy(X.at[j, pl.ds(TOP, rows), :], tile_of(val_hbm, j), out_sem.at[0, j])
        copy.start()
        stores.append(copy)

    def pass3(r, n, accs, keep):
        last, start = masks(n)
        x = rows_of(X, r, n)
        xe, xw = to_east(x, last), to_west(x, start)
        xs, xn = rows_of(X, r + 1, n), rows_of(X, r - 1, n)
        q, lp, center = rows_of(Q, r, n), rows_of(LP, r, n), rows_of(CE, r, n)
        u1, full = [], []
        for j in range(ext):
            dr, dc = xs[j] - xn[j], xe[j] - xw[j]
            g = (0.25 / (2.0 * 0.25) * SCALE) * (dr * dr + dc * dc)
            full.append(center[j] + g)
            u1.append(lp[j] + g * q[j])
        u1 = keep_in(u1, keep)
        put(CE, r, n, full)
        put(U1, r, n, u1)
        if accs is None:
            return None
        return add(accs, ((q, u1), (u1, u1)))

    mu1, mu2 = over_rows(pass3, blank(2))

    def pass4(r, n, accs, keep):
        u1 = rows_of(U1, r, n)
        u2 = apply_from(u1, U1, r, n, rows_of(CE, r, n), *weights_of(r, n), keep)
        put(U2, r, n, u2)
        return None if accs is None else add(accs, ((u1, u2), (u2, u2)))

    mu3, mu4 = over_rows(pass4, blank(2))
    mu5 = energy(U2, CE)

    gc[me_c] = gather((mu0, mu1, mu2, mu3, mu4, mu5))
    stage_c = start_stage(gc, 2, True)
    erg_ref[...] = (t_qb - DISCOUNT * (c0 * t_qb + (c1 * t_q1 + c2 * t_q2))) / t_q
    for copy in stage_b:
        copy.wait_send()
    gd[me_r] = finish_stage(gc, stage_c)
    stage_d = start_stage(gd, 3, False)
    for copy in stage_c:
        copy.wait_send()
    for copy in stores:
        copy.wait()
    sums = finish_stage(gd, stage_d)
    d0, d1, d2 = solve([spread(sums, k) for k in range(6)])

    def last_pass(i, carry):
        r = pl.multiple_of(TOP + i * STEP, STEP)
        at = pl.ds(r, STEP)
        for j in range(tiles):
            Y[j, pl.ds(pl.multiple_of(i * STEP, STEP), STEP), :] = d0 * Q[j, at, :] + (d1 * U1[j, at, :] + d2 * U2[j, at, :])
        return carry

    lax.fori_loop(0, rows // STEP, last_pass, 0)
    outs = []
    for j in range(tiles):
        copy = pltpu.make_async_copy(Y.at[j], tile_of(den_hbm, j), out_sem.at[1, j])
        copy.start()
        outs.append(copy)
    for copy in stage_d:
        copy.wait_send()
    for copy in outs:
        copy.wait()


def solution(mesh):
    nrow, ncol = mesh.shape["row"], mesh.shape["col"]

    def body(running_cost, control_x, control_y, prior_density):
        rows, cols = running_cost.shape
        tiles = cols // LANE
        ext = tiles + 1
        pile = rows // 8
        big = pltpu.VMEM((ext, rows + 2 * TOP, LANE), jnp.float32)
        plain = pltpu.VMEM((tiles, rows, LANE), jnp.float32)
        most = max(nrow, ncol)
        value, density, ergodic = pl.pallas_call(
            functools.partial(kernel, nrow, ncol, rows, tiles),
            out_shape=(
                jax.ShapeDtypeStruct((rows, cols), jnp.float32),
                jax.ShapeDtypeStruct((rows, cols), jnp.float32),
                jax.ShapeDtypeStruct((1, LANE), jnp.float32),
            ),
            in_specs=[pl.BlockSpec(memory_space=pltpu.HBM)] * 4,
            out_specs=(
                pl.BlockSpec(memory_space=pltpu.HBM),
                pl.BlockSpec(memory_space=pltpu.HBM),
                pl.BlockSpec(memory_space=pltpu.VMEM),
            ),
            scratch_shapes=[plain] * 3
            + [big] * 13
            + [plain]
            + [pltpu.VMEM((pile, LANE), jnp.float32)] * 2
            + [pltpu.VMEM((pile + 16, LANE), jnp.float32)] * 2
            + [pltpu.VMEM((ncol, 1, LANE), jnp.float32), pltpu.VMEM((nrow, 1, LANE), jnp.float32)] * 2
            + [
                pltpu.SemaphoreType.DMA((4, tiles)),
                pltpu.SemaphoreType.DMA((2, tiles)),
                pltpu.SemaphoreType.DMA((12,)),
                pltpu.SemaphoreType.DMA((12,)),
                pltpu.SemaphoreType.DMA((4, most)),
                pltpu.SemaphoreType.DMA((4, most)),
            ],
            compiler_params=pltpu.CompilerParams(
                collective_id=0, has_side_effects=True, vmem_limit_bytes=48 * 1024 * 1024
            ),
        )(running_cost, control_x, control_y, prior_density)
        return value, density, ergodic[0, 0]

    spec = P("row", "col")
    return jax.shard_map(
        body,
        mesh=mesh,
        in_specs=(spec, spec, spec, spec),
        out_specs=(spec, spec, P()),
        check_vma=False,
    )
```

```python
import functools

import jax
import jax.numpy as jnp
from jax import lax
from jax.experimental import pallas as pl
from jax.experimental.pallas import tpu as pltpu
from jax.sharding import PartitionSpec as P

MESH = pl.DeviceIdType.MESH

SCALE = 1.0 / 64.0
FACE = 0.25 * 0.5 * SCALE
DISCOUNT = 0.05

LANE = 128
TOP = 16
HALO = 8


def solve(nu):
    shift = DISCOUNT * SCALE
    m = [nu[k + 1] + shift * nu[k] for k in range(5)]
    l1 = m[1] / m[0]
    l2 = m[2] / m[0]
    d1 = m[2] - l1 * m[1]
    e = m[3] - l2 * m[1]
    l3 = e / d1
    d2 = (m[4] - l2 * m[2]) - l3 * e
    y0 = nu[0]
    y1 = nu[1] - l1 * y0
    y2 = (nu[2] - l2 * y0) - l3 * y1
    c2 = y2 / d2
    c1 = y1 / d1 - l3 * c2
    c0 = y0 / m[0] - l1 * c1 - l2 * c2
    return c0 * SCALE, c1 * SCALE, c2 * SCALE


def kernel(
    nrow, ncol, nx, rows, tiles, step_rows,
    rc_hbm, cx_hbm, cy_hbm, pr_hbm,
    val_ref, den_ref, erg_ref,
    cx, cy, rc, C, B, Q, WE, WW, WS, CE, V1, V2, X, LP, U1, U2,
    pack_e, pack_w, from_w, from_e, ga, gb, gc, gd,
    in_sem, hs_sem, hr_sem, as_sem, ar_sem, near_sem,
):
    me_r = lax.axis_index("row")
    me_c = lax.axis_index("col")
    up, down = lax.rem(me_r + nrow - 1, nrow), lax.rem(me_r + 1, nrow)
    west, east = lax.rem(me_c + ncol - 1, ncol), lax.rem(me_c + 1, ncol)
    ext = tiles + 1
    END = TOP + rows

    def tile_of(ref, j):
        return ref.at[:, pl.ds(j * LANE, LANE)]

    loads = {}
    for n, (src, dst, top) in enumerate(((cx_hbm, cx, 0), (cy_hbm, cy, 0), (rc_hbm, rc, 0), (pr_hbm, Q, TOP))):
        for j in range(tiles):
            copy = pltpu.make_async_copy(tile_of(src, j), dst.at[j, pl.ds(top, rows), :], in_sem.at[n, j])
            copy.start()
            loads[n, j] = copy

    nz, ny = nrow // 2, ncol // nx
    core, z = lax.rem(me_r, 2), me_r // 2
    x, y = me_c // ny, lax.rem(me_c, ny)

    def at_offset(dz, dc, dx, dy):
        r = 2 * lax.rem(z + dz, nz) + lax.rem(core + dc, 2)
        return r, ny * lax.rem(x + dx, nx) + lax.rem(y + dy, ny)

    def offsets(zs, cs, xs, ys):
        every = {(a % nz, b, c % nx, d % ny) for a in zs for b in cs for c in xs for d in ys}
        return sorted(every - {(0, 0, 0, 0)})

    def tell(sem, to):
        pl.semaphore_signal(sem, inc=1, device_id=to, device_id_type=MESH)

    not_first, not_last = me_r > 0, me_r < nrow - 1
    not_west, not_east = me_c > 0, me_c < ncol - 1
    beyond = me_r + 2 * core - 1
    far_row = lax.rem(beyond + nrow, nrow)

    def when(*conditions):
        def run(fn):
            for c in conditions[::-1]:
                fn = functools.partial(lambda c, f: pl.when(c)(f) and None, c, fn)
            fn()
        return run

    far_there = (beyond >= 0, beyond < nrow)

    barrier = pltpu.get_barrier_semaphore()
    around = (-1, 0, 1)
    near = offsets((0,), (0, 1), around, around) + offsets(around, (0,), (0,), (0,))
    for o in near:
        tell(barrier, at_offset(*o))
    when(*far_there)(lambda: tell(barrier, (far_row, me_c)))
    when(*far_there, not_west)(lambda: tell(barrier, (far_row, west)))
    when(*far_there, not_east)(lambda: tell(barrier, (far_row, east)))

    zero = jnp.zeros((8, LANE), jnp.float32)
    for ref in (C, B, Q, WS, V1, V2, X, U1, U2):
        for j in range(ext):
            ref[j, pl.ds(0, 8), :] = zero
            ref[j, pl.ds(END + HALO, 8), :] = zero

    low, high = pl.ds(0, 8), pl.ds(rows // 8 - 8, 8)
    sw_at, nw_at = pl.ds(rows // 8, 8), pl.ds(rows // 8 + 8, 8)

    @pl.when(me_c == 0)
    def _():
        from_w[...] = jnp.zeros_like(from_w)

    @pl.when(me_c == ncol - 1)
    def _():
        from_e[...] = jnp.zeros_like(from_e)

    def no_row(top, corner):
        for f in (C, B, Q):
            for j in range(tiles):
                f[j, pl.ds(top, HALO), :] = zero
        from_w[corner, :] = zero
        from_e[corner, :] = zero

    @pl.when(me_r == 0)
    def _():
        no_row(TOP - HALO, nw_at)

    @pl.when(me_r == nrow - 1)
    def _():
        no_row(END, sw_at)

    for copy in loads.values():
        copy.wait()

    def first(i, carry):
        r = pl.multiple_of(i * step_rows, step_rows)
        for j in range(tiles):
            a, b = cx[j, pl.ds(r, step_rows), :], cy[j, pl.ds(r, step_rows), :]
            cost = 0.5 * (a * a + b * b)
            C[j, pl.ds(TOP + r, step_rows), :] = (1.0 + cost) * FACE
            B[j, pl.ds(TOP + r, step_rows), :] = rc[j, pl.ds(r, step_rows), :] + cost
        return carry

    lax.fori_loop(0, rows // step_rows, first, 0)

    parts = LANE // 16
    pile = rows // parts
    lane = lax.broadcasted_iota(jnp.int32, (pile, LANE), 1)
    slot = lane & 15
    is_c, is_b = slot < 6, slot < 11
    acc_e = jnp.zeros((pile, LANE), jnp.float32)
    acc_w = jnp.zeros((pile, LANE), jnp.float32)
    for k in range(parts):
        at = pl.ds(TOP + pile * k, pile)
        here = (lane >> 4) == k
        got = []
        for j, firsts in ((tiles - 1, (122, 123, 125)), (0, (0, 0, 0))):
            rolled = [
                pltpu.roll(f[j, at, :], (16 * k + o - s) % LANE, 1)
                for f, o, s in zip((C, B, Q), (0, 6, 11), firsts)
            ]
            got.append(jnp.where(is_c, rolled[0], jnp.where(is_b, rolled[1], rolled[2])))
        acc_e = jnp.where(here, got[0], acc_e)
        acc_w = jnp.where(here, got[1], acc_w)
    pack_e[...] = acc_e
    pack_w[...] = acc_w

    any_west, any_east = (me_c + ncol - 1) // ncol, (2 * ncol - 2 - me_c) // ncol
    any_far = core * ((2 * nrow - 2 - me_r) // nrow) + (1 - core) * ((me_r + nrow - 1) // nrow)
    pl.semaphore_wait(barrier, len(near) + any_far * (1 + any_west + any_east))

    sends = []

    def send(src, dst, to, there, here):
        n = len(sends)
        copy = pltpu.make_async_remote_copy(
            src_ref=src, dst_ref=dst, send_sem=hs_sem.at[n], recv_sem=hr_sem.at[n],
            device_id=to, device_id_type=MESH,
        )
        when(*there)(copy.start)
        sends.append((copy, there, here))

    send(pack_e.at[high, :], from_w.at[nw_at, :], (down, east), (not_last, not_east), (not_first, not_west))
    send(pack_e.at[low, :], from_w.at[sw_at, :], (up, east), (not_first, not_east), (not_last, not_west))
    send(pack_w.at[high, :], from_e.at[nw_at, :], (down, west), (not_last, not_west), (not_first, not_east))
    send(pack_w.at[low, :], from_e.at[sw_at, :], (up, west), (not_first, not_west), (not_last, not_east))
    send(pack_e, from_w.at[pl.ds(0, pile), :], (me_r, east), (not_east,), (not_west,))
    send(pack_w, from_e.at[pl.ds(0, pile), :], (me_r, west), (not_west,), (not_east,))
    body = pl.ds(0, tiles)
    for f in (C, B, Q):
        send(f.at[body, pl.ds(TOP, HALO), :], f.at[body, pl.ds(END, HALO), :], (up, me_c), (not_first,), (not_last,))
        send(f.at[body, pl.ds(END - HALO, HALO), :], f.at[body, pl.ds(TOP - HALO, HALO), :], (down, me_c), (not_last,), (not_first,))

    first_ring = offsets((0,), (0,), around, around) + offsets(around, (0,), (0,), (0,))
    second_ring = offsets((-2, 2), (0,), (0,), (0,))
    for o in first_ring:
        tell(near_sem.at[0], at_offset(*o))

    for copy, _, here in sends:
        when(*here)(copy.wait_recv)

    pl.semaphore_wait(near_sem.at[0], len(first_ring))
    for o in second_ring:
        tell(near_sem.at[1], at_offset(*o))

    fone, fnil = jnp.float32(1.0), jnp.float32(0.0)
    has_n, has_s = jnp.where(not_first, fone, fnil), jnp.where(not_last, fone, fnil)
    has_w, has_e = jnp.where(not_west, fone, fnil), jnp.where(not_east, fone, fnil)

    def unpack(at, src, k, n):
        w, e = from_w[src, :], from_e[src, :]
        l = lax.broadcasted_iota(jnp.int32, (n, LANE), 1)
        none = jnp.zeros((n, LANE), jnp.float32)
        for f, o, s, wide in zip((C, B, Q), (0, 6, 11), (122, 123, 125), (6, 5, 3)):
            rw = pltpu.roll(w, (s - 16 * k - o) % LANE, 1)
            re = pltpu.roll(e, (-16 * k - o) % LANE, 1)
            f[tiles, at, :] = jnp.where(l >= s, rw, jnp.where(l < wide, re, none))

    for k in range(parts):
        unpack(pl.ds(TOP + pile * k, pile), pl.ds(0, pile), k, pile)
    unpack(pl.ds(TOP - HALO, HALO), nw_at, parts - 1, HALO)
    unpack(pl.ds(END, HALO), sw_at, 0, HALO)

    lane1 = lax.broadcasted_iota(jnp.int32, (1, LANE), 1)
    inside = jnp.where(lane1 < LANE // 2, has_e, has_w)

    def masks(n):
        l = lax.broadcasted_iota(jnp.int32, (n, LANE), 1)
        return l == LANE - 1, l == 0

    def to_east(vs, last):
        r = [pltpu.roll(v, LANE - 1, 1) for v in vs]
        return [jnp.where(last, r[(j + 1) % ext], r[j]) for j in range(ext)]

    def to_west(vs, start):
        r = [pltpu.roll(v, 1, 1) for v in vs]
        return [jnp.where(start, r[(j - 1) % ext], r[j]) for j in range(ext)]

    def rows_of(ref, r, n):
        return [ref[j, pl.ds(r, n), :] for j in range(ext)]

    def keep_in(vs, keep):
        vs = vs[:tiles] + [vs[tiles] * inside]
        return vs if keep is None else [v * keep for v in vs]

    def put(ref, r, n, vs):
        for j, v in enumerate(vs):
            ref[j, pl.ds(r, n), :] = v

    def fold(acc, v):
        while v.shape[0] > 8:
            half = v.shape[0] // 2
            v = v[:half, :] + v[half:, :]
        return acc + v

    def add(accs, lists):
        out = []
        for acc, (p, q) in zip(accs, lists):
            total = None
            for j in range(tiles):
                t = p[j] if q is None else p[j] * q[j]
                total = t if total is None else total + t
            out.append(fold(acc, total))
        return tuple(out)

    def apply_from(vs, ref, r, n, center, we, ww, ws, wn, keep):
        last, start = masks(n)
        ve, vw = to_east(vs, last), to_west(vs, start)
        vs_, vn = rows_of(ref, r + 1, n), rows_of(ref, r - 1, n)
        return keep_in(
            [
                center[j] * vs[j] - ((ws[j] * vs_[j] + wn[j] * vn[j]) + (we[j] * ve[j] + ww[j] * vw[j]))
                for j in range(ext)
            ],
            keep,
        )

    def over_rows(step, accs):
        step(TOP - HALO, HALO, None, has_n)
        step(END, HALO, None, has_s)

        def loop(i, accs):
            return step(pl.multiple_of(TOP + i * step_rows, TOP), step_rows, accs, None)

        return lax.fori_loop(0, rows // step_rows, loop, accs)

    def blank(k):
        return tuple(zero for _ in range(k))

    def pass1(r, n, accs, keep):
        last, start = masks(n)
        c0 = rows_of(C, r, n)
        cs, cn = rows_of(C, r + 1, n), rows_of(C, r - 1, n)
        ce, cw = to_east(c0, last), to_west(c0, start)
        we = [c0[j] + ce[j] for j in range(ext)]
        ww = [c0[j] + cw[j] for j in range(ext)]
        ws = [c0[j] + cs[j] for j in range(ext)]
        wn = [c0[j] + cn[j] for j in range(ext)]
        center = [(ws[j] + wn[j]) + (we[j] + ww[j]) for j in range(ext)]
        put(WE, r, n, we)
        put(WW, r, n, ww)
        put(WS, r, n, ws)
        put(CE, r, n, center)
        b = rows_of(B, r, n)
        v1 = apply_from(b, B, r, n, center, we, ww, ws, wn, keep)
        put(V1, r, n, v1)
        if accs is None:
            return None
        q = rows_of(Q, r, n)
        return add(accs, ((b, b), (b, v1), (v1, v1), (q, None), (q, b), (q, v1), (q, q)))

    nu0, nu1, nu2, s_q, s_qb, s_q1, mu0 = over_rows(pass1, blank(7))

    def weights_of(r, n):
        return rows_of(WE, r, n), rows_of(WW, r, n), rows_of(WS, r, n), rows_of(WS, r - 1, n)

    def pass2(r, n, accs, keep):
        v1 = rows_of(V1, r, n)
        v2 = apply_from(v1, V1, r, n, rows_of(CE, r, n), *weights_of(r, n), keep)
        put(V2, r, n, v2)
        if accs is None:
            return None
        q = rows_of(Q, r, n)
        return add(accs, ((v1, v2), (v2, v2), (q, v2)))

    nu3, nu4, s_q2 = over_rows(pass2, blank(3))

    def energy(V, center):
        def step(i, acc):
            r = pl.multiple_of(TOP + i * step_rows, TOP)
            last, _ = masks(step_rows)
            v = rows_of(V, r, step_rows)
            ve = to_east(v, last)
            total = None
            for j in range(tiles):
                out = WE[j, pl.ds(r, step_rows), :] * ve[j] + WS[j, pl.ds(r, step_rows), :] * V[j, pl.ds(r + 1, step_rows), :]
                t = v[j] * (center[j, pl.ds(r, step_rows), :] * v[j] - (out + out))
                total = t if total is None else total + t
            return fold(acc, total)

        return lax.fori_loop(0, rows // step_rows, step, zero)

    nu5 = energy(V2, CE)

    lane8 = lax.broadcasted_iota(jnp.int32, (8, LANE), 1)

    def add_up(buf, count):
        terms = [buf[k] for k in range(count)]
        while len(terms) > 1:
            terms = [terms[k] + terms[k + 1] if k + 1 < len(terms) else terms[k] for k in range(0, len(terms), 2)]
        return terms[0]

    def start_sum(part, ga, gb, stage):
        slot = core * ncol + me_c
        ga[slot] = part
        out = []
        for d in sorted(range(ncol), key=lambda d: -min(d, ncol - d)):
            copy = pltpu.make_async_remote_copy(
                src_ref=ga.at[slot], dst_ref=ga.at[slot],
                send_sem=as_sem.at[stage, d], recv_sem=ar_sem.at[stage, core * ncol + d],
                device_id=(2 * z + 1, lax.rem(me_c + d, ncol)), device_id_type=MESH,
            )
            if d == 0:
                pl.when(core == 0)(copy.start)
            else:
                copy.start()
            out.append((d, copy))
        return out

    def arrival(buf, slot, sem):
        return pltpu.make_async_remote_copy(
            src_ref=buf.at[slot], dst_ref=buf.at[slot], send_sem=sem, recv_sem=sem,
            device_id=(far_row, me_c), device_id_type=MESH,
        )

    def finish_sum(out, ga, gb, stage):
        again = []
        for dz in sorted(range(nz), key=lambda d: -min(d, nz - d)):
            for to_core in (0, 1):
                if dz or to_core == 0:
                    again.append(
                        pltpu.make_async_remote_copy(
                            src_ref=gb.at[z], dst_ref=gb.at[z],
                            send_sem=as_sem.at[stage + 1, 2 * dz + to_core], recv_sem=ar_sem.at[stage + 1, dz],
                            device_id=(2 * lax.rem(z + dz, nz) + to_core, me_c), device_id_type=MESH,
                        )
                    )

        @pl.when(core == 1)
        def _():
            for n in range(2 * ncol):
                if n != ncol:
                    arrival(ga, 0, ar_sem.at[stage, n]).wait_recv()
            if stage == 0:
                pl.semaphore_wait(near_sem.at[1], len(second_ring))
            gb[z] = add_up(ga, 2 * ncol)
            for copy in again:
                copy.start()

        if stage == 0:
            pl.when(core == 0)(lambda: pl.semaphore_wait(near_sem.at[1], len(second_ring)))
        for d, copy in out:
            if d == 0:
                pl.when(core == 0)(copy.wait_send)
            else:
                copy.wait_send()
        for dz in range(nz):
            come = arrival(gb, 0, ar_sem.at[stage + 1, dz])
            if dz == 0:
                pl.when(core == 0)(come.wait_recv)
            else:
                come.wait_recv()
        return add_up(gb, nz), again

    def settle(again):
        @pl.when(core == 1)
        def _():
            for copy in again:
                copy.wait_send()

    def gather(accs):
        packed = jnp.zeros((8, LANE), jnp.float32)
        for k, acc in enumerate(accs):
            packed = jnp.where(lane8 == k, jnp.sum(acc, axis=1, keepdims=True), packed)
        return jnp.sum(packed, axis=0, keepdims=True)

    def spread(row, k):
        return jnp.broadcast_to(row[:, k : k + 1], (1, LANE))

    out1 = start_sum(gather((nu0, nu1, nu2, nu3, nu4, nu5, s_q, s_qb, s_q1, s_q2)), ga, gb, 0)

    def pass_q(r, n, accs, keep):
        put(LP, r, n, apply_from(rows_of(Q, r, n), Q, r, n, rows_of(CE, r, n), *weights_of(r, n), keep))
        return accs

    over_rows(pass_q, 0)

    for copy, there, _ in sends:
        when(*there)(copy.wait_send)
    sums, again1 = finish_sum(out1, ga, gb, 0)

    c0, c1, c2 = solve([spread(sums, k) for k in range(6)])
    t_q, t_qb, t_q1, t_q2 = [spread(sums, k) for k in range(6, 10)]

    def pass_x(r, n, accs, keep):
        b, v1, v2 = rows_of(B, r, n), rows_of(V1, r, n), rows_of(V2, r, n)
        value = [c0 * b[j] + (c1 * v1[j] + c2 * v2[j]) for j in range(ext)]
        put(X, r, n, value)
        if keep is None:
            for j in range(tiles):
                val_ref[pl.ds(pl.multiple_of(r - TOP, 8), n), pl.ds(j * LANE, LANE)] = value[j]
        return accs

    over_rows(pass_x, 0)

    def pass3(r, n, accs, keep):
        last, start = masks(n)
        x = rows_of(X, r, n)
        xe, xw = to_east(x, last), to_west(x, start)
        xs, xn = rows_of(X, r + 1, n), rows_of(X, r - 1, n)
        q, lp, center = rows_of(Q, r, n), rows_of(LP, r, n), rows_of(CE, r, n)
        u1, full = [], []
        for j in range(ext):
            dr, dc = xs[j] - xn[j], xe[j] - xw[j]
            g = (0.25 / (2.0 * 0.25) * SCALE) * (dr * dr + dc * dc)
            full.append(center[j] + g)
            u1.append(lp[j] + g * q[j])
        u1 = keep_in(u1, keep)
        put(CE, r, n, full)
        put(U1, r, n, u1)
        if accs is None:
            return None
        return add(accs, ((q, u1), (u1, u1)))

    mu1, mu2 = over_rows(pass3, blank(2))

    def pass4(r, n, accs, keep):
        u1 = rows_of(U1, r, n)
        u2 = apply_from(u1, U1, r, n, rows_of(CE, r, n), *weights_of(r, n), keep)
        put(U2, r, n, u2)
        return None if accs is None else add(accs, ((u1, u2), (u2, u2)))

    mu3, mu4 = over_rows(pass4, blank(2))
    mu5 = energy(U2, CE)

    out2 = start_sum(gather((mu0, mu1, mu2, mu3, mu4, mu5)), gc, gd, 2)
    erg_ref[...] = (t_qb - DISCOUNT * (c0 * t_qb + (c1 * t_q1 + c2 * t_q2))) / t_q
    settle(again1)
    sums, again2 = finish_sum(out2, gc, gd, 2)
    d0, d1, d2 = solve([spread(sums, k) for k in range(6)])

    def last_pass(i, carry):
        r = pl.multiple_of(i * step_rows, step_rows)
        at = pl.ds(TOP + r, step_rows)
        for j in range(tiles):
            den_ref[pl.ds(r, step_rows), pl.ds(j * LANE, LANE)] = d0 * Q[j, at, :] + (d1 * U1[j, at, :] + d2 * U2[j, at, :])
        return carry

    lax.fori_loop(0, rows // step_rows, last_pass, 0)
    settle(again2)


def store_kernel(val_ref, den_ref, val_hbm, den_hbm, sem):
    copies = [pltpu.make_async_copy(val_ref, val_hbm, sem.at[0]), pltpu.make_async_copy(den_ref, den_hbm, sem.at[1])]
    for copy in copies:
        copy.start()
    for copy in copies:
        copy.wait()


def solution(mesh):
    nrow, ncol = mesh.shape["row"], mesh.shape["col"]

    def body(running_cost, control_x, control_y, prior_density):
        rows, cols = running_cost.shape
        tiles = cols // LANE
        ext = tiles + 1
        pile = rows // 8
        big = pltpu.VMEM((ext, rows + 2 * TOP, LANE), jnp.float32)
        plain = pltpu.VMEM((tiles, rows, LANE), jnp.float32)
        most = max(nrow, ncol)
        value, density, ergodic = pl.pallas_call(
            functools.partial(kernel, nrow, ncol, 4 if ncol % 4 == 0 else 1, rows, tiles, min(rows, 64)),
            out_shape=(
                jax.ShapeDtypeStruct((rows, cols), jnp.float32),
                jax.ShapeDtypeStruct((rows, cols), jnp.float32),
                jax.ShapeDtypeStruct((1, LANE), jnp.float32),
            ),
            in_specs=[pl.BlockSpec(memory_space=pltpu.HBM)] * 4,
            out_specs=(pl.BlockSpec(memory_space=pltpu.VMEM),) * 3,
            scratch_shapes=[plain] * 3
            + [big] * 13
            + [pltpu.VMEM((pile, LANE), jnp.float32)] * 2
            + [pltpu.VMEM((pile + 16, LANE), jnp.float32)] * 2
            + [pltpu.VMEM((2 * ncol, 1, LANE), jnp.float32), pltpu.VMEM((nrow // 2, 1, LANE), jnp.float32)] * 2
            + [
                pltpu.SemaphoreType.DMA((4, tiles)),
                pltpu.SemaphoreType.DMA((12,)),
                pltpu.SemaphoreType.DMA((12,)),
                pltpu.SemaphoreType.DMA((4, most)),
                pltpu.SemaphoreType.DMA((4, 2 * ncol)),
                pltpu.SemaphoreType.REGULAR((2,)),
            ],
            compiler_params=pltpu.CompilerParams(
                collective_id=0, has_side_effects=True, vmem_limit_bytes=55200000
            ),
        )(running_cost, control_x, control_y, prior_density)
        value, density = pl.pallas_call(
            store_kernel,
            out_shape=(jax.ShapeDtypeStruct((rows, cols), jnp.float32),) * 2,
            in_specs=[pl.BlockSpec(memory_space=pltpu.VMEM)] * 2,
            out_specs=(pl.BlockSpec(memory_space=pltpu.HBM),) * 2,
            scratch_shapes=[pltpu.SemaphoreType.DMA((2,))],
            compiler_params=pltpu.CompilerParams(vmem_limit_bytes=4 * 1024 * 1024),
        )(value, density)
        return value, density, ergodic[0, 0]

    spec = P("row", "col")
    return jax.shard_map(
        body,
        mesh=mesh,
        in_specs=(spec, spec, spec, spec),
        out_specs=(spec, spec, P()),
        check_vma=False,
    )
```

```python
import functools

import jax
import jax.numpy as jnp
from jax import lax
from jax.experimental import pallas as pl
from jax.experimental.pallas import tpu as pltpu
from jax.sharding import PartitionSpec as P

MESH = pl.DeviceIdType.MESH

SCALE = 1.0 / 64.0
FACE = 0.25 * 0.5 * SCALE
DISCOUNT = 0.05

LANE = 128
TOP = 16
HALO = 8


def solve(nu):
    shift = DISCOUNT * SCALE
    m = [nu[k + 1] + shift * nu[k] for k in range(5)]
    l1 = m[1] / m[0]
    l2 = m[2] / m[0]
    d1 = m[2] - l1 * m[1]
    e = m[3] - l2 * m[1]
    l3 = e / d1
    d2 = (m[4] - l2 * m[2]) - l3 * e
    y0 = nu[0]
    y1 = nu[1] - l1 * y0
    y2 = (nu[2] - l2 * y0) - l3 * y1
    c2 = y2 / d2
    c1 = y1 / d1 - l3 * c2
    c0 = y0 / m[0] - l1 * c1 - l2 * c2
    return c0 * SCALE, c1 * SCALE, c2 * SCALE


def kernel(
    nrow, ncol, nx, rows, tiles, step_rows,
    rc_hbm, cx_hbm, cy_hbm, pr_hbm,
    val_ref, den_ref, erg_ref,
    cx, cy, rc, C, B, Q, WE, WW, WS, CE, V1, V2, X, LP, U1, U2,
    pack_e, pack_w, from_w, from_e, SC, SB, S1, S2, ga, gb, gc, gd,
    in_sem, hs_sem, hr_sem, as_sem, ar_sem, near_sem,
):
    me_r = lax.axis_index("row")
    me_c = lax.axis_index("col")
    up, down = lax.rem(me_r + nrow - 1, nrow), lax.rem(me_r + 1, nrow)
    west, east = lax.rem(me_c + ncol - 1, ncol), lax.rem(me_c + 1, ncol)
    ext = tiles + 1
    END = TOP + rows

    def tile_of(ref, j):
        return ref.at[:, pl.ds(j * LANE, LANE)]

    loads = {}
    for n, (src, dst, top) in enumerate(((cx_hbm, cx, 0), (cy_hbm, cy, 0), (rc_hbm, rc, 0), (pr_hbm, Q, TOP))):
        for j in range(tiles):
            copy = pltpu.make_async_copy(tile_of(src, j), dst.at[j, pl.ds(top, rows), :], in_sem.at[n, j])
            copy.start()
            loads[n, j] = copy

    nz, ny = nrow // 2, ncol // nx
    core, z = lax.rem(me_r, 2), me_r // 2
    x, y = me_c // ny, lax.rem(me_c, ny)

    def at_offset(dz, dc, dx, dy):
        r = 2 * lax.rem(z + dz, nz) + lax.rem(core + dc, 2)
        return r, ny * lax.rem(x + dx, nx) + lax.rem(y + dy, ny)

    def offsets(zs, cs, xs, ys):
        every = {(a % nz, b, c % nx, d % ny) for a in zs for b in cs for c in xs for d in ys}
        return sorted(every - {(0, 0, 0, 0)})

    def tell(sem, to):
        pl.semaphore_signal(sem, inc=1, device_id=to, device_id_type=MESH)

    not_first, not_last = me_r > 0, me_r < nrow - 1
    not_west, not_east = me_c > 0, me_c < ncol - 1
    beyond = me_r + 2 * core - 1
    far_row = lax.rem(beyond + nrow, nrow)

    def when(*conditions):
        def run(fn):
            for c in conditions[::-1]:
                fn = functools.partial(lambda c, f: pl.when(c)(f) and None, c, fn)
            fn()
        return run

    far_there = (beyond >= 0, beyond < nrow)

    barrier = pltpu.get_barrier_semaphore()
    around = (-1, 0, 1)
    near = offsets((0,), (0, 1), around, around) + offsets(around, (0,), (0,), (0,))
    for o in near:
        tell(barrier, at_offset(*o))
    when(*far_there)(lambda: tell(barrier, (far_row, me_c)))
    when(*far_there, not_west)(lambda: tell(barrier, (far_row, west)))
    when(*far_there, not_east)(lambda: tell(barrier, (far_row, east)))

    zero = jnp.zeros((8, LANE), jnp.float32)
    for ref in (C, B, Q, WS, V1, V2, X, U1, U2):
        for j in range(ext):
            ref[j, pl.ds(0, 8), :] = zero
            ref[j, pl.ds(END + HALO, 8), :] = zero

    low, high = pl.ds(0, 8), pl.ds(rows // 8 - 8, 8)
    sw_at, nw_at = pl.ds(rows // 8, 8), pl.ds(rows // 8 + 8, 8)

    @pl.when(me_c == 0)
    def _():
        from_w[...] = jnp.zeros_like(from_w)

    @pl.when(me_c == ncol - 1)
    def _():
        from_e[...] = jnp.zeros_like(from_e)

    def no_row(top, corner):
        for f in (C, B, Q):
            for j in range(tiles):
                f[j, pl.ds(top, HALO), :] = zero
        from_w[corner, :] = zero
        from_e[corner, :] = zero

    @pl.when(me_r == 0)
    def _():
        no_row(TOP - HALO, nw_at)

    @pl.when(me_r == nrow - 1)
    def _():
        no_row(END, sw_at)

    for copy in loads.values():
        copy.wait()

    def fold(acc, v):
        while v.shape[0] > 8:
            n = v.shape[0]
            if n % 16 == 0:
                v = v[: n // 2, :] + v[n // 2 :, :]
            else:
                acc, v = acc + v[n - 8 :, :], v[: n - 8, :]
        return acc + v

    def blank(k):
        return tuple(zero for _ in range(k))

    def first(i, accs):
        r = pl.multiple_of(i * step_rows, step_rows)
        at = pl.ds(TOP + r, step_rows)
        terms = [None] * 4
        for j in range(tiles):
            a, b = cx[j, pl.ds(r, step_rows), :], cy[j, pl.ds(r, step_rows), :]
            cost = 0.5 * (a * a + b * b)
            force = rc[j, pl.ds(r, step_rows), :] + cost
            C[j, at, :] = (1.0 + cost) * FACE
            B[j, at, :] = force
            q = Q[j, at, :]
            for k, t in enumerate((force * force, q, q * force, q * q)):
                terms[k] = t if j == 0 else terms[k] + t
        return tuple(fold(acc, t) for acc, t in zip(accs, terms))

    nu0, s_q, s_qb, mu0 = lax.fori_loop(0, rows // step_rows, first, blank(4))

    parts = LANE // 16
    pile = rows // parts
    lane = lax.broadcasted_iota(jnp.int32, (pile, LANE), 1)
    slot = lane & 15
    is_c, is_b = slot < 6, slot < 11
    acc_e = jnp.zeros((pile, LANE), jnp.float32)
    acc_w = jnp.zeros((pile, LANE), jnp.float32)
    for k in range(parts):
        at = pl.ds(TOP + pile * k, pile)
        here = (lane >> 4) == k
        got = []
        for j, firsts in ((tiles - 1, (122, 123, 125)), (0, (0, 0, 0))):
            rolled = [
                pltpu.roll(f[j, at, :], (16 * k + o - s) % LANE, 1)
                for f, o, s in zip((C, B, Q), (0, 6, 11), firsts)
            ]
            got.append(jnp.where(is_c, rolled[0], jnp.where(is_b, rolled[1], rolled[2])))
        acc_e = jnp.where(here, got[0], acc_e)
        acc_w = jnp.where(here, got[1], acc_w)
    pack_e[...] = acc_e
    pack_w[...] = acc_w

    any_west, any_east = (me_c + ncol - 1) // ncol, (2 * ncol - 2 - me_c) // ncol
    any_far = core * ((2 * nrow - 2 - me_r) // nrow) + (1 - core) * ((me_r + nrow - 1) // nrow)
    pl.semaphore_wait(barrier, len(near) + any_far * (1 + any_west + any_east))

    sends = []

    def send(src, dst, to, there, here):
        n = len(sends)
        copy = pltpu.make_async_remote_copy(
            src_ref=src, dst_ref=dst, send_sem=hs_sem.at[n], recv_sem=hr_sem.at[n],
            device_id=to, device_id_type=MESH,
        )
        when(*there)(copy.start)
        sends.append((copy, there, here))

    send(pack_e.at[high, :], from_w.at[nw_at, :], (down, east), (not_last, not_east), (not_first, not_west))
    send(pack_e.at[low, :], from_w.at[sw_at, :], (up, east), (not_first, not_east), (not_last, not_west))
    send(pack_w.at[high, :], from_e.at[nw_at, :], (down, west), (not_last, not_west), (not_first, not_east))
    send(pack_w.at[low, :], from_e.at[sw_at, :], (up, west), (not_first, not_west), (not_last, not_east))
    send(pack_e, from_w.at[pl.ds(0, pile), :], (me_r, east), (not_east,), (not_west,))
    send(pack_w, from_e.at[pl.ds(0, pile), :], (me_r, west), (not_west,), (not_east,))
    body = pl.ds(0, tiles)
    for f in (C, B, Q):
        send(f.at[body, pl.ds(TOP, HALO), :], f.at[body, pl.ds(END, HALO), :], (up, me_c), (not_first,), (not_last,))
        send(f.at[body, pl.ds(END - HALO, HALO), :], f.at[body, pl.ds(TOP - HALO, HALO), :], (down, me_c), (not_last,), (not_first,))

    first_ring = offsets((0,), (0,), around, around) + offsets(around, (0,), (0,), (0,))
    second_ring = offsets((-2, 2), (0,), (0,), (0,))
    for o in first_ring:
        tell(near_sem.at[0], at_offset(*o))

    fone, fnil = jnp.float32(1.0), jnp.float32(0.0)
    has_n, has_s = jnp.where(not_first, fone, fnil), jnp.where(not_last, fone, fnil)
    has_w, has_e = jnp.where(not_west, fone, fnil), jnp.where(not_east, fone, fnil)
    lane1 = lax.broadcasted_iota(jnp.int32, (1, LANE), 1)
    inside = jnp.where(lane1 < LANE // 2, has_e, has_w)

    def masks(n):
        l = lax.broadcasted_iota(jnp.int32, (n, LANE), 1)
        return l == LANE - 1, l == 0

    def to_east(vs, last):
        r = [pltpu.roll(v, LANE - 1, 1) for v in vs]
        return [jnp.where(last, r[(j + 1) % len(vs)], r[j]) for j in range(len(vs))]

    def to_west(vs, start):
        r = [pltpu.roll(v, 1, 1) for v in vs]
        return [jnp.where(start, r[(j - 1) % len(vs)], r[j]) for j in range(len(vs))]

    def rows_of(ref, r, n, count=ext):
        return [ref[j, pl.ds(r, n), :] for j in range(count)]

    def keep_in(vs, keep):
        if len(vs) == ext:
            vs = vs[:tiles] + [vs[tiles] * inside]
        return vs if keep is None else [v * keep for v in vs]

    def put(ref, r, n, vs):
        for j, v in enumerate(vs):
            ref[j, pl.ds(r, n), :] = v

    def add(accs, lists, weigh=None):
        out = []
        for acc, (p, q) in zip(accs, lists):
            total = None
            for j in range(tiles):
                t = p[j] * q[j]
                if weigh is not None and weigh[j] is not None:
                    t = t * weigh[j]
                total = t if total is None else total + t
            out.append(fold(acc, total))
        return tuple(out)

    def apply_from(vs, ref, r, n, center, we, ww, ws, wn, keep):
        count = len(vs)
        last, start = masks(n)
        ve, vw = to_east(vs, last), to_west(vs, start)
        vs_, vn = rows_of(ref, r + 1, n, count), rows_of(ref, r - 1, n, count)
        return keep_in(
            [
                center[j] * vs[j] - ((ws[j] * vs_[j] + wn[j] * vn[j]) + (we[j] * ve[j] + ww[j] * vw[j]))
                for j in range(count)
            ],
            keep,
        )

    def over_rows(step, accs):
        step(TOP - HALO, HALO, None, has_n)
        step(END, HALO, None, has_s)

        def loop(i, accs):
            return step(pl.multiple_of(TOP + i * step_rows, TOP), step_rows, accs, None)

        return lax.fori_loop(0, rows // step_rows, loop, accs)

    def weights_and_v1(r, n, count, keep):
        last, start = masks(n)
        c0 = rows_of(C, r, n, count)
        cs, cn = rows_of(C, r + 1, n, count), rows_of(C, r - 1, n, count)
        ce, cw = to_east(c0, last), to_west(c0, start)
        we = [c0[j] + ce[j] for j in range(count)]
        ww = [c0[j] + cw[j] for j in range(count)]
        ws = [c0[j] + cs[j] for j in range(count)]
        wn = [c0[j] + cn[j] for j in range(count)]
        center = [(ws[j] + wn[j]) + (we[j] + ww[j]) for j in range(count)]
        put(WE, r, n, we)
        put(WW, r, n, ww)
        put(WS, r, n, ws)
        put(CE, r, n, center)
        v1 = apply_from(rows_of(B, r, n, count), B, r, n, center, we, ww, ws, wn, keep)
        put(V1, r, n, v1)
        return v1

    def weights_of(r, n, count=ext):
        return rows_of(WE, r, n, count), rows_of(WW, r, n, count), rows_of(WS, r, n, count), rows_of(WS, r - 1, n, count)

    def second(r, n, count, keep):
        v1 = rows_of(V1, r, n, count)
        v2 = apply_from(v1, V1, r, n, rows_of(CE, r, n, count), *weights_of(r, n, count), keep)
        put(V2, r, n, v2)
        return v1, v2

    def face_terms(V, r, n, count, weigh=None):
        last, _ = masks(n)
        v = rows_of(V, r, n, count)
        ve = to_east(v, last)
        total = None
        for j in range(tiles):
            out = WE[j, pl.ds(r, n), :] * ve[j] + WS[j, pl.ds(r, n), :] * V[j, pl.ds(r + 1, n), :]
            t = v[j] * (CE[j, pl.ds(r, n), :] * v[j] - (out + out))
            if weigh is not None and weigh[j] is not None:
                t = t * weigh[j]
            total = t if total is None else total + t
        return total

    in_west = jnp.where(lane1 >= 6, jnp.ones((1, LANE), jnp.float32), jnp.zeros((1, LANE), jnp.float32))
    in_east = jnp.where(lane1 < LANE - 6, jnp.ones((1, LANE), jnp.float32), jnp.zeros((1, LANE), jnp.float32))
    weigh = [None] * tiles
    weigh[0] = in_west
    weigh[tiles - 1] = in_east if tiles > 1 else in_west * in_east
    INNER = 16
    part = (rows - 2 * INNER) // 4

    def over_center(step, accs):
        step(TOP + 8, 8, None)
        step(END - 16, 8, None)

        def loop(i, accs):
            return step(pl.multiple_of(TOP + INNER + i * part, 8), part, accs)

        return lax.fori_loop(0, 4, loop, accs)

    def center1(r, n, accs):
        v1 = weights_and_v1(r, n, tiles, None)
        if accs is None:
            return None
        return add(accs, ((rows_of(B, r, n, tiles), v1), (v1, v1), (rows_of(Q, r, n, tiles), v1)), weigh)

    def center2(r, n, accs):
        v1, v2 = second(r, n, tiles, None)
        if accs is None:
            return None
        return add(accs, ((v1, v2), (v2, v2), (rows_of(Q, r, n, tiles), v2)), weigh)

    def center3(i, acc):
        return fold(acc, face_terms(V2, pl.multiple_of(TOP + INNER + i * part, 8), part, tiles, weigh))

    nu1, nu2, s_q1 = over_center(center1, blank(3))
    nu3, nu4, s_q2 = over_center(center2, blank(3))
    nu5 = lax.fori_loop(0, 4, center3, zero)

    def own_columns(f, j, shift):
        acc = jnp.zeros((pile, LANE), jnp.float32)
        for k in range(parts):
            acc = jnp.where((lane >> 4) == k, pltpu.roll(f[j, pl.ds(TOP + pile * k, pile), :], (16 * k + shift) % LANE, 1), acc)
        return acc

    own_w = [own_columns(f, 0, 6) for f in (C, B, Q)]
    own_e = [own_columns(f, tiles - 1, 10 - LANE) for f in (C, B, Q)]

    for copy, _, here in sends[:10]:
        when(*here)(copy.wait_recv)

    pl.semaphore_wait(near_sem.at[0], len(first_ring))
    for o in second_ring:
        tell(near_sem.at[1], at_offset(*o))

    def unpack(at, src, k, n, fields):
        w, e = from_w[src, :], from_e[src, :]
        l = lax.broadcasted_iota(jnp.int32, (n, LANE), 1)
        none = jnp.zeros((n, LANE), jnp.float32)
        for f, o, s, wide in zip((C, B, Q)[:fields], (0, 6, 11), (122, 123, 125), (6, 5, 3)):
            rw = pltpu.roll(w, (s - 16 * k - o) % LANE, 1)
            re = pltpu.roll(e, (-16 * k - o) % LANE, 1)
            f[tiles, at, :] = jnp.where(l >= s, rw, jnp.where(l < wide, re, none))

    top_at, end_at = pl.ds(TOP - HALO, HALO), pl.ds(END, HALO)
    for k in range(parts):
        if pile * k < 32 or pile * (k + 1) > rows - 32:
            unpack(pl.ds(TOP + pile * k, pile), pl.ds(0, pile), k, pile, 2)
    unpack(top_at, nw_at, parts - 1, HALO, 2)
    unpack(end_at, sw_at, 0, HALO, 2)

    rows32 = lax.broadcasted_iota(jnp.int32, (32, LANE), 0)
    ones32 = jnp.ones((32, LANE), jnp.float32)
    tops = ((TOP - HALO, jnp.where(rows32 < HALO, has_n * ones32, ones32), HALO), (END - 24, jnp.where(rows32 >= 24, has_s * ones32, ones32), HALO))
    def own_16(vs, skip):
        return [v[skip : skip + 16, :] for v in vs]

    for r, keep, skip in tops:
        v1 = own_16(weights_and_v1(r, 32, ext, keep), skip)
        b, q = rows_of(B, r + skip, 16, tiles), rows_of(Q, r + skip, 16, tiles)
        nu1, nu2, s_q1 = add((nu1, nu2, s_q1), ((b, v1), (v1, v1), (q, v1)))
    for r, keep, skip in tops:
        v1, v2 = [own_16(v, skip) for v in second(r, 32, ext, keep)]
        q = rows_of(Q, r + skip, 16, tiles)
        nu3, nu4, s_q2 = add((nu3, nu4, s_q2), ((v1, v2), (v2, v2), (q, v2)))
    for r, keep, skip in tops:
        nu5 = fold(nu5, face_terms(V2, r + skip, 16, ext))

    def put_strip(ref, n, v):
        ref[n, pl.ds(8, pile), :] = v
        ref[n, pl.ds(7, 1), :] = pltpu.roll(v[pile - 1 :, :], 16, 1)
        ref[n, pl.ds(8 + pile, 1), :] = pltpu.roll(v[:1, :], LANE - 16, 1)

    def below_above(ref, n):
        return ref[n, pl.ds(9, pile), :], ref[n, pl.ds(7, pile), :]

    sides = ((own_w, from_w, (0, -5), slot < 6, has_w, 6), (own_e, from_e, (10, 4), slot >= 10, has_e, 4))
    row_at = lax.broadcasted_iota(jnp.int32, (pile, LANE), 0) + pile * (lane >> 4)
    for n, (own, come, shifts, outer, there, begin) in enumerate(sides):
        got = come[pl.ds(0, pile), :]
        keep = jnp.where(outer, there * jnp.ones((pile, LANE), jnp.float32), jnp.ones((pile, LANE), jnp.float32))
        middle = (row_at >= INNER) & (row_at < rows - INNER) & (slot >= begin) & (slot < begin + 6)
        mine = jnp.where(middle, jnp.ones((pile, LANE), jnp.float32), jnp.zeros((pile, LANE), jnp.float32))
        c, b = [jnp.where(outer, pltpu.roll(got, h % LANE, 1), o) for h, o in zip(shifts, own)]
        q = own[2] * mine
        put_strip(SC, n, c)
        put_strip(SB, n, b)
        c_s, c_n = below_above(SC, n)
        we, ww, ws, wn = c + pltpu.roll(c, LANE - 1, 1), c + pltpu.roll(c, 1, 1), c + c_s, c + c_n
        mid = (ws + wn) + (we + ww)

        def strip_apply(ref, v):
            put_strip(ref, n, v)
            v_s, v_n = below_above(ref, n)
            beside = we * pltpu.roll(v, LANE - 1, 1) + ww * pltpu.roll(v, 1, 1)
            return (mid * v - ((ws * v_s + wn * v_n) + beside)) * keep

        v1 = strip_apply(SB, b)
        v2 = strip_apply(S1, v1)
        put_strip(S2, n, v2)
        out = we * pltpu.roll(v2, LANE - 1, 1) + ws * S2[n, pl.ds(9, pile), :]
        m1, m2 = v1 * mine, v2 * mine
        nu1, nu2, nu3 = fold(nu1, b * m1), fold(nu2, v1 * m1), fold(nu3, v1 * m2)
        nu4, nu5 = fold(nu4, v2 * m2), fold(nu5, m2 * (mid * v2 - (out + out)))
        s_q1, s_q2 = fold(s_q1, q * v1), fold(s_q2, q * v2)

    lane8 = lax.broadcasted_iota(jnp.int32, (8, LANE), 1)

    def add_up(buf, count):
        terms = [buf[k] for k in range(count)]
        while len(terms) > 1:
            terms = [terms[k] + terms[k + 1] if k + 1 < len(terms) else terms[k] for k in range(0, len(terms), 2)]
        return terms[0]

    def start_sum(part, ga, gb, stage):
        slot = core * ncol + me_c
        ga[slot] = part
        out = []
        for d in sorted(range(ncol), key=lambda d: -min(d, ncol - d)):
            copy = pltpu.make_async_remote_copy(
                src_ref=ga.at[slot], dst_ref=ga.at[slot],
                send_sem=as_sem.at[stage, d], recv_sem=ar_sem.at[stage, core * ncol + d],
                device_id=(2 * z + 1, lax.rem(me_c + d, ncol)), device_id_type=MESH,
            )
            if d == 0:
                pl.when(core == 0)(copy.start)
            else:
                copy.start()
            out.append((d, copy))
        return out

    def arrival(buf, slot, sem):
        return pltpu.make_async_remote_copy(
            src_ref=buf.at[slot], dst_ref=buf.at[slot], send_sem=sem, recv_sem=sem,
            device_id=(far_row, me_c), device_id_type=MESH,
        )

    def finish_sum(out, ga, gb, stage):
        again = []
        for dz in sorted(range(nz), key=lambda d: -min(d, nz - d)):
            for to_core in (0, 1):
                if dz or to_core == 0:
                    again.append(
                        pltpu.make_async_remote_copy(
                            src_ref=gb.at[z], dst_ref=gb.at[z],
                            send_sem=as_sem.at[stage + 1, 2 * dz + to_core], recv_sem=ar_sem.at[stage + 1, dz],
                            device_id=(2 * lax.rem(z + dz, nz) + to_core, me_c), device_id_type=MESH,
                        )
                    )

        @pl.when(core == 1)
        def _():
            for n in range(2 * ncol):
                if n != ncol:
                    arrival(ga, 0, ar_sem.at[stage, n]).wait_recv()
            if stage == 0:
                pl.semaphore_wait(near_sem.at[1], len(second_ring))
            gb[z] = add_up(ga, 2 * ncol)
            for copy in again:
                copy.start()

        if stage == 0:
            pl.when(core == 0)(lambda: pl.semaphore_wait(near_sem.at[1], len(second_ring)))
        for d, copy in out:
            if d == 0:
                pl.when(core == 0)(copy.wait_send)
            else:
                copy.wait_send()
        for dz in range(nz):
            come = arrival(gb, 0, ar_sem.at[stage + 1, dz])
            if dz == 0:
                pl.when(core == 0)(come.wait_recv)
            else:
                come.wait_recv()
        return add_up(gb, nz), again

    def settle(again):
        @pl.when(core == 1)
        def _():
            for copy in again:
                copy.wait_send()

    def gather(accs):
        packed = jnp.zeros((8, LANE), jnp.float32)
        for k, acc in enumerate(accs):
            packed = jnp.where(lane8 == k, jnp.sum(acc, axis=1, keepdims=True), packed)
        return jnp.sum(packed, axis=0, keepdims=True)

    def spread(row, k):
        return jnp.broadcast_to(row[:, k : k + 1], (1, LANE))

    out1 = start_sum(gather((nu0, nu1, nu2, nu3, nu4, nu5, s_q, s_qb, s_q1, s_q2)), ga, gb, 0)

    for copy, _, here in sends[10:]:
        when(*here)(copy.wait_recv)
    for k in range(parts):
        unpack(pl.ds(TOP + pile * k, pile), pl.ds(0, pile), k, pile, 3)
    unpack(top_at, nw_at, parts - 1, HALO, 3)
    unpack(end_at, sw_at, 0, HALO, 3)

    def all1(r, n, accs, keep):
        weights_and_v1(r, n, ext, keep)
        return accs

    def all2(r, n, accs, keep):
        second(r, n, ext, keep)
        return accs

    def pass_q(r, n, accs, keep):
        put(LP, r, n, apply_from(rows_of(Q, r, n), Q, r, n, rows_of(CE, r, n), *weights_of(r, n), keep))
        return accs

    over_rows(all1, 0)
    over_rows(all2, 0)
    over_rows(pass_q, 0)

    for copy, there, _ in sends:
        when(*there)(copy.wait_send)
    sums, again1 = finish_sum(out1, ga, gb, 0)

    c0, c1, c2 = solve([spread(sums, k) for k in range(6)])
    t_q, t_qb, t_q1, t_q2 = [spread(sums, k) for k in range(6, 10)]

    def pass_x(r, n, accs, keep):
        b, v1, v2 = rows_of(B, r, n), rows_of(V1, r, n), rows_of(V2, r, n)
        value = [c0 * b[j] + (c1 * v1[j] + c2 * v2[j]) for j in range(ext)]
        put(X, r, n, value)
        if keep is None:
            for j in range(tiles):
                val_ref[pl.ds(pl.multiple_of(r - TOP, 8), n), pl.ds(j * LANE, LANE)] = value[j]
        return accs

    over_rows(pass_x, 0)

    def pass3(r, n, accs, keep):
        last, start = masks(n)
        x = rows_of(X, r, n)
        xe, xw = to_east(x, last), to_west(x, start)
        xs, xn = rows_of(X, r + 1, n), rows_of(X, r - 1, n)
        q, lp, center = rows_of(Q, r, n), rows_of(LP, r, n), rows_of(CE, r, n)
        u1, full = [], []
        for j in range(ext):
            dr, dc = xs[j] - xn[j], xe[j] - xw[j]
            g = (0.25 / (2.0 * 0.25) * SCALE) * (dr * dr + dc * dc)
            full.append(center[j] + g)
            u1.append(lp[j] + g * q[j])
        u1 = keep_in(u1, keep)
        put(CE, r, n, full)
        put(U1, r, n, u1)
        if accs is None:
            return None
        return add(accs, ((q, u1), (u1, u1)))

    mu1, mu2 = over_rows(pass3, blank(2))

    def pass4(r, n, accs, keep):
        u1 = rows_of(U1, r, n)
        u2 = apply_from(u1, U1, r, n, rows_of(CE, r, n), *weights_of(r, n), keep)
        put(U2, r, n, u2)
        return None if accs is None else add(accs, ((u1, u2), (u2, u2)))

    mu3, mu4 = over_rows(pass4, blank(2))

    def pass5(i, acc):
        return fold(acc, face_terms(U2, pl.multiple_of(TOP + i * step_rows, TOP), step_rows, ext))

    mu5 = lax.fori_loop(0, rows // step_rows, pass5, zero)


    out2 = start_sum(gather((mu0, mu1, mu2, mu3, mu4, mu5)), gc, gd, 2)
    erg_ref[...] = (t_qb - DISCOUNT * (c0 * t_qb + (c1 * t_q1 + c2 * t_q2))) / t_q
    settle(again1)
    sums, again2 = finish_sum(out2, gc, gd, 2)
    d0, d1, d2 = solve([spread(sums, k) for k in range(6)])

    def last_pass(i, carry):
        r = pl.multiple_of(i * step_rows, step_rows)
        at = pl.ds(TOP + r, step_rows)
        for j in range(tiles):
            den_ref[pl.ds(r, step_rows), pl.ds(j * LANE, LANE)] = d0 * Q[j, at, :] + (d1 * U1[j, at, :] + d2 * U2[j, at, :])
        return carry

    lax.fori_loop(0, rows // step_rows, last_pass, 0)
    settle(again2)


def store_kernel(val_ref, den_ref, val_hbm, den_hbm, sem):
    copies = [pltpu.make_async_copy(val_ref, val_hbm, sem.at[0]), pltpu.make_async_copy(den_ref, den_hbm, sem.at[1])]
    for copy in copies:
        copy.start()
    for copy in copies:
        copy.wait()


def solution(mesh):
    nrow, ncol = mesh.shape["row"], mesh.shape["col"]

    def body(running_cost, control_x, control_y, prior_density):
        rows, cols = running_cost.shape
        tiles = cols // LANE
        ext = tiles + 1
        pile = rows // 8
        big = pltpu.VMEM((ext, rows + 2 * TOP, LANE), jnp.float32)
        plain = pltpu.VMEM((tiles, rows, LANE), jnp.float32)
        most = max(nrow, ncol)
        value, density, ergodic = pl.pallas_call(
            functools.partial(kernel, nrow, ncol, 4 if ncol % 4 == 0 else 1, rows, tiles, min(rows, 64)),
            out_shape=(
                jax.ShapeDtypeStruct((rows, cols), jnp.float32),
                jax.ShapeDtypeStruct((rows, cols), jnp.float32),
                jax.ShapeDtypeStruct((1, LANE), jnp.float32),
            ),
            in_specs=[pl.BlockSpec(memory_space=pltpu.HBM)] * 4,
            out_specs=(pl.BlockSpec(memory_space=pltpu.VMEM),) * 3,
            scratch_shapes=[plain] * 3
            + [big] * 13
            + [pltpu.VMEM((pile, LANE), jnp.float32)] * 2
            + [pltpu.VMEM((pile + 16, LANE), jnp.float32)] * 2
            + [pltpu.VMEM((2, pile + 16, LANE), jnp.float32)] * 4
            + [pltpu.VMEM((2 * ncol, 1, LANE), jnp.float32), pltpu.VMEM((nrow // 2, 1, LANE), jnp.float32)] * 2
            + [
                pltpu.SemaphoreType.DMA((4, tiles)),
                pltpu.SemaphoreType.DMA((12,)),
                pltpu.SemaphoreType.DMA((12,)),
                pltpu.SemaphoreType.DMA((4, most)),
                pltpu.SemaphoreType.DMA((4, 2 * ncol)),
                pltpu.SemaphoreType.REGULAR((2,)),
            ],
            compiler_params=pltpu.CompilerParams(
                collective_id=0, has_side_effects=True, vmem_limit_bytes=55200000
            ),
        )(running_cost, control_x, control_y, prior_density)
        value, density = pl.pallas_call(
            store_kernel,
            out_shape=(jax.ShapeDtypeStruct((rows, cols), jnp.float32),) * 2,
            in_specs=[pl.BlockSpec(memory_space=pltpu.VMEM)] * 2,
            out_specs=(pl.BlockSpec(memory_space=pltpu.HBM),) * 2,
            scratch_shapes=[pltpu.SemaphoreType.DMA((2,))],
            compiler_params=pltpu.CompilerParams(vmem_limit_bytes=4 * 1024 * 1024),
        )(value, density)
        return value, density, ergodic[0, 0]

    spec = P("row", "col")
    return jax.shard_map(
        body,
        mesh=mesh,
        in_specs=(spec, spec, spec, spec),
        out_specs=(spec, spec, P()),
        check_vma=False,
    )
```

```python
import functools

import jax
import jax.numpy as jnp
from jax import lax
from jax.experimental import pallas as pl
from jax.experimental.pallas import tpu as pltpu
from jax.sharding import PartitionSpec as P

MESH = pl.DeviceIdType.MESH

SCALE = 1.0 / 64.0
FACE = 0.25 * 0.5 * SCALE
DISCOUNT = 0.05

LANE = 128
TOP = 16
HALO = 8


def solve(nu):
    shift = DISCOUNT * SCALE
    m = [nu[k + 1] + shift * nu[k] for k in range(5)]
    l1 = m[1] / m[0]
    l2 = m[2] / m[0]
    d1 = m[2] - l1 * m[1]
    e = m[3] - l2 * m[1]
    l3 = e / d1
    d2 = (m[4] - l2 * m[2]) - l3 * e
    y0 = nu[0]
    y1 = nu[1] - l1 * y0
    y2 = (nu[2] - l2 * y0) - l3 * y1
    c2 = y2 / d2
    c1 = y1 / d1 - l3 * c2
    c0 = y0 / m[0] - l1 * c1 - l2 * c2
    return c0 * SCALE, c1 * SCALE, c2 * SCALE


def kernel(
    nrow, ncol, nx, rows, tiles, step_rows,
    rc_hbm, cx_hbm, cy_hbm, pr_hbm,
    val_ref, den_ref, erg_ref,
    cx, cy, rc, C, B, Q, WE, WW, WS, CE, V1, V2, X, LP, U1, U2,
    pack_e, pack_w, from_w, from_e, SC, SB, S1, S2, ga, gb, gc, gd,
    in_sem, hs_sem, hr_sem, as_sem, ar_sem, near_sem,
):
    me_r = lax.axis_index("row")
    me_c = lax.axis_index("col")
    up, down = lax.rem(me_r + nrow - 1, nrow), lax.rem(me_r + 1, nrow)
    west, east = lax.rem(me_c + ncol - 1, ncol), lax.rem(me_c + 1, ncol)
    ext = tiles + 1
    END = TOP + rows

    def tile_of(ref, j):
        return ref.at[:, pl.ds(j * LANE, LANE)]

    loads = {}
    for n, (src, dst, top) in enumerate(((cx_hbm, cx, 0), (cy_hbm, cy, 0), (rc_hbm, rc, 0), (pr_hbm, Q, TOP))):
        for j in range(tiles):
            copy = pltpu.make_async_copy(tile_of(src, j), dst.at[j, pl.ds(top, rows), :], in_sem.at[n, j])
            copy.start()
            loads[n, j] = copy

    nz, ny = nrow // 2, ncol // nx
    core, z = lax.rem(me_r, 2), me_r // 2
    x, y = me_c // ny, lax.rem(me_c, ny)

    def at_offset(dz, dc, dx, dy):
        r = 2 * lax.rem(z + dz, nz) + lax.rem(core + dc, 2)
        return r, ny * lax.rem(x + dx, nx) + lax.rem(y + dy, ny)

    def offsets(zs, cs, xs, ys):
        every = {(a % nz, b, c % nx, d % ny) for a in zs for b in cs for c in xs for d in ys}
        return sorted(every - {(0, 0, 0, 0)})

    def tell(sem, to):
        pl.semaphore_signal(sem, inc=1, device_id=to, device_id_type=MESH)

    not_first, not_last = me_r > 0, me_r < nrow - 1
    not_west, not_east = me_c > 0, me_c < ncol - 1
    beyond = me_r + 2 * core - 1
    far_row = lax.rem(beyond + nrow, nrow)

    def when(*conditions):
        def run(fn):
            for c in conditions[::-1]:
                fn = functools.partial(lambda c, f: pl.when(c)(f) and None, c, fn)
            fn()
        return run

    far_there = (beyond >= 0, beyond < nrow)

    barrier = pltpu.get_barrier_semaphore()
    around = (-1, 0, 1)
    near = offsets((0,), (0, 1), around, around) + offsets(around, (0,), (0,), (0,))
    for o in near:
        tell(barrier, at_offset(*o))
    when(*far_there)(lambda: tell(barrier, (far_row, me_c)))
    when(*far_there, not_west)(lambda: tell(barrier, (far_row, west)))
    when(*far_there, not_east)(lambda: tell(barrier, (far_row, east)))

    zero = jnp.zeros((8, LANE), jnp.float32)
    for ref in (C, B, Q, WS, V1, V2, X, U1, U2):
        for j in range(ext):
            ref[j, pl.ds(0, 8), :] = zero
            ref[j, pl.ds(END + HALO, 8), :] = zero

    low, high = pl.ds(0, 8), pl.ds(rows // 8 - 8, 8)
    sw_at, nw_at = pl.ds(rows // 8, 8), pl.ds(rows // 8 + 8, 8)

    @pl.when(me_c == 0)
    def _():
        from_w[...] = jnp.zeros_like(from_w)

    @pl.when(me_c == ncol - 1)
    def _():
        from_e[...] = jnp.zeros_like(from_e)

    def no_row(top, corner):
        for f in (C, B, Q):
            for j in range(tiles):
                f[j, pl.ds(top, HALO), :] = zero
        from_w[corner, :] = zero
        from_e[corner, :] = zero

    @pl.when(me_r == 0)
    def _():
        no_row(TOP - HALO, nw_at)

    @pl.when(me_r == nrow - 1)
    def _():
        no_row(END, sw_at)

    for copy in loads.values():
        copy.wait()

    def fold(acc, v):
        while v.shape[0] > 8:
            n = v.shape[0]
            if n % 16 == 0:
                v = v[: n // 2, :] + v[n // 2 :, :]
            else:
                acc, v = acc + v[n - 8 :, :], v[: n - 8, :]
        return acc + v

    def blank(k):
        return tuple(zero for _ in range(k))

    def first(i, accs):
        r = pl.multiple_of(i * step_rows, step_rows)
        at = pl.ds(TOP + r, step_rows)
        terms = [None] * 4
        for j in range(tiles):
            a, b = cx[j, pl.ds(r, step_rows), :], cy[j, pl.ds(r, step_rows), :]
            cost = 0.5 * (a * a + b * b)
            force = rc[j, pl.ds(r, step_rows), :] + cost
            C[j, at, :] = (1.0 + cost) * FACE
            B[j, at, :] = force
            q = Q[j, at, :]
            for k, t in enumerate((force * force, q, q * force, q * q)):
                terms[k] = t if j == 0 else terms[k] + t
        return tuple(fold(acc, t) for acc, t in zip(accs, terms))

    nu0, s_q, s_qb, mu0 = lax.fori_loop(0, rows // step_rows, first, blank(4))

    parts = LANE // 16
    pile = rows // parts
    lane = lax.broadcasted_iota(jnp.int32, (pile, LANE), 1)
    slot = lane & 15
    is_c, is_b = slot < 6, slot < 11
    acc_e = jnp.zeros((pile, LANE), jnp.float32)
    acc_w = jnp.zeros((pile, LANE), jnp.float32)
    for k in range(parts):
        at = pl.ds(TOP + pile * k, pile)
        here = (lane >> 4) == k
        got = []
        for j, firsts in ((tiles - 1, (122, 123, 125)), (0, (0, 0, 0))):
            rolled = [
                pltpu.roll(f[j, at, :], (16 * k + o - s) % LANE, 1)
                for f, o, s in zip((C, B, Q), (0, 6, 11), firsts)
            ]
            got.append(jnp.where(is_c, rolled[0], jnp.where(is_b, rolled[1], rolled[2])))
        acc_e = jnp.where(here, got[0], acc_e)
        acc_w = jnp.where(here, got[1], acc_w)
    pack_e[...] = acc_e
    pack_w[...] = acc_w

    any_west, any_east = (me_c + ncol - 1) // ncol, (2 * ncol - 2 - me_c) // ncol
    any_far = core * ((2 * nrow - 2 - me_r) // nrow) + (1 - core) * ((me_r + nrow - 1) // nrow)
    pl.semaphore_wait(barrier, len(near) + any_far * (1 + any_west + any_east))

    sends = []

    def send(src, dst, to, there, here):
        n = len(sends)
        copy = pltpu.make_async_remote_copy(
            src_ref=src, dst_ref=dst, send_sem=hs_sem.at[n], recv_sem=hr_sem.at[n],
            device_id=to, device_id_type=MESH,
        )
        when(*there)(copy.start)
        sends.append((copy, there, here))

    send(pack_e.at[high, :], from_w.at[nw_at, :], (down, east), (not_last, not_east), (not_first, not_west))
    send(pack_e.at[low, :], from_w.at[sw_at, :], (up, east), (not_first, not_east), (not_last, not_west))
    send(pack_w.at[high, :], from_e.at[nw_at, :], (down, west), (not_last, not_west), (not_first, not_east))
    send(pack_w.at[low, :], from_e.at[sw_at, :], (up, west), (not_first, not_west), (not_last, not_east))
    send(pack_e, from_w.at[pl.ds(0, pile), :], (me_r, east), (not_east,), (not_west,))
    send(pack_w, from_e.at[pl.ds(0, pile), :], (me_r, west), (not_west,), (not_east,))
    body = pl.ds(0, tiles)
    for f in (C, B, Q):
        send(f.at[body, pl.ds(TOP, HALO), :], f.at[body, pl.ds(END, HALO), :], (up, me_c), (not_first,), (not_last,))
        send(f.at[body, pl.ds(END - HALO, HALO), :], f.at[body, pl.ds(TOP - HALO, HALO), :], (down, me_c), (not_last,), (not_first,))

    first_ring = offsets((0,), (0,), around, around) + offsets(around, (0,), (0,), (0,))
    second_ring = offsets((-2, 2), (0,), (0,), (0,))
    for o in first_ring:
        tell(near_sem.at[0], at_offset(*o))

    fone, fnil = jnp.float32(1.0), jnp.float32(0.0)
    has_n, has_s = jnp.where(not_first, fone, fnil), jnp.where(not_last, fone, fnil)
    has_w, has_e = jnp.where(not_west, fone, fnil), jnp.where(not_east, fone, fnil)
    lane1 = lax.broadcasted_iota(jnp.int32, (1, LANE), 1)
    inside = jnp.where(lane1 < LANE // 2, has_e, has_w)

    def masks(n):
        l = lax.broadcasted_iota(jnp.int32, (n, LANE), 1)
        return l == LANE - 1, l == 0

    def to_east(vs, last):
        r = [pltpu.roll(v, LANE - 1, 1) for v in vs]
        return [jnp.where(last, r[(j + 1) % len(vs)], r[j]) for j in range(len(vs))]

    def to_west(vs, start):
        r = [pltpu.roll(v, 1, 1) for v in vs]
        return [jnp.where(start, r[(j - 1) % len(vs)], r[j]) for j in range(len(vs))]

    def rows_of(ref, r, n, count=ext):
        return [ref[j, pl.ds(r, n), :] for j in range(count)]

    def keep_in(vs, keep):
        if len(vs) == ext:
            vs = vs[:tiles] + [vs[tiles] * inside]
        return vs if keep is None else [v * keep for v in vs]

    def put(ref, r, n, vs):
        for j, v in enumerate(vs):
            ref[j, pl.ds(r, n), :] = v

    def add(accs, lists, weigh=None):
        out = []
        for acc, (p, q) in zip(accs, lists):
            total = None
            for j in range(tiles):
                t = p[j] * q[j]
                if weigh is not None and weigh[j] is not None:
                    t = t * weigh[j]
                total = t if total is None else total + t
            out.append(fold(acc, total))
        return tuple(out)

    def apply_from(vs, ref, r, n, center, we, ww, ws, wn, keep):
        count = len(vs)
        last, start = masks(n)
        ve, vw = to_east(vs, last), to_west(vs, start)
        vs_, vn = rows_of(ref, r + 1, n, count), rows_of(ref, r - 1, n, count)
        return keep_in(
            [
                center[j] * vs[j] - ((ws[j] * vs_[j] + wn[j] * vn[j]) + (we[j] * ve[j] + ww[j] * vw[j]))
                for j in range(count)
            ],
            keep,
        )

    def over_rows(step, accs, above=True):
        if above:
            step(TOP - HALO, HALO, None, has_n)
        step(END, HALO, None, has_s)

        def loop(i, accs):
            return step(pl.multiple_of(TOP + i * step_rows, TOP), step_rows, accs, None)

        return lax.fori_loop(0, rows // step_rows, loop, accs)

    def weights_and_v1(r, n, count, keep):
        last, start = masks(n)
        c0 = rows_of(C, r, n, count)
        cs, cn = rows_of(C, r + 1, n, count), rows_of(C, r - 1, n, count)
        ce, cw = to_east(c0, last), to_west(c0, start)
        we = [c0[j] + ce[j] for j in range(count)]
        ww = [c0[j] + cw[j] for j in range(count)]
        ws = [c0[j] + cs[j] for j in range(count)]
        wn = [c0[j] + cn[j] for j in range(count)]
        center = [(ws[j] + wn[j]) + (we[j] + ww[j]) for j in range(count)]
        put(WE, r, n, we)
        put(WW, r, n, ww)
        put(WS, r, n, ws)
        put(CE, r, n, center)
        v1 = apply_from(rows_of(B, r, n, count), B, r, n, center, we, ww, ws, wn, keep)
        put(V1, r, n, v1)
        return v1

    def weights_of(r, n, count=ext):
        return rows_of(WE, r, n, count), rows_of(WW, r, n, count), rows_of(WS, r, n, count), rows_of(WS, r - 1, n, count)

    def second(r, n, count, keep):
        v1 = rows_of(V1, r, n, count)
        v2 = apply_from(v1, V1, r, n, rows_of(CE, r, n, count), *weights_of(r, n, count), keep)
        put(V2, r, n, v2)
        return v1, v2

    def face_terms(V, r, n, count, weigh=None):
        last, _ = masks(n)
        v = rows_of(V, r, n, count)
        ve = to_east(v, last)
        total = None
        for j in range(tiles):
            out = WE[j, pl.ds(r, n), :] * ve[j] + WS[j, pl.ds(r, n), :] * V[j, pl.ds(r + 1, n), :]
            t = v[j] * (CE[j, pl.ds(r, n), :] * v[j] - (out + out))
            if weigh is not None and weigh[j] is not None:
                t = t * weigh[j]
            total = t if total is None else total + t
        return total

    in_west = jnp.where(lane1 >= 6, jnp.ones((1, LANE), jnp.float32), jnp.zeros((1, LANE), jnp.float32))
    in_east = jnp.where(lane1 < LANE - 6, jnp.ones((1, LANE), jnp.float32), jnp.zeros((1, LANE), jnp.float32))
    weigh = [None] * tiles
    weigh[0] = in_west
    weigh[tiles - 1] = in_east if tiles > 1 else in_west * in_east
    INNER = 16
    pieces = 2
    part = (rows - 2 * INNER) // pieces

    def over_center(step, accs):
        step(TOP + 8, 8, None)
        step(END - 16, 8, None)

        def loop(i, accs):
            return step(pl.multiple_of(TOP + INNER + i * part, 8), part, accs)

        return lax.fori_loop(0, pieces, loop, accs)

    def center1(r, n, accs):
        v1 = weights_and_v1(r, n, tiles, None)
        if accs is None:
            return None
        return add(accs, ((rows_of(B, r, n, tiles), v1), (v1, v1), (rows_of(Q, r, n, tiles), v1)), weigh)

    def center2(r, n, accs):
        v1, v2 = second(r, n, tiles, None)
        if accs is None:
            return None
        return add(accs, ((v1, v2), (v2, v2), (rows_of(Q, r, n, tiles), v2)), weigh)

    def center3(i, acc):
        return fold(acc, face_terms(V2, pl.multiple_of(TOP + INNER + i * part, 8), part, tiles, weigh))

    nu1, nu2, s_q1 = over_center(center1, blank(3))
    nu3, nu4, s_q2 = over_center(center2, blank(3))
    nu5 = lax.fori_loop(0, pieces, center3, zero)

    def own_columns(f, j, shift):
        acc = jnp.zeros((pile, LANE), jnp.float32)
        for k in range(parts):
            acc = jnp.where((lane >> 4) == k, pltpu.roll(f[j, pl.ds(TOP + pile * k, pile), :], (16 * k + shift) % LANE, 1), acc)
        return acc

    own_w = [own_columns(f, 0, 6) for f in (C, B, Q)]
    own_e = [own_columns(f, tiles - 1, 10 - LANE) for f in (C, B, Q)]

    for copy, _, here in sends[:10]:
        when(*here)(copy.wait_recv)

    pl.semaphore_wait(near_sem.at[0], len(first_ring))
    for o in second_ring:
        tell(near_sem.at[1], at_offset(*o))

    def unpack(at, src, k, n, fields):
        w, e = from_w[src, :], from_e[src, :]
        l = lax.broadcasted_iota(jnp.int32, (n, LANE), 1)
        none = jnp.zeros((n, LANE), jnp.float32)
        for f, o, s, wide in zip((C, B, Q)[:fields], (0, 6, 11), (122, 123, 125), (6, 5, 3)):
            rw = pltpu.roll(w, (s - 16 * k - o) % LANE, 1)
            re = pltpu.roll(e, (-16 * k - o) % LANE, 1)
            f[tiles, at, :] = jnp.where(l >= s, rw, jnp.where(l < wide, re, none))

    top_at, end_at = pl.ds(TOP - HALO, HALO), pl.ds(END, HALO)
    for k in range(parts):
        if pile * k < 32 or pile * (k + 1) > rows - 32:
            unpack(pl.ds(TOP + pile * k, pile), pl.ds(0, pile), k, pile, 2)
    unpack(top_at, nw_at, parts - 1, HALO, 2)
    unpack(end_at, sw_at, 0, HALO, 2)

    rows32 = lax.broadcasted_iota(jnp.int32, (32, LANE), 0)
    ones32 = jnp.ones((32, LANE), jnp.float32)
    tops = ((TOP - HALO, jnp.where(rows32 < HALO, has_n * ones32, ones32), HALO), (END - 24, jnp.where(rows32 >= 24, has_s * ones32, ones32), HALO))
    def own_16(vs, skip):
        return [v[skip : skip + 16, :] for v in vs]

    for r, keep, skip in tops:
        v1 = own_16(weights_and_v1(r, 32, ext, keep), skip)
        b, q = rows_of(B, r + skip, 16, tiles), rows_of(Q, r + skip, 16, tiles)
        nu1, nu2, s_q1 = add((nu1, nu2, s_q1), ((b, v1), (v1, v1), (q, v1)))
    for r, keep, skip in tops:
        v1, v2 = [own_16(v, skip) for v in second(r, 32, ext, keep)]
        q = rows_of(Q, r + skip, 16, tiles)
        nu3, nu4, s_q2 = add((nu3, nu4, s_q2), ((v1, v2), (v2, v2), (q, v2)))
    for r, keep, skip in tops:
        nu5 = fold(nu5, face_terms(V2, r + skip, 16, ext))

    def put_strip(ref, n, v):
        ref[n, pl.ds(8, pile), :] = v
        ref[n, pl.ds(7, 1), :] = pltpu.roll(v[pile - 1 :, :], 16, 1)
        ref[n, pl.ds(8 + pile, 1), :] = pltpu.roll(v[:1, :], LANE - 16, 1)

    def below_above(ref, n):
        return ref[n, pl.ds(9, pile), :], ref[n, pl.ds(7, pile), :]

    sides = ((own_w, from_w, (0, -5), slot < 6, has_w, 6), (own_e, from_e, (10, 4), slot >= 10, has_e, 4))
    row_at = lax.broadcasted_iota(jnp.int32, (pile, LANE), 0) + pile * (lane >> 4)
    for n, (own, come, shifts, outer, there, begin) in enumerate(sides):
        got = come[pl.ds(0, pile), :]
        keep = jnp.where(outer, there * jnp.ones((pile, LANE), jnp.float32), jnp.ones((pile, LANE), jnp.float32))
        middle = (row_at >= INNER) & (row_at < rows - INNER) & (slot >= begin) & (slot < begin + 6)
        mine = jnp.where(middle, jnp.ones((pile, LANE), jnp.float32), jnp.zeros((pile, LANE), jnp.float32))
        c, b = [jnp.where(outer, pltpu.roll(got, h % LANE, 1), o) for h, o in zip(shifts, own)]
        q = own[2] * mine
        put_strip(SC, n, c)
        put_strip(SB, n, b)
        c_s, c_n = below_above(SC, n)
        we, ww, ws, wn = c + pltpu.roll(c, LANE - 1, 1), c + pltpu.roll(c, 1, 1), c + c_s, c + c_n
        mid = (ws + wn) + (we + ww)

        def strip_apply(ref, v):
            put_strip(ref, n, v)
            v_s, v_n = below_above(ref, n)
            beside = we * pltpu.roll(v, LANE - 1, 1) + ww * pltpu.roll(v, 1, 1)
            return (mid * v - ((ws * v_s + wn * v_n) + beside)) * keep

        v1 = strip_apply(SB, b)
        v2 = strip_apply(S1, v1)
        put_strip(S2, n, v2)
        out = we * pltpu.roll(v2, LANE - 1, 1) + ws * S2[n, pl.ds(9, pile), :]
        m1, m2 = v1 * mine, v2 * mine
        nu1, nu2, nu3 = fold(nu1, b * m1), fold(nu2, v1 * m1), fold(nu3, v1 * m2)
        nu4, nu5 = fold(nu4, v2 * m2), fold(nu5, m2 * (mid * v2 - (out + out)))
        s_q1, s_q2 = fold(s_q1, q * v1), fold(s_q2, q * v2)

    lane8 = lax.broadcasted_iota(jnp.int32, (8, LANE), 1)

    def add_up(buf, count):
        terms = [buf[k] for k in range(count)]
        while len(terms) > 1:
            terms = [terms[k] + terms[k + 1] if k + 1 < len(terms) else terms[k] for k in range(0, len(terms), 2)]
        return terms[0]

    def start_sum(part, ga, gb, stage):
        slot = core * ncol + me_c
        ga[slot] = part
        for d in sorted(range(ncol), key=lambda d: -min(d, ncol - d)):
            copy = pltpu.make_async_remote_copy(
                src_ref=ga.at[slot], dst_ref=ga.at[slot], send_sem=as_sem.at[stage], recv_sem=ar_sem.at[stage],
                device_id=(2 * z + 1, lax.rem(me_c + d, ncol)), device_id_type=MESH,
            )
            if d == 0:
                pl.when(core == 0)(copy.start)
            else:
                copy.start()

    def wait_bytes(buf, count, sem):
        some = buf.at[pl.ds(0, count)]
        pltpu.make_async_copy(some, some, sem).wait()

    def finish_sum(ga, gb, stage):
        @pl.when(core == 1)
        def _():
            wait_bytes(ga, 2 * ncol - 1, ar_sem.at[stage])
            if stage == 0:
                pl.semaphore_wait(near_sem.at[1], len(second_ring))
            gb[z] = add_up(ga, 2 * ncol)
            for dz in sorted(range(nz), key=lambda d: -min(d, nz - d)):
                for to_core in (0, 1):
                    if dz or to_core == 0:
                        pltpu.make_async_remote_copy(
                            src_ref=gb.at[z], dst_ref=gb.at[z],
                            send_sem=as_sem.at[stage + 1], recv_sem=ar_sem.at[stage + 1],
                            device_id=(2 * lax.rem(z + dz, nz) + to_core, me_c), device_id_type=MESH,
                        ).start()
            wait_bytes(ga, ncol - 1, as_sem.at[stage])
            wait_bytes(gb, nz - 1, ar_sem.at[stage + 1])

        @pl.when(core == 0)
        def _():
            if stage == 0:
                pl.semaphore_wait(near_sem.at[1], len(second_ring))
            wait_bytes(ga, ncol, as_sem.at[stage])
            wait_bytes(gb, nz, ar_sem.at[stage + 1])

        return add_up(gb, nz)

    def settle(stage):
        @pl.when(core == 1)
        def _():
            wait_bytes(ga, 2 * nz - 1, as_sem.at[stage])

    def gather(accs):
        packed = jnp.zeros((8, LANE), jnp.float32)
        for k, acc in enumerate(accs):
            packed = jnp.where(lane8 == k, jnp.sum(acc, axis=1, keepdims=True), packed)
        return jnp.sum(packed, axis=0, keepdims=True)

    def spread(row, k):
        return jnp.broadcast_to(row[:, k : k + 1], (1, LANE))

    start_sum(gather((nu0, nu1, nu2, nu3, nu4, nu5, s_q, s_qb, s_q1, s_q2)), ga, gb, 0)

    for copy, _, here in sends[10:]:
        when(*here)(copy.wait_recv)
    for k in range(parts):
        unpack(pl.ds(TOP + pile * k, pile), pl.ds(0, pile), k, pile, 3)
    unpack(top_at, nw_at, parts - 1, HALO, 3)
    unpack(end_at, sw_at, 0, HALO, 3)

    def all1(r, n, accs, keep):
        weights_and_v1(r, n, ext, keep)
        return accs

    def all2(r, n, accs, keep):
        second(r, n, ext, keep)
        return accs

    def pass_q(r, n, accs, keep):
        put(LP, r, n, apply_from(rows_of(Q, r, n), Q, r, n, rows_of(CE, r, n), *weights_of(r, n), keep))
        return accs

    over_rows(all1, 0)
    over_rows(all2, 0)
    over_rows(pass_q, 0)

    for copy, there, _ in sends:
        when(*there)(copy.wait_send)
    sums = finish_sum(ga, gb, 0)

    c0, c1, c2 = solve([spread(sums, k) for k in range(6)])
    t_q, t_qb, t_q1, t_q2 = [spread(sums, k) for k in range(6, 10)]

    def pass_x(r, n, accs, keep):
        b, v1, v2 = rows_of(B, r, n), rows_of(V1, r, n), rows_of(V2, r, n)
        value = [c0 * b[j] + (c1 * v1[j] + c2 * v2[j]) for j in range(ext)]
        put(X, r, n, value)
        if keep is None:
            for j in range(tiles):
                val_ref[pl.ds(pl.multiple_of(r - TOP, 8), n), pl.ds(j * LANE, LANE)] = value[j]
        return accs

    over_rows(pass_x, 0)

    def pass3(r, n, accs, keep):
        last, start = masks(n)
        x = rows_of(X, r, n)
        xe, xw = to_east(x, last), to_west(x, start)
        xs, xn = rows_of(X, r + 1, n), rows_of(X, r - 1, n)
        q, lp, center = rows_of(Q, r, n), rows_of(LP, r, n), rows_of(CE, r, n)
        u1, full = [], []
        for j in range(ext):
            dr, dc = xs[j] - xn[j], xe[j] - xw[j]
            g = (0.25 / (2.0 * 0.25) * SCALE) * (dr * dr + dc * dc)
            full.append(center[j] + g)
            u1.append(lp[j] + g * q[j])
        u1 = keep_in(u1, keep)
        put(CE, r, n, full)
        put(U1, r, n, u1)
        if accs is None:
            return None
        return add(accs, ((q, u1), (u1, u1)))

    mu1, mu2 = over_rows(pass3, blank(2))

    def pass4(r, n, accs, keep):
        u1 = rows_of(U1, r, n)
        u2 = apply_from(u1, U1, r, n, rows_of(CE, r, n), *weights_of(r, n), keep)
        put(U2, r, n, u2)
        return None if accs is None else add(accs, ((u1, u2), (u2, u2)))

    mu3, mu4 = over_rows(pass4, blank(2), False)

    def pass5(i, acc):
        return fold(acc, face_terms(U2, pl.multiple_of(TOP + i * step_rows, TOP), step_rows, ext))

    mu5 = lax.fori_loop(0, rows // step_rows, pass5, zero)


    start_sum(gather((mu0, mu1, mu2, mu3, mu4, mu5)), gc, gd, 2)
    erg_ref[...] = (t_qb - DISCOUNT * (c0 * t_qb + (c1 * t_q1 + c2 * t_q2))) / t_q
    settle(1)
    sums = finish_sum(gc, gd, 2)
    d0, d1, d2 = solve([spread(sums, k) for k in range(6)])

    def last_pass(i, carry):
        r = pl.multiple_of(i * step_rows, step_rows)
        at = pl.ds(TOP + r, step_rows)
        for j in range(tiles):
            den_ref[pl.ds(r, step_rows), pl.ds(j * LANE, LANE)] = d0 * Q[j, at, :] + (d1 * U1[j, at, :] + d2 * U2[j, at, :])
        return carry

    lax.fori_loop(0, rows // step_rows, last_pass, 0)
    settle(3)


def store_kernel(val_ref, den_ref, val_hbm, den_hbm, sem):
    copies = [pltpu.make_async_copy(val_ref, val_hbm, sem.at[0]), pltpu.make_async_copy(den_ref, den_hbm, sem.at[1])]
    for copy in copies:
        copy.start()
    for copy in copies:
        copy.wait()


def solution(mesh):
    nrow, ncol = mesh.shape["row"], mesh.shape["col"]

    def body(running_cost, control_x, control_y, prior_density):
        rows, cols = running_cost.shape
        tiles = cols // LANE
        ext = tiles + 1
        pile = rows // 8
        big = pltpu.VMEM((ext, rows + 2 * TOP, LANE), jnp.float32)
        plain = pltpu.VMEM((tiles, rows, LANE), jnp.float32)
        value, density, ergodic = pl.pallas_call(
            functools.partial(kernel, nrow, ncol, 4 if ncol % 4 == 0 else 1, rows, tiles, min(rows, 128)),
            out_shape=(
                jax.ShapeDtypeStruct((rows, cols), jnp.float32),
                jax.ShapeDtypeStruct((rows, cols), jnp.float32),
                jax.ShapeDtypeStruct((1, LANE), jnp.float32),
            ),
            in_specs=[pl.BlockSpec(memory_space=pltpu.HBM)] * 4,
            out_specs=(pl.BlockSpec(memory_space=pltpu.VMEM),) * 3,
            scratch_shapes=[plain] * 3
            + [big] * 13
            + [pltpu.VMEM((pile, LANE), jnp.float32)] * 2
            + [pltpu.VMEM((pile + 16, LANE), jnp.float32)] * 2
            + [pltpu.VMEM((2, pile + 16, LANE), jnp.float32)] * 4
            + [pltpu.VMEM((2 * ncol, 1, LANE), jnp.float32), pltpu.VMEM((nrow // 2, 1, LANE), jnp.float32)] * 2
            + [
                pltpu.SemaphoreType.DMA((4, tiles)),
                pltpu.SemaphoreType.DMA((12,)),
                pltpu.SemaphoreType.DMA((12,)),
                pltpu.SemaphoreType.DMA((4,)),
                pltpu.SemaphoreType.DMA((4,)),
                pltpu.SemaphoreType.REGULAR((2,)),
            ],
            compiler_params=pltpu.CompilerParams(
                collective_id=0, has_side_effects=True, vmem_limit_bytes=55200000
            ),
        )(running_cost, control_x, control_y, prior_density)
        value, density = pl.pallas_call(
            store_kernel,
            out_shape=(jax.ShapeDtypeStruct((rows, cols), jnp.float32),) * 2,
            in_specs=[pl.BlockSpec(memory_space=pltpu.VMEM)] * 2,
            out_specs=(pl.BlockSpec(memory_space=pltpu.HBM),) * 2,
            scratch_shapes=[pltpu.SemaphoreType.DMA((2,))],
            compiler_params=pltpu.CompilerParams(vmem_limit_bytes=4 * 1024 * 1024),
        )(value, density)
        return value, density, ergodic[0, 0]

    spec = P("row", "col")
    return jax.shard_map(
        body,
        mesh=mesh,
        in_specs=(spec, spec, spec, spec),
        out_specs=(spec, spec, P()),
        check_vma=False,
    )
```

```python
import functools

import jax
import jax.numpy as jnp
from jax import lax
from jax.experimental import pallas as pl
from jax.experimental.pallas import tpu as pltpu
from jax.sharding import PartitionSpec as P

MESH = pl.DeviceIdType.MESH

SCALE = 1.0 / 64.0
FACE = 0.25 * 0.5 * SCALE
DISCOUNT = 0.05

LANE = 128
TOP = 16
HALO = 8


def solve(nu):
    shift = DISCOUNT * SCALE
    m = [nu[k + 1] + shift * nu[k] for k in range(5)]
    l1 = m[1] / m[0]
    l2 = m[2] / m[0]
    d1 = m[2] - l1 * m[1]
    e = m[3] - l2 * m[1]
    l3 = e / d1
    d2 = (m[4] - l2 * m[2]) - l3 * e
    y0 = nu[0]
    y1 = nu[1] - l1 * y0
    y2 = (nu[2] - l2 * y0) - l3 * y1
    c2 = y2 / d2
    c1 = y1 / d1 - l3 * c2
    c0 = y0 / m[0] - l1 * c1 - l2 * c2
    return c0 * SCALE, c1 * SCALE, c2 * SCALE


def kernel(
    nrow, ncol, nx, rows, tiles, step_rows,
    rc_hbm, cx_hbm, cy_hbm, pr_hbm,
    val_ref, den_ref, erg_ref,
    cx, cy, rc, C, B, Q, WE, WW, WS, CE, V1, V2, X, LP, U1, U2,
    pack_e, pack_w, from_w, from_e, SC, SB, S1, S2, ga, gb, gc, gd,
    in_sem, hs_sem, hr_sem, as_sem, ar_sem, near_sem,
):
    me_r = lax.axis_index("row")
    me_c = lax.axis_index("col")
    up, down = lax.rem(me_r + nrow - 1, nrow), lax.rem(me_r + 1, nrow)
    west, east = lax.rem(me_c + ncol - 1, ncol), lax.rem(me_c + 1, ncol)
    ext = tiles + 1
    END = TOP + rows

    def tile_of(ref, j):
        return ref.at[:, pl.ds(j * LANE, LANE)]

    loads = {}
    outer_tiles = tuple(sorted({0, tiles - 1}))
    inner_tiles = tuple(range(1, tiles - 1))
    fields = ((cx_hbm, cx, 0), (cy_hbm, cy, 0), (rc_hbm, rc, 0), (pr_hbm, Q, TOP))
    for n, (src, dst, top), js in [(n, f, js) for js in (outer_tiles, inner_tiles) for n, f in enumerate(fields)]:
        for j in js:
            copy = pltpu.make_async_copy(tile_of(src, j), dst.at[j, pl.ds(top, rows), :], in_sem.at[n, j])
            copy.start()
            loads[n, j] = copy

    nz, ny = nrow // 2, ncol // nx
    core, z = lax.rem(me_r, 2), me_r // 2
    x, y = me_c // ny, lax.rem(me_c, ny)

    def at_offset(dz, dc, dx, dy):
        r = 2 * lax.rem(z + dz, nz) + lax.rem(core + dc, 2)
        return r, ny * lax.rem(x + dx, nx) + lax.rem(y + dy, ny)

    def offsets(zs, cs, xs, ys):
        every = {(a % nz, b, c % nx, d % ny) for a in zs for b in cs for c in xs for d in ys}
        return sorted(every - {(0, 0, 0, 0)})

    def tell(sem, to):
        pl.semaphore_signal(sem, inc=1, device_id=to, device_id_type=MESH)

    not_first, not_last = me_r > 0, me_r < nrow - 1
    not_west, not_east = me_c > 0, me_c < ncol - 1
    beyond = me_r + 2 * core - 1
    far_row = lax.rem(beyond + nrow, nrow)

    def when(*conditions):
        def run(fn):
            for c in conditions[::-1]:
                fn = functools.partial(lambda c, f: pl.when(c)(f) and None, c, fn)
            fn()
        return run

    far_there = (beyond >= 0, beyond < nrow)

    barrier = pltpu.get_barrier_semaphore()
    around = (-1, 0, 1)
    near = offsets((0,), (0, 1), around, around) + offsets(around, (0,), (0,), (0,))
    for o in near:
        tell(barrier, at_offset(*o))
    when(*far_there)(lambda: tell(barrier, (far_row, me_c)))
    when(*far_there, not_west)(lambda: tell(barrier, (far_row, west)))
    when(*far_there, not_east)(lambda: tell(barrier, (far_row, east)))

    zero = jnp.zeros((8, LANE), jnp.float32)
    for ref in (C, B, Q, WS, V1, V2, X, U1, U2):
        for j in range(ext):
            ref[j, pl.ds(0, 8), :] = zero
            ref[j, pl.ds(END + HALO, 8), :] = zero

    low, high = pl.ds(0, 8), pl.ds(rows // 8 - 8, 8)
    sw_at, nw_at = pl.ds(rows // 8, 8), pl.ds(rows // 8 + 8, 8)

    @pl.when(me_c == 0)
    def _():
        from_w[...] = jnp.zeros_like(from_w)

    @pl.when(me_c == ncol - 1)
    def _():
        from_e[...] = jnp.zeros_like(from_e)

    def no_row(top, corner):
        for f in (C, B, Q):
            for j in range(tiles):
                f[j, pl.ds(top, HALO), :] = zero
        from_w[corner, :] = zero
        from_e[corner, :] = zero

    @pl.when(me_r == 0)
    def _():
        no_row(TOP - HALO, nw_at)

    @pl.when(me_r == nrow - 1)
    def _():
        no_row(END, sw_at)

    def fold(acc, v):
        while v.shape[0] > 8:
            n = v.shape[0]
            if n % 16 == 0:
                v = v[: n // 2, :] + v[n // 2 :, :]
            else:
                acc, v = acc + v[n - 8 :, :], v[: n - 8, :]
        return acc + v

    def blank(k):
        return tuple(zero for _ in range(k))

    def prepare(js, accs):
        for n in range(len(fields)):
            for j in js:
                loads[n, j].wait()

        def first(i, accs):
            r = pl.multiple_of(i * step_rows, step_rows)
            at = pl.ds(TOP + r, step_rows)
            terms = [None] * 4
            for j in js:
                a, b = cx[j, pl.ds(r, step_rows), :], cy[j, pl.ds(r, step_rows), :]
                cost = 0.5 * (a * a + b * b)
                force = rc[j, pl.ds(r, step_rows), :] + cost
                C[j, at, :] = (1.0 + cost) * FACE
                B[j, at, :] = force
                q = Q[j, at, :]
                for k, t in enumerate((force * force, q, q * force, q * q)):
                    terms[k] = t if terms[k] is None else terms[k] + t
            return tuple(fold(acc, t) for acc, t in zip(accs, terms))

        return lax.fori_loop(0, rows // step_rows, first, accs)

    sums0 = prepare(outer_tiles, blank(4))

    parts = LANE // 16
    pile = rows // parts
    lane = lax.broadcasted_iota(jnp.int32, (pile, LANE), 1)
    slot = lane & 15
    is_c, is_b = slot < 6, slot < 11
    acc_e = jnp.zeros((pile, LANE), jnp.float32)
    acc_w = jnp.zeros((pile, LANE), jnp.float32)
    for k in range(parts):
        at = pl.ds(TOP + pile * k, pile)
        here = (lane >> 4) == k
        got = []
        for j, firsts in ((tiles - 1, (122, 123, 125)), (0, (0, 0, 0))):
            rolled = [
                pltpu.roll(f[j, at, :], (16 * k + o - s) % LANE, 1)
                for f, o, s in zip((C, B, Q), (0, 6, 11), firsts)
            ]
            got.append(jnp.where(is_c, rolled[0], jnp.where(is_b, rolled[1], rolled[2])))
        acc_e = jnp.where(here, got[0], acc_e)
        acc_w = jnp.where(here, got[1], acc_w)
    pack_e[...] = acc_e
    pack_w[...] = acc_w

    any_west, any_east = (me_c + ncol - 1) // ncol, (2 * ncol - 2 - me_c) // ncol
    any_far = core * ((2 * nrow - 2 - me_r) // nrow) + (1 - core) * ((me_r + nrow - 1) // nrow)
    pl.semaphore_wait(barrier, len(near) + any_far * (1 + any_west + any_east))

    sends = []

    def send(src, dst, to, there, here):
        n = len(sends)
        copy = pltpu.make_async_remote_copy(
            src_ref=src, dst_ref=dst, send_sem=hs_sem.at[n], recv_sem=hr_sem.at[n],
            device_id=to, device_id_type=MESH,
        )
        when(*there)(copy.start)
        sends.append((copy, there, here))

    send(pack_e.at[high, :], from_w.at[nw_at, :], (down, east), (not_last, not_east), (not_first, not_west))
    send(pack_e.at[low, :], from_w.at[sw_at, :], (up, east), (not_first, not_east), (not_last, not_west))
    send(pack_w.at[high, :], from_e.at[nw_at, :], (down, west), (not_last, not_west), (not_first, not_east))
    send(pack_w.at[low, :], from_e.at[sw_at, :], (up, west), (not_first, not_west), (not_last, not_east))
    send(pack_e, from_w.at[pl.ds(0, pile), :], (me_r, east), (not_east,), (not_west,))
    send(pack_w, from_e.at[pl.ds(0, pile), :], (me_r, west), (not_west,), (not_east,))
    if inner_tiles:
        sums0 = prepare(inner_tiles, sums0)
    nu0, s_q, s_qb, mu0 = sums0

    body = pl.ds(0, tiles)
    for f in (C, B, Q):
        send(f.at[body, pl.ds(TOP, HALO), :], f.at[body, pl.ds(END, HALO), :], (up, me_c), (not_first,), (not_last,))
        send(f.at[body, pl.ds(END - HALO, HALO), :], f.at[body, pl.ds(TOP - HALO, HALO), :], (down, me_c), (not_last,), (not_first,))

    first_ring = offsets((0,), (0,), around, around) + offsets(around, (0,), (0,), (0,))
    second_ring = offsets((-2, 2), (0,), (0,), (0,))
    for o in first_ring:
        tell(near_sem.at[0], at_offset(*o))

    fone, fnil = jnp.float32(1.0), jnp.float32(0.0)
    has_n, has_s = jnp.where(not_first, fone, fnil), jnp.where(not_last, fone, fnil)
    has_w, has_e = jnp.where(not_west, fone, fnil), jnp.where(not_east, fone, fnil)
    lane1 = lax.broadcasted_iota(jnp.int32, (1, LANE), 1)
    inside = jnp.where(lane1 < LANE // 2, has_e, has_w)

    def masks(n):
        l = lax.broadcasted_iota(jnp.int32, (n, LANE), 1)
        return l == LANE - 1, l == 0

    def to_east(vs, last):
        r = [pltpu.roll(v, LANE - 1, 1) for v in vs]
        return [jnp.where(last, r[(j + 1) % len(vs)], r[j]) for j in range(len(vs))]

    def to_west(vs, start):
        r = [pltpu.roll(v, 1, 1) for v in vs]
        return [jnp.where(start, r[(j - 1) % len(vs)], r[j]) for j in range(len(vs))]

    def rows_of(ref, r, n, count=ext):
        return [ref[j, pl.ds(r, n), :] for j in range(count)]

    def keep_in(vs, keep):
        if len(vs) == ext:
            vs = vs[:tiles] + [vs[tiles] * inside]
        return vs if keep is None else [v * keep for v in vs]

    def put(ref, r, n, vs):
        for j, v in enumerate(vs):
            ref[j, pl.ds(r, n), :] = v

    def add(accs, lists, weigh=None):
        out = []
        for acc, (p, q) in zip(accs, lists):
            total = None
            for j in range(tiles):
                t = p[j] * q[j]
                if weigh is not None and weigh[j] is not None:
                    t = t * weigh[j]
                total = t if total is None else total + t
            out.append(fold(acc, total))
        return tuple(out)

    def apply_from(vs, ref, r, n, center, we, ww, ws, wn, keep):
        count = len(vs)
        last, start = masks(n)
        ve, vw = to_east(vs, last), to_west(vs, start)
        vs_, vn = rows_of(ref, r + 1, n, count), rows_of(ref, r - 1, n, count)
        return keep_in(
            [
                center[j] * vs[j] - ((ws[j] * vs_[j] + wn[j] * vn[j]) + (we[j] * ve[j] + ww[j] * vw[j]))
                for j in range(count)
            ],
            keep,
        )

    def over_rows(step, accs, above=True, unrolled=False):
        if above:
            step(TOP - HALO, HALO, None, has_n)
        step(END, HALO, None, has_s)

        def loop(i, accs):
            return step(pl.multiple_of(TOP + i * step_rows, TOP), step_rows, accs, None)

        if unrolled:
            for i in range(rows // step_rows):
                accs = step(TOP + i * step_rows, step_rows, accs, None)
            return accs
        return lax.fori_loop(0, rows // step_rows, loop, accs)

    def weights_and_v1(r, n, count, keep):
        last, start = masks(n)
        c0 = rows_of(C, r, n, count)
        cs, cn = rows_of(C, r + 1, n, count), rows_of(C, r - 1, n, count)
        ce, cw = to_east(c0, last), to_west(c0, start)
        we = [c0[j] + ce[j] for j in range(count)]
        ww = [c0[j] + cw[j] for j in range(count)]
        ws = [c0[j] + cs[j] for j in range(count)]
        wn = [c0[j] + cn[j] for j in range(count)]
        center = [(ws[j] + wn[j]) + (we[j] + ww[j]) for j in range(count)]
        put(WE, r, n, we)
        put(WW, r, n, ww)
        put(WS, r, n, ws)
        put(CE, r, n, center)
        v1 = apply_from(rows_of(B, r, n, count), B, r, n, center, we, ww, ws, wn, keep)
        put(V1, r, n, v1)
        return v1

    def weights_of(r, n, count=ext):
        return rows_of(WE, r, n, count), rows_of(WW, r, n, count), rows_of(WS, r, n, count), rows_of(WS, r - 1, n, count)

    def second(r, n, count, keep):
        v1 = rows_of(V1, r, n, count)
        v2 = apply_from(v1, V1, r, n, rows_of(CE, r, n, count), *weights_of(r, n, count), keep)
        put(V2, r, n, v2)
        return v1, v2

    def face_terms(V, r, n, count, weigh=None):
        last, _ = masks(n)
        v = rows_of(V, r, n, count)
        ve = to_east(v, last)
        total = None
        for j in range(tiles):
            out = WE[j, pl.ds(r, n), :] * ve[j] + WS[j, pl.ds(r, n), :] * V[j, pl.ds(r + 1, n), :]
            t = v[j] * (CE[j, pl.ds(r, n), :] * v[j] - (out + out))
            if weigh is not None and weigh[j] is not None:
                t = t * weigh[j]
            total = t if total is None else total + t
        return total

    in_west = jnp.where(lane1 >= 6, jnp.ones((1, LANE), jnp.float32), jnp.zeros((1, LANE), jnp.float32))
    in_east = jnp.where(lane1 < LANE - 6, jnp.ones((1, LANE), jnp.float32), jnp.zeros((1, LANE), jnp.float32))
    weigh = [None] * tiles
    weigh[0] = in_west
    weigh[tiles - 1] = in_east if tiles > 1 else in_west * in_east
    INNER = 16
    pieces = 2
    part = (rows - 2 * INNER) // pieces

    def over_center(step, accs):
        step(TOP + 8, 8, None)
        step(END - 16, 8, None)

        def loop(i, accs):
            return step(pl.multiple_of(TOP + INNER + i * part, 8), part, accs)

        return lax.fori_loop(0, pieces, loop, accs)

    def center1(r, n, accs):
        v1 = weights_and_v1(r, n, tiles, None)
        if accs is None:
            return None
        return add(accs, ((rows_of(B, r, n, tiles), v1), (v1, v1), (rows_of(Q, r, n, tiles), v1)), weigh)

    def center2(r, n, accs):
        v1, v2 = second(r, n, tiles, None)
        if accs is None:
            return None
        return add(accs, ((v1, v2), (v2, v2), (rows_of(Q, r, n, tiles), v2)), weigh)

    def center3(i, acc):
        return fold(acc, face_terms(V2, pl.multiple_of(TOP + INNER + i * part, 8), part, tiles, weigh))

    nu1, nu2, s_q1 = over_center(center1, blank(3))
    nu3, nu4, s_q2 = over_center(center2, blank(3))
    nu5 = lax.fori_loop(0, pieces, center3, zero)

    def own_columns(f, j, shift):
        acc = jnp.zeros((pile, LANE), jnp.float32)
        for k in range(parts):
            acc = jnp.where((lane >> 4) == k, pltpu.roll(f[j, pl.ds(TOP + pile * k, pile), :], (16 * k + shift) % LANE, 1), acc)
        return acc

    own_w = [own_columns(f, 0, 6) for f in (C, B, Q)]
    own_e = [own_columns(f, tiles - 1, 10 - LANE) for f in (C, B, Q)]

    for copy, _, here in sends[:10]:
        when(*here)(copy.wait_recv)

    pl.semaphore_wait(near_sem.at[0], len(first_ring))
    for o in second_ring:
        tell(near_sem.at[1], at_offset(*o))

    def unpack(at, src, k, n, fields):
        w, e = from_w[src, :], from_e[src, :]
        l = lax.broadcasted_iota(jnp.int32, (n, LANE), 1)
        none = jnp.zeros((n, LANE), jnp.float32)
        for f, o, s, wide in zip((C, B, Q)[:fields], (0, 6, 11), (122, 123, 125), (6, 5, 3)):
            rw = pltpu.roll(w, (s - 16 * k - o) % LANE, 1)
            re = pltpu.roll(e, (-16 * k - o) % LANE, 1)
            f[tiles, at, :] = jnp.where(l >= s, rw, jnp.where(l < wide, re, none))

    top_at, end_at = pl.ds(TOP - HALO, HALO), pl.ds(END, HALO)
    for k in range(parts):
        if pile * k < 32 or pile * (k + 1) > rows - 32:
            unpack(pl.ds(TOP + pile * k, pile), pl.ds(0, pile), k, pile, 2)
    unpack(top_at, nw_at, parts - 1, HALO, 2)
    unpack(end_at, sw_at, 0, HALO, 2)

    rows32 = lax.broadcasted_iota(jnp.int32, (32, LANE), 0)
    ones32 = jnp.ones((32, LANE), jnp.float32)
    tops = ((TOP - HALO, jnp.where(rows32 < HALO, has_n * ones32, ones32), HALO), (END - 24, jnp.where(rows32 >= 24, has_s * ones32, ones32), HALO))
    def own_16(vs, skip):
        return [v[skip : skip + 16, :] for v in vs]

    for r, keep, skip in tops:
        v1 = own_16(weights_and_v1(r, 32, ext, keep), skip)
        b, q = rows_of(B, r + skip, 16, tiles), rows_of(Q, r + skip, 16, tiles)
        nu1, nu2, s_q1 = add((nu1, nu2, s_q1), ((b, v1), (v1, v1), (q, v1)))
    for r, keep, skip in tops:
        v1, v2 = [own_16(v, skip) for v in second(r, 32, ext, keep)]
        q = rows_of(Q, r + skip, 16, tiles)
        nu3, nu4, s_q2 = add((nu3, nu4, s_q2), ((v1, v2), (v2, v2), (q, v2)))
    for r, keep, skip in tops:
        nu5 = fold(nu5, face_terms(V2, r + skip, 16, ext))

    def put_strip(ref, n, v):
        ref[n, pl.ds(8, pile), :] = v
        ref[n, pl.ds(7, 1), :] = pltpu.roll(v[pile - 1 :, :], 16, 1)
        ref[n, pl.ds(8 + pile, 1), :] = pltpu.roll(v[:1, :], LANE - 16, 1)

    def below_above(ref, n):
        return ref[n, pl.ds(9, pile), :], ref[n, pl.ds(7, pile), :]

    sides = ((own_w, from_w, (0, -5), slot < 6, has_w, 6), (own_e, from_e, (10, 4), slot >= 10, has_e, 4))
    row_at = lax.broadcasted_iota(jnp.int32, (pile, LANE), 0) + pile * (lane >> 4)
    for n, (own, come, shifts, outer, there, begin) in enumerate(sides):
        got = come[pl.ds(0, pile), :]
        keep = jnp.where(outer, there * jnp.ones((pile, LANE), jnp.float32), jnp.ones((pile, LANE), jnp.float32))
        middle = (row_at >= INNER) & (row_at < rows - INNER) & (slot >= begin) & (slot < begin + 6)
        mine = jnp.where(middle, jnp.ones((pile, LANE), jnp.float32), jnp.zeros((pile, LANE), jnp.float32))
        c, b = [jnp.where(outer, pltpu.roll(got, h % LANE, 1), o) for h, o in zip(shifts, own)]
        q = own[2] * mine
        put_strip(SC, n, c)
        put_strip(SB, n, b)
        c_s, c_n = below_above(SC, n)
        we, ww, ws, wn = c + pltpu.roll(c, LANE - 1, 1), c + pltpu.roll(c, 1, 1), c + c_s, c + c_n
        mid = (ws + wn) + (we + ww)

        def strip_apply(ref, v):
            put_strip(ref, n, v)
            v_s, v_n = below_above(ref, n)
            beside = we * pltpu.roll(v, LANE - 1, 1) + ww * pltpu.roll(v, 1, 1)
            return (mid * v - ((ws * v_s + wn * v_n) + beside)) * keep

        v1 = strip_apply(SB, b)
        v2 = strip_apply(S1, v1)
        put_strip(S2, n, v2)
        out = we * pltpu.roll(v2, LANE - 1, 1) + ws * S2[n, pl.ds(9, pile), :]
        m1, m2 = v1 * mine, v2 * mine
        nu1, nu2, nu3 = fold(nu1, b * m1), fold(nu2, v1 * m1), fold(nu3, v1 * m2)
        nu4, nu5 = fold(nu4, v2 * m2), fold(nu5, m2 * (mid * v2 - (out + out)))
        s_q1, s_q2 = fold(s_q1, q * v1), fold(s_q2, q * v2)

    lane8 = lax.broadcasted_iota(jnp.int32, (8, LANE), 1)

    def add_up(buf, count):
        terms = [buf[k] for k in range(count)]
        while len(terms) > 1:
            terms = [terms[k] + terms[k + 1] if k + 1 < len(terms) else terms[k] for k in range(0, len(terms), 2)]
        return terms[0]

    def start_sum(part, ga, gb, stage):
        slot = core * ncol + me_c
        ga[slot] = part
        for d in sorted(range(ncol), key=lambda d: -min(d, ncol - d)):
            copy = pltpu.make_async_remote_copy(
                src_ref=ga.at[slot], dst_ref=ga.at[slot], send_sem=as_sem.at[stage], recv_sem=ar_sem.at[stage],
                device_id=(2 * z + 1, lax.rem(me_c + d, ncol)), device_id_type=MESH,
            )
            if d == 0:
                pl.when(core == 0)(copy.start)
            else:
                copy.start()

    def wait_bytes(buf, count, sem):
        some = buf.at[pl.ds(0, count)]
        pltpu.make_async_copy(some, some, sem).wait()

    def finish_sum(ga, gb, stage):
        @pl.when(core == 1)
        def _():
            wait_bytes(ga, 2 * ncol - 1, ar_sem.at[stage])
            if stage == 0:
                pl.semaphore_wait(near_sem.at[1], len(second_ring))
            gb[z] = add_up(ga, 2 * ncol)
            for dz in sorted(range(nz), key=lambda d: -min(d, nz - d)):
                for to_core in (0, 1):
                    if dz or to_core == 0:
                        pltpu.make_async_remote_copy(
                            src_ref=gb.at[z], dst_ref=gb.at[z],
                            send_sem=as_sem.at[stage + 1], recv_sem=ar_sem.at[stage + 1],
                            device_id=(2 * lax.rem(z + dz, nz) + to_core, me_c), device_id_type=MESH,
                        ).start()
            wait_bytes(ga, ncol - 1, as_sem.at[stage])
            wait_bytes(gb, nz - 1, ar_sem.at[stage + 1])

        @pl.when(core == 0)
        def _():
            if stage == 0:
                pl.semaphore_wait(near_sem.at[1], len(second_ring))
            wait_bytes(ga, ncol, as_sem.at[stage])
            wait_bytes(gb, nz, ar_sem.at[stage + 1])

        return add_up(gb, nz)

    def settle(stage):
        @pl.when(core == 1)
        def _():
            wait_bytes(ga, 2 * nz - 1, as_sem.at[stage])

    def gather(accs):
        packed = jnp.zeros((8, LANE), jnp.float32)
        for k, acc in enumerate(accs):
            packed = jnp.where(lane8 == k, jnp.sum(acc, axis=1, keepdims=True), packed)
        return jnp.sum(packed, axis=0, keepdims=True)

    def spread(row, k):
        return jnp.broadcast_to(row[:, k : k + 1], (1, LANE))

    start_sum(gather((nu0, nu1, nu2, nu3, nu4, nu5, s_q, s_qb, s_q1, s_q2)), ga, gb, 0)

    for copy, _, here in sends[10:]:
        when(*here)(copy.wait_recv)
    for k in range(parts):
        unpack(pl.ds(TOP + pile * k, pile), pl.ds(0, pile), k, pile, 3)
    unpack(top_at, nw_at, parts - 1, HALO, 3)
    unpack(end_at, sw_at, 0, HALO, 3)

    def all1(r, n, accs, keep):
        weights_and_v1(r, n, ext, keep)
        return accs

    def all2(r, n, accs, keep):
        second(r, n, ext, keep)
        return accs

    def pass_q(r, n, accs, keep):
        put(LP, r, n, apply_from(rows_of(Q, r, n), Q, r, n, rows_of(CE, r, n), *weights_of(r, n), keep))
        return accs

    over_rows(all1, 0)
    over_rows(all2, 0)
    over_rows(pass_q, 0)

    for copy, there, _ in sends:
        when(*there)(copy.wait_send)
    sums = finish_sum(ga, gb, 0)

    c0, c1, c2 = solve([spread(sums, k) for k in range(6)])
    t_q, t_qb, t_q1, t_q2 = [spread(sums, k) for k in range(6, 10)]

    def pass_x(r, n, accs, keep):
        b, v1, v2 = rows_of(B, r, n), rows_of(V1, r, n), rows_of(V2, r, n)
        value = [c0 * b[j] + (c1 * v1[j] + c2 * v2[j]) for j in range(ext)]
        put(X, r, n, value)
        if keep is None:
            for j in range(tiles):
                val_ref[pl.ds(pl.multiple_of(r - TOP, 8), n), pl.ds(j * LANE, LANE)] = value[j]
        return accs

    over_rows(pass_x, 0)

    def pass3(r, n, accs, keep):
        last, start = masks(n)
        x = rows_of(X, r, n)
        xe, xw = to_east(x, last), to_west(x, start)
        xs, xn = rows_of(X, r + 1, n), rows_of(X, r - 1, n)
        q, lp, center = rows_of(Q, r, n), rows_of(LP, r, n), rows_of(CE, r, n)
        u1, full = [], []
        for j in range(ext):
            dr, dc = xs[j] - xn[j], xe[j] - xw[j]
            g = (0.25 / (2.0 * 0.25) * SCALE) * (dr * dr + dc * dc)
            full.append(center[j] + g)
            u1.append(lp[j] + g * q[j])
        u1 = keep_in(u1, keep)
        put(CE, r, n, full)
        put(U1, r, n, u1)
        if accs is None:
            return None
        return add(accs, ((q, u1), (u1, u1)))

    mu1, mu2 = over_rows(pass3, blank(2), unrolled=True)

    def pass4(r, n, accs, keep):
        u1 = rows_of(U1, r, n)
        u2 = apply_from(u1, U1, r, n, rows_of(CE, r, n), *weights_of(r, n), keep)
        put(U2, r, n, u2)
        return None if accs is None else add(accs, ((u1, u2), (u2, u2)))

    mu3, mu4 = over_rows(pass4, blank(2), False, True)

    mu5 = zero
    for i in range(rows // step_rows):
        mu5 = fold(mu5, face_terms(U2, TOP + i * step_rows, step_rows, ext))


    start_sum(gather((mu0, mu1, mu2, mu3, mu4, mu5)), gc, gd, 2)
    erg_ref[...] = (t_qb - DISCOUNT * (c0 * t_qb + (c1 * t_q1 + c2 * t_q2))) / t_q
    settle(1)
    sums = finish_sum(gc, gd, 2)
    d0, d1, d2 = solve([spread(sums, k) for k in range(6)])

    def last_pass(i, carry):
        r = pl.multiple_of(i * step_rows, step_rows)
        at = pl.ds(TOP + r, step_rows)
        for j in range(tiles):
            den_ref[pl.ds(r, step_rows), pl.ds(j * LANE, LANE)] = d0 * Q[j, at, :] + (d1 * U1[j, at, :] + d2 * U2[j, at, :])
        return carry

    lax.fori_loop(0, rows // step_rows, last_pass, 0)
    settle(3)


def store_kernel(val_ref, den_ref, val_hbm, den_hbm, sem):
    copies = [pltpu.make_async_copy(val_ref, val_hbm, sem.at[0]), pltpu.make_async_copy(den_ref, den_hbm, sem.at[1])]
    for copy in copies:
        copy.start()
    for copy in copies:
        copy.wait()


def solution(mesh):
    nrow, ncol = mesh.shape["row"], mesh.shape["col"]

    def body(running_cost, control_x, control_y, prior_density):
        rows, cols = running_cost.shape
        tiles = cols // LANE
        ext = tiles + 1
        pile = rows // 8
        big = pltpu.VMEM((ext, rows + 2 * TOP, LANE), jnp.float32)
        plain = pltpu.VMEM((tiles, rows, LANE), jnp.float32)
        value, density, ergodic = pl.pallas_call(
            functools.partial(kernel, nrow, ncol, 4 if ncol % 4 == 0 else 1, rows, tiles, min(rows, 128)),
            out_shape=(
                jax.ShapeDtypeStruct((rows, cols), jnp.float32),
                jax.ShapeDtypeStruct((rows, cols), jnp.float32),
                jax.ShapeDtypeStruct((1, LANE), jnp.float32),
            ),
            in_specs=[pl.BlockSpec(memory_space=pltpu.HBM)] * 4,
            out_specs=(pl.BlockSpec(memory_space=pltpu.VMEM),) * 3,
            scratch_shapes=[plain] * 3
            + [big] * 13
            + [pltpu.VMEM((pile, LANE), jnp.float32)] * 2
            + [pltpu.VMEM((pile + 16, LANE), jnp.float32)] * 2
            + [pltpu.VMEM((2, pile + 16, LANE), jnp.float32)] * 4
            + [pltpu.VMEM((2 * ncol, 1, LANE), jnp.float32), pltpu.VMEM((nrow // 2, 1, LANE), jnp.float32)] * 2
            + [
                pltpu.SemaphoreType.DMA((4, tiles)),
                pltpu.SemaphoreType.DMA((12,)),
                pltpu.SemaphoreType.DMA((12,)),
                pltpu.SemaphoreType.DMA((4,)),
                pltpu.SemaphoreType.DMA((4,)),
                pltpu.SemaphoreType.REGULAR((2,)),
            ],
            compiler_params=pltpu.CompilerParams(
                collective_id=0, has_side_effects=True, vmem_limit_bytes=55200000
            ),
        )(running_cost, control_x, control_y, prior_density)
        value, density = pl.pallas_call(
            store_kernel,
            out_shape=(jax.ShapeDtypeStruct((rows, cols), jnp.float32),) * 2,
            in_specs=[pl.BlockSpec(memory_space=pltpu.VMEM)] * 2,
            out_specs=(pl.BlockSpec(memory_space=pltpu.HBM),) * 2,
            scratch_shapes=[pltpu.SemaphoreType.DMA((2,))],
            compiler_params=pltpu.CompilerParams(vmem_limit_bytes=4 * 1024 * 1024),
        )(value, density)
        return value, density, ergodic[0, 0]

    spec = P("row", "col")
    return jax.shard_map(
        body,
        mesh=mesh,
        in_specs=(spec, spec, spec, spec),
        out_specs=(spec, spec, P()),
        check_vma=False,
    )
```

```python
import functools

import jax
import jax.numpy as jnp
from jax import lax
from jax.experimental import pallas as pl
from jax.experimental.pallas import tpu as pltpu
from jax.sharding import PartitionSpec as P

MESH = pl.DeviceIdType.MESH

SCALE = 1.0 / 64.0
FACE = 0.25 * 0.5 * SCALE
DISCOUNT = 0.05

LANE = 128
TOP = 16
HALO = 8


def solve(nu):
    shift = DISCOUNT * SCALE
    m = [nu[k + 1] + shift * nu[k] for k in range(5)]
    l1 = m[1] / m[0]
    l2 = m[2] / m[0]
    d1 = m[2] - l1 * m[1]
    e = m[3] - l2 * m[1]
    l3 = e / d1
    d2 = (m[4] - l2 * m[2]) - l3 * e
    y0 = nu[0]
    y1 = nu[1] - l1 * y0
    y2 = (nu[2] - l2 * y0) - l3 * y1
    c2 = y2 / d2
    c1 = y1 / d1 - l3 * c2
    c0 = y0 / m[0] - l1 * c1 - l2 * c2
    return c0 * SCALE, c1 * SCALE, c2 * SCALE


def kernel(
    nrow, ncol, nx, rows, tiles, step_rows,
    rc_hbm, cx_hbm, cy_hbm, pr_hbm,
    val_ref, den_ref, erg_ref,
    cx, cy, rc, C, B, Q, WE, WW, WS, CE, V1, V2, X, LP, U1, U2,
    pack_e, pack_w, from_w, from_e, SC, SB, S1, S2, ga, gb, gc, gd,
    in_sem, hs_sem, hr_sem, as_sem, ar_sem, near_sem,
):
    me_r = lax.axis_index("row")
    me_c = lax.axis_index("col")
    up, down = lax.rem(me_r + nrow - 1, nrow), lax.rem(me_r + 1, nrow)
    west, east = lax.rem(me_c + ncol - 1, ncol), lax.rem(me_c + 1, ncol)
    ext = tiles + 1
    END = TOP + rows

    def tile_of(ref, j):
        return ref.at[:, pl.ds(j * LANE, LANE)]

    loads = {}
    outer_tiles = tuple(sorted({0, tiles - 1}))
    inner_tiles = tuple(range(1, tiles - 1))
    fields = ((cx_hbm, cx, 0), (cy_hbm, cy, 0), (rc_hbm, rc, 0), (pr_hbm, Q, TOP))
    for n, (src, dst, top), js in [(n, f, js) for js in (outer_tiles, inner_tiles) for n, f in enumerate(fields)]:
        for j in js:
            copy = pltpu.make_async_copy(tile_of(src, j), dst.at[j, pl.ds(top, rows), :], in_sem.at[n, j])
            copy.start()
            loads[n, j] = copy

    nz, ny = nrow // 2, ncol // nx
    core, z = lax.rem(me_r, 2), me_r // 2
    x, y = me_c // ny, lax.rem(me_c, ny)

    def at_offset(dz, dc, dx, dy):
        r = 2 * lax.rem(z + dz, nz) + lax.rem(core + dc, 2)
        return r, ny * lax.rem(x + dx, nx) + lax.rem(y + dy, ny)

    def offsets(zs, cs, xs, ys):
        every = {(a % nz, b, c % nx, d % ny) for a in zs for b in cs for c in xs for d in ys}
        return sorted(every - {(0, 0, 0, 0)})

    def tell(sem, to):
        pl.semaphore_signal(sem, inc=1, device_id=to, device_id_type=MESH)

    not_first, not_last = me_r > 0, me_r < nrow - 1
    not_west, not_east = me_c > 0, me_c < ncol - 1
    beyond = me_r + 2 * core - 1
    far_row = lax.rem(beyond + nrow, nrow)

    def when(*conditions):
        def run(fn):
            for c in conditions[::-1]:
                fn = functools.partial(lambda c, f: pl.when(c)(f) and None, c, fn)
            fn()
        return run

    far_there = (beyond >= 0, beyond < nrow)

    barrier = pltpu.get_barrier_semaphore()
    around = (-1, 0, 1)
    near = offsets((0,), (0, 1), around, around) + offsets(around, (0,), (0,), (0,))
    for o in near:
        tell(barrier, at_offset(*o))
    when(*far_there)(lambda: tell(barrier, (far_row, me_c)))
    when(*far_there, not_west)(lambda: tell(barrier, (far_row, west)))
    when(*far_there, not_east)(lambda: tell(barrier, (far_row, east)))

    zero = jnp.zeros((8, LANE), jnp.float32)
    for ref in (C, B, Q, WS, V1, V2, X, U1, U2):
        for j in range(ext):
            ref[j, pl.ds(0, 8), :] = zero
            ref[j, pl.ds(END + HALO, 8), :] = zero

    low, high = pl.ds(0, 8), pl.ds(rows // 8 - 8, 8)
    sw_at, nw_at = pl.ds(rows // 8, 8), pl.ds(rows // 8 + 8, 8)

    @pl.when(me_c == 0)
    def _():
        from_w[...] = jnp.zeros_like(from_w)

    @pl.when(me_c == ncol - 1)
    def _():
        from_e[...] = jnp.zeros_like(from_e)

    def no_row(top, corner):
        for f in (C, B, Q):
            for j in range(tiles):
                f[j, pl.ds(top, HALO), :] = zero
        from_w[corner, :] = zero
        from_e[corner, :] = zero

    @pl.when(me_r == 0)
    def _():
        no_row(TOP - HALO, nw_at)

    @pl.when(me_r == nrow - 1)
    def _():
        no_row(END, sw_at)

    def fold(acc, v):
        while v.shape[0] > 8:
            n = v.shape[0]
            if n % 16 == 0:
                v = v[: n // 2, :] + v[n // 2 :, :]
            else:
                acc, v = acc + v[n - 8 :, :], v[: n - 8, :]
        return acc + v

    def blank(k):
        return tuple(zero for _ in range(k))

    def prepare(js, accs):
        for n in range(len(fields)):
            for j in js:
                loads[n, j].wait()

        def first(i, accs):
            r = pl.multiple_of(i * step_rows, step_rows)
            at = pl.ds(TOP + r, step_rows)
            terms = [None] * 4
            for j in js:
                a, b = cx[j, pl.ds(r, step_rows), :], cy[j, pl.ds(r, step_rows), :]
                cost = 0.5 * (a * a + b * b)
                force = rc[j, pl.ds(r, step_rows), :] + cost
                C[j, at, :] = (1.0 + cost) * FACE
                B[j, at, :] = force
                q = Q[j, at, :]
                for k, t in enumerate((force * force, q, q * force, q * q)):
                    terms[k] = t if terms[k] is None else terms[k] + t
            return tuple(fold(acc, t) for acc, t in zip(accs, terms))

        return lax.fori_loop(0, rows // step_rows, first, accs)

    sums0 = prepare(outer_tiles, blank(4))

    parts = LANE // 16
    pile = rows // parts
    lane = lax.broadcasted_iota(jnp.int32, (pile, LANE), 1)
    slot = lane & 15
    is_c, is_b = slot < 6, slot < 11
    acc_e = jnp.zeros((pile, LANE), jnp.float32)
    acc_w = jnp.zeros((pile, LANE), jnp.float32)
    for k in range(parts):
        at = pl.ds(TOP + pile * k, pile)
        here = (lane >> 4) == k
        got = []
        for j, firsts in ((tiles - 1, (122, 123, 125)), (0, (0, 0, 0))):
            rolled = [
                pltpu.roll(f[j, at, :], (16 * k + o - s) % LANE, 1)
                for f, o, s in zip((C, B, Q), (0, 6, 11), firsts)
            ]
            got.append(jnp.where(is_c, rolled[0], jnp.where(is_b, rolled[1], rolled[2])))
        acc_e = jnp.where(here, got[0], acc_e)
        acc_w = jnp.where(here, got[1], acc_w)
    pack_e[...] = acc_e
    pack_w[...] = acc_w

    any_west, any_east = (me_c + ncol - 1) // ncol, (2 * ncol - 2 - me_c) // ncol
    any_far = core * ((2 * nrow - 2 - me_r) // nrow) + (1 - core) * ((me_r + nrow - 1) // nrow)
    pl.semaphore_wait(barrier, len(near) + any_far * (1 + any_west + any_east))

    sends = []

    def send(src, dst, to, there, here):
        n = len(sends)
        copy = pltpu.make_async_remote_copy(
            src_ref=src, dst_ref=dst, send_sem=hs_sem.at[n], recv_sem=hr_sem.at[n],
            device_id=to, device_id_type=MESH,
        )
        when(*there)(copy.start)
        sends.append((copy, there, here))

    send(pack_e.at[high, :], from_w.at[nw_at, :], (down, east), (not_last, not_east), (not_first, not_west))
    send(pack_e.at[low, :], from_w.at[sw_at, :], (up, east), (not_first, not_east), (not_last, not_west))
    send(pack_w.at[high, :], from_e.at[nw_at, :], (down, west), (not_last, not_west), (not_first, not_east))
    send(pack_w.at[low, :], from_e.at[sw_at, :], (up, west), (not_first, not_west), (not_last, not_east))
    send(pack_e, from_w.at[pl.ds(0, pile), :], (me_r, east), (not_east,), (not_west,))
    send(pack_w, from_e.at[pl.ds(0, pile), :], (me_r, west), (not_west,), (not_east,))
    if inner_tiles:
        sums0 = prepare(inner_tiles, sums0)
    nu0, s_q, s_qb, mu0 = sums0

    body = pl.ds(0, tiles)
    for f in (C, B, Q):
        send(f.at[body, pl.ds(TOP, HALO), :], f.at[body, pl.ds(END, HALO), :], (up, me_c), (not_first,), (not_last,))
        send(f.at[body, pl.ds(END - HALO, HALO), :], f.at[body, pl.ds(TOP - HALO, HALO), :], (down, me_c), (not_last,), (not_first,))

    first_ring = offsets((0,), (0,), around, around) + offsets(around, (0,), (0,), (0,))
    second_ring = offsets((-2, 2), (0,), (0,), (0,))
    for o in first_ring:
        tell(near_sem.at[0], at_offset(*o))

    fone, fnil = jnp.float32(1.0), jnp.float32(0.0)
    has_n, has_s = jnp.where(not_first, fone, fnil), jnp.where(not_last, fone, fnil)
    has_w, has_e = jnp.where(not_west, fone, fnil), jnp.where(not_east, fone, fnil)
    lane1 = lax.broadcasted_iota(jnp.int32, (1, LANE), 1)
    inside = jnp.where(lane1 < LANE // 2, has_e, has_w)

    def masks(n):
        l = lax.broadcasted_iota(jnp.int32, (n, LANE), 1)
        return l == LANE - 1, l == 0

    def to_east(vs, last):
        r = [pltpu.roll(v, LANE - 1, 1) for v in vs]
        return [jnp.where(last, r[(j + 1) % len(vs)], r[j]) for j in range(len(vs))]

    def to_west(vs, start):
        r = [pltpu.roll(v, 1, 1) for v in vs]
        return [jnp.where(start, r[(j - 1) % len(vs)], r[j]) for j in range(len(vs))]

    def rows_of(ref, r, n, count=ext):
        return [ref[j, pl.ds(r, n), :] for j in range(count)]

    def keep_in(vs, keep):
        if len(vs) == ext:
            vs = vs[:tiles] + [vs[tiles] * inside]
        return vs if keep is None else [v * keep for v in vs]

    def put(ref, r, n, vs):
        for j, v in enumerate(vs):
            ref[j, pl.ds(r, n), :] = v

    def add(accs, lists, weigh=None):
        out = []
        for acc, (p, q) in zip(accs, lists):
            total = None
            for j in range(tiles):
                t = p[j] * q[j]
                if weigh is not None and weigh[j] is not None:
                    t = t * weigh[j]
                total = t if total is None else total + t
            out.append(fold(acc, total))
        return tuple(out)

    def apply_from(vs, ref, r, n, center, we, ww, ws, wn, keep):
        count = len(vs)
        last, start = masks(n)
        ve, vw = to_east(vs, last), to_west(vs, start)
        vs_, vn = rows_of(ref, r + 1, n, count), rows_of(ref, r - 1, n, count)
        return keep_in(
            [
                center[j] * vs[j] - ((ws[j] * vs_[j] + wn[j] * vn[j]) + (we[j] * ve[j] + ww[j] * vw[j]))
                for j in range(count)
            ],
            keep,
        )

    def over_rows(step, accs, above=True, unrolled=False):
        if above:
            step(TOP - HALO, HALO, None, has_n)
        step(END, HALO, None, has_s)

        def loop(i, accs):
            return step(pl.multiple_of(TOP + i * step_rows, TOP), step_rows, accs, None)

        if unrolled:
            for i in range(rows // step_rows):
                accs = step(TOP + i * step_rows, step_rows, accs, None)
            return accs
        return lax.fori_loop(0, rows // step_rows, loop, accs)

    def weights_and_v1(r, n, count, keep):
        last, start = masks(n)
        c0 = rows_of(C, r, n, count)
        cs, cn = rows_of(C, r + 1, n, count), rows_of(C, r - 1, n, count)
        ce, cw = to_east(c0, last), to_west(c0, start)
        we = [c0[j] + ce[j] for j in range(count)]
        ww = [c0[j] + cw[j] for j in range(count)]
        ws = [c0[j] + cs[j] for j in range(count)]
        wn = [c0[j] + cn[j] for j in range(count)]
        center = [(ws[j] + wn[j]) + (we[j] + ww[j]) for j in range(count)]
        put(WE, r, n, we)
        put(WW, r, n, ww)
        put(WS, r, n, ws)
        put(CE, r, n, center)
        v1 = apply_from(rows_of(B, r, n, count), B, r, n, center, we, ww, ws, wn, keep)
        put(V1, r, n, v1)
        return v1

    def weights_of(r, n, count=ext):
        return rows_of(WE, r, n, count), rows_of(WW, r, n, count), rows_of(WS, r, n, count), rows_of(WS, r - 1, n, count)

    def second(r, n, count, keep):
        v1 = rows_of(V1, r, n, count)
        v2 = apply_from(v1, V1, r, n, rows_of(CE, r, n, count), *weights_of(r, n, count), keep)
        put(V2, r, n, v2)
        return v1, v2

    def face_terms(V, r, n, count, weigh=None):
        last, _ = masks(n)
        v = rows_of(V, r, n, count)
        ve = to_east(v, last)
        total = None
        for j in range(tiles):
            out = WE[j, pl.ds(r, n), :] * ve[j] + WS[j, pl.ds(r, n), :] * V[j, pl.ds(r + 1, n), :]
            t = v[j] * (CE[j, pl.ds(r, n), :] * v[j] - (out + out))
            if weigh is not None and weigh[j] is not None:
                t = t * weigh[j]
            total = t if total is None else total + t
        return total

    in_west = jnp.where(lane1 >= 6, jnp.ones((1, LANE), jnp.float32), jnp.zeros((1, LANE), jnp.float32))
    in_east = jnp.where(lane1 < LANE - 6, jnp.ones((1, LANE), jnp.float32), jnp.zeros((1, LANE), jnp.float32))
    weigh = [None] * tiles
    weigh[0] = in_west
    weigh[tiles - 1] = in_east if tiles > 1 else in_west * in_east
    INNER = 16
    pieces = 2
    part = (rows - 2 * INNER) // pieces

    def over_center(step, accs):
        step(TOP + 8, 8, None)
        step(END - 16, 8, None)

        def loop(i, accs):
            return step(pl.multiple_of(TOP + INNER + i * part, 8), part, accs)

        return lax.fori_loop(0, pieces, loop, accs)

    def center1(r, n, accs):
        v1 = weights_and_v1(r, n, tiles, None)
        if accs is None:
            return None
        return add(accs, ((rows_of(B, r, n, tiles), v1), (v1, v1), (rows_of(Q, r, n, tiles), v1)), weigh)

    def center2(r, n, accs):
        v1, v2 = second(r, n, tiles, None)
        if accs is None:
            return None
        return add(accs, ((v1, v2), (v2, v2), (rows_of(Q, r, n, tiles), v2)), weigh)

    def center3(i, acc):
        return fold(acc, face_terms(V2, pl.multiple_of(TOP + INNER + i * part, 8), part, tiles, weigh))

    nu1, nu2, s_q1 = over_center(center1, blank(3))
    nu3, nu4, s_q2 = over_center(center2, blank(3))
    nu5 = lax.fori_loop(0, pieces, center3, zero)

    def own_columns(f, j, shift):
        acc = jnp.zeros((pile, LANE), jnp.float32)
        for k in range(parts):
            acc = jnp.where((lane >> 4) == k, pltpu.roll(f[j, pl.ds(TOP + pile * k, pile), :], (16 * k + shift) % LANE, 1), acc)
        return acc

    own_w = [own_columns(f, 0, 6) for f in (C, B, Q)]
    own_e = [own_columns(f, tiles - 1, 10 - LANE) for f in (C, B, Q)]

    for copy, _, here in sends[:10]:
        when(*here)(copy.wait_recv)

    pl.semaphore_wait(near_sem.at[0], len(first_ring))
    for o in second_ring:
        tell(near_sem.at[1], at_offset(*o))

    def unpack(at, src, k, n, fields):
        w, e = from_w[src, :], from_e[src, :]
        l = lax.broadcasted_iota(jnp.int32, (n, LANE), 1)
        none = jnp.zeros((n, LANE), jnp.float32)
        for f, o, s, wide in zip((C, B, Q)[:fields], (0, 6, 11), (122, 123, 125), (6, 5, 3)):
            rw = pltpu.roll(w, (s - 16 * k - o) % LANE, 1)
            re = pltpu.roll(e, (-16 * k - o) % LANE, 1)
            f[tiles, at, :] = jnp.where(l >= s, rw, jnp.where(l < wide, re, none))

    top_at, end_at = pl.ds(TOP - HALO, HALO), pl.ds(END, HALO)
    for k in range(parts):
        if pile * k < 32 or pile * (k + 1) > rows - 32:
            unpack(pl.ds(TOP + pile * k, pile), pl.ds(0, pile), k, pile, 2)
    unpack(top_at, nw_at, parts - 1, HALO, 2)
    unpack(end_at, sw_at, 0, HALO, 2)

    rows32 = lax.broadcasted_iota(jnp.int32, (32, LANE), 0)
    ones32 = jnp.ones((32, LANE), jnp.float32)
    tops = ((TOP - HALO, jnp.where(rows32 < HALO, has_n * ones32, ones32), HALO), (END - 24, jnp.where(rows32 >= 24, has_s * ones32, ones32), HALO))
    def own_16(vs, skip):
        return [v[skip : skip + 16, :] for v in vs]

    for r, keep, skip in tops:
        v1 = own_16(weights_and_v1(r, 32, ext, keep), skip)
        b, q = rows_of(B, r + skip, 16, tiles), rows_of(Q, r + skip, 16, tiles)
        nu1, nu2, s_q1 = add((nu1, nu2, s_q1), ((b, v1), (v1, v1), (q, v1)))
    for r, keep, skip in tops:
        v1, v2 = [own_16(v, skip) for v in second(r, 32, ext, keep)]
        q = rows_of(Q, r + skip, 16, tiles)
        nu3, nu4, s_q2 = add((nu3, nu4, s_q2), ((v1, v2), (v2, v2), (q, v2)))
    for r, keep, skip in tops:
        nu5 = fold(nu5, face_terms(V2, r + skip, 16, ext))

    def put_strip(ref, n, v):
        ref[n, pl.ds(8, pile), :] = v
        ref[n, pl.ds(7, 1), :] = pltpu.roll(v[pile - 1 :, :], 16, 1)
        ref[n, pl.ds(8 + pile, 1), :] = pltpu.roll(v[:1, :], LANE - 16, 1)

    def below_above(ref, n):
        return ref[n, pl.ds(9, pile), :], ref[n, pl.ds(7, pile), :]

    sides = ((own_w, from_w, (0, -5), slot < 6, has_w, 6), (own_e, from_e, (10, 4), slot >= 10, has_e, 4))
    row_at = lax.broadcasted_iota(jnp.int32, (pile, LANE), 0) + pile * (lane >> 4)
    for n, (own, come, shifts, outer, there, begin) in enumerate(sides):
        got = come[pl.ds(0, pile), :]
        keep = jnp.where(outer, there * jnp.ones((pile, LANE), jnp.float32), jnp.ones((pile, LANE), jnp.float32))
        middle = (row_at >= INNER) & (row_at < rows - INNER) & (slot >= begin) & (slot < begin + 6)
        mine = jnp.where(middle, jnp.ones((pile, LANE), jnp.float32), jnp.zeros((pile, LANE), jnp.float32))
        c, b = [jnp.where(outer, pltpu.roll(got, h % LANE, 1), o) for h, o in zip(shifts, own)]
        q = own[2] * mine
        put_strip(SC, n, c)
        put_strip(SB, n, b)
        c_s, c_n = below_above(SC, n)
        we, ww, ws, wn = c + pltpu.roll(c, LANE - 1, 1), c + pltpu.roll(c, 1, 1), c + c_s, c + c_n
        mid = (ws + wn) + (we + ww)

        def strip_apply(ref, v):
            put_strip(ref, n, v)
            v_s, v_n = below_above(ref, n)
            beside = we * pltpu.roll(v, LANE - 1, 1) + ww * pltpu.roll(v, 1, 1)
            return (mid * v - ((ws * v_s + wn * v_n) + beside)) * keep

        v1 = strip_apply(SB, b)
        v2 = strip_apply(S1, v1)
        put_strip(S2, n, v2)
        out = we * pltpu.roll(v2, LANE - 1, 1) + ws * S2[n, pl.ds(9, pile), :]
        m1, m2 = v1 * mine, v2 * mine
        nu1, nu2, nu3 = fold(nu1, b * m1), fold(nu2, v1 * m1), fold(nu3, v1 * m2)
        nu4, nu5 = fold(nu4, v2 * m2), fold(nu5, m2 * (mid * v2 - (out + out)))
        s_q1, s_q2 = fold(s_q1, q * v1), fold(s_q2, q * v2)

    lane8 = lax.broadcasted_iota(jnp.int32, (8, LANE), 1)

    def add_up(buf, count):
        terms = [buf[k] for k in range(count)]
        while len(terms) > 1:
            terms = [terms[k] + terms[k + 1] if k + 1 < len(terms) else terms[k] for k in range(0, len(terms), 2)]
        return terms[0]

    def start_sum(part, ga, gb, stage):
        slot = core * ncol + me_c
        ga[slot] = part
        for d in sorted(range(ncol), key=lambda d: -min(d, ncol - d)):
            copy = pltpu.make_async_remote_copy(
                src_ref=ga.at[slot], dst_ref=ga.at[slot], send_sem=as_sem.at[stage], recv_sem=ar_sem.at[stage],
                device_id=(2 * z + 1, lax.rem(me_c + d, ncol)), device_id_type=MESH,
            )
            if d == 0:
                pl.when(core == 0)(copy.start)
            else:
                copy.start()

    def wait_bytes(buf, count, sem):
        some = buf.at[pl.ds(0, count)]
        pltpu.make_async_copy(some, some, sem).wait()

    def finish_sum(ga, gb, stage):
        @pl.when(core == 1)
        def _():
            wait_bytes(ga, 2 * ncol - 1, ar_sem.at[stage])
            if stage == 0:
                pl.semaphore_wait(near_sem.at[1], len(second_ring))
            gb[z] = add_up(ga, 2 * ncol)
            for dz in sorted(range(nz), key=lambda d: -min(d, nz - d)):
                for to_core in (0, 1):
                    if dz or to_core == 0:
                        pltpu.make_async_remote_copy(
                            src_ref=gb.at[z], dst_ref=gb.at[z],
                            send_sem=as_sem.at[stage + 1], recv_sem=ar_sem.at[stage + 1],
                            device_id=(2 * lax.rem(z + dz, nz) + to_core, me_c), device_id_type=MESH,
                        ).start()
            wait_bytes(ga, ncol - 1, as_sem.at[stage])
            wait_bytes(gb, nz - 1, ar_sem.at[stage + 1])

        @pl.when(core == 0)
        def _():
            if stage == 0:
                pl.semaphore_wait(near_sem.at[1], len(second_ring))
            wait_bytes(ga, ncol, as_sem.at[stage])
            wait_bytes(gb, nz, ar_sem.at[stage + 1])

        return add_up(gb, nz)

    def settle(stage):
        @pl.when(core == 1)
        def _():
            wait_bytes(ga, 2 * nz - 1, as_sem.at[stage])

    chips = nz * ncol

    def start_direct(part):
        slot = me_r * ncol + me_c
        gc[slot] = part
        zs = [2 * lax.rem(z + d, nz) + 1 for d in range(nz)]
        cs = [[ny * lax.rem(x + a, nx) + lax.rem(y + b, ny) for b in range(ny)] for a in range(nx)]

        def hops(o):
            return min(o[0], nz - o[0]) + min(o[1], nx - o[1]) + min(o[2], ny - o[2])

        every = [(d, a, b) for d in range(nz) for a in range(nx) for b in range(ny)]
        for o in sorted(every, key=lambda o: -hops(o)):
            copy = pltpu.make_async_remote_copy(
                src_ref=gc.at[slot], dst_ref=gc.at[slot], send_sem=as_sem.at[2], recv_sem=ar_sem.at[2],
                device_id=(zs[o[0]], cs[o[1]][o[2]]), device_id_type=MESH,
            )
            if hops(o) == 0:
                pl.when(core == 0)(copy.start)
            else:
                copy.start()

    hand_over = pltpu.make_async_remote_copy(
        src_ref=gd.at[0], dst_ref=gd.at[0], send_sem=as_sem.at[3], recv_sem=ar_sem.at[3],
        device_id=(2 * z, me_c), device_id_type=MESH,
    )

    def finish_direct():
        @pl.when(core == 1)
        def _():
            wait_bytes(gc, 2 * chips - 1, ar_sem.at[2])
            gd[0] = jnp.sum(gc[...], axis=0)
            hand_over.start()
            wait_bytes(gc, chips - 1, as_sem.at[2])

        @pl.when(core == 0)
        def _():
            wait_bytes(gc, chips, as_sem.at[2])
            wait_bytes(gd, 1, ar_sem.at[3])

        return gd[0]

    def gather(accs):
        packed = jnp.zeros((8, LANE), jnp.float32)
        for k, acc in enumerate(accs):
            packed = jnp.where(lane8 == k, jnp.sum(acc, axis=1, keepdims=True), packed)
        return jnp.sum(packed, axis=0, keepdims=True)

    def spread(row, k):
        return jnp.broadcast_to(row[:, k : k + 1], (1, LANE))

    start_sum(gather((nu0, nu1, nu2, nu3, nu4, nu5, s_q, s_qb, s_q1, s_q2)), ga, gb, 0)

    for copy, _, here in sends[10:]:
        when(*here)(copy.wait_recv)
    for k in range(parts):
        unpack(pl.ds(TOP + pile * k, pile), pl.ds(0, pile), k, pile, 3)
    unpack(top_at, nw_at, parts - 1, HALO, 3)
    unpack(end_at, sw_at, 0, HALO, 3)

    def all1(r, n, accs, keep):
        weights_and_v1(r, n, ext, keep)
        return accs

    def all2(r, n, accs, keep):
        second(r, n, ext, keep)
        return accs

    def pass_q(r, n, accs, keep):
        put(LP, r, n, apply_from(rows_of(Q, r, n), Q, r, n, rows_of(CE, r, n), *weights_of(r, n), keep))
        return accs

    over_rows(all1, 0)
    over_rows(all2, 0)
    over_rows(pass_q, 0)

    for copy, there, _ in sends:
        when(*there)(copy.wait_send)
    sums = finish_sum(ga, gb, 0)

    c0, c1, c2 = solve([spread(sums, k) for k in range(6)])
    t_q, t_qb, t_q1, t_q2 = [spread(sums, k) for k in range(6, 10)]

    def pass_x(r, n, accs, keep):
        b, v1, v2 = rows_of(B, r, n), rows_of(V1, r, n), rows_of(V2, r, n)
        value = [c0 * b[j] + (c1 * v1[j] + c2 * v2[j]) for j in range(ext)]
        put(X, r, n, value)
        if keep is None:
            for j in range(tiles):
                val_ref[pl.ds(pl.multiple_of(r - TOP, 8), n), pl.ds(j * LANE, LANE)] = value[j]
        return accs

    over_rows(pass_x, 0)

    def pass3(r, n, accs, keep):
        last, start = masks(n)
        x = rows_of(X, r, n)
        xe, xw = to_east(x, last), to_west(x, start)
        xs, xn = rows_of(X, r + 1, n), rows_of(X, r - 1, n)
        q, lp, center = rows_of(Q, r, n), rows_of(LP, r, n), rows_of(CE, r, n)
        u1, full = [], []
        for j in range(ext):
            dr, dc = xs[j] - xn[j], xe[j] - xw[j]
            g = (0.25 / (2.0 * 0.25) * SCALE) * (dr * dr + dc * dc)
            full.append(center[j] + g)
            u1.append(lp[j] + g * q[j])
        u1 = keep_in(u1, keep)
        put(CE, r, n, full)
        put(U1, r, n, u1)
        if accs is None:
            return None
        return add(accs, ((q, u1), (u1, u1)))

    mu1, mu2 = over_rows(pass3, blank(2), unrolled=True)

    def pass4(r, n, accs, keep):
        u1 = rows_of(U1, r, n)
        u2 = apply_from(u1, U1, r, n, rows_of(CE, r, n), *weights_of(r, n), keep)
        put(U2, r, n, u2)
        return None if accs is None else add(accs, ((u1, u2), (u2, u2)))

    mu3, mu4 = over_rows(pass4, blank(2), False, True)

    mu5 = zero
    for i in range(rows // step_rows):
        mu5 = fold(mu5, face_terms(U2, TOP + i * step_rows, step_rows, ext))


    start_direct(gather((mu0, mu1, mu2, mu3, mu4, mu5)))
    erg_ref[...] = (t_qb - DISCOUNT * (c0 * t_qb + (c1 * t_q1 + c2 * t_q2))) / t_q
    settle(1)
    sums = finish_direct()
    d0, d1, d2 = solve([spread(sums, k) for k in range(6)])

    def last_pass(i, carry):
        r = pl.multiple_of(i * step_rows, step_rows)
        at = pl.ds(TOP + r, step_rows)
        for j in range(tiles):
            den_ref[pl.ds(r, step_rows), pl.ds(j * LANE, LANE)] = d0 * Q[j, at, :] + (d1 * U1[j, at, :] + d2 * U2[j, at, :])
        return carry

    lax.fori_loop(0, rows // step_rows, last_pass, 0)
    pl.when(core == 1)(hand_over.wait_send)


def store_kernel(val_ref, den_ref, val_hbm, den_hbm, sem):
    copies = [pltpu.make_async_copy(val_ref, val_hbm, sem.at[0]), pltpu.make_async_copy(den_ref, den_hbm, sem.at[1])]
    for copy in copies:
        copy.start()
    for copy in copies:
        copy.wait()


def solution(mesh):
    nrow, ncol = mesh.shape["row"], mesh.shape["col"]

    def body(running_cost, control_x, control_y, prior_density):
        rows, cols = running_cost.shape
        tiles = cols // LANE
        ext = tiles + 1
        pile = rows // 8
        big = pltpu.VMEM((ext, rows + 2 * TOP, LANE), jnp.float32)
        plain = pltpu.VMEM((tiles, rows, LANE), jnp.float32)
        value, density, ergodic = pl.pallas_call(
            functools.partial(kernel, nrow, ncol, 4 if ncol % 4 == 0 else 1, rows, tiles, min(rows, 128)),
            out_shape=(
                jax.ShapeDtypeStruct((rows, cols), jnp.float32),
                jax.ShapeDtypeStruct((rows, cols), jnp.float32),
                jax.ShapeDtypeStruct((1, LANE), jnp.float32),
            ),
            in_specs=[pl.BlockSpec(memory_space=pltpu.HBM)] * 4,
            out_specs=(pl.BlockSpec(memory_space=pltpu.VMEM),) * 3,
            scratch_shapes=[plain] * 3
            + [big] * 13
            + [pltpu.VMEM((pile, LANE), jnp.float32)] * 2
            + [pltpu.VMEM((pile + 16, LANE), jnp.float32)] * 2
            + [pltpu.VMEM((2, pile + 16, LANE), jnp.float32)] * 4
            + [pltpu.VMEM((2 * ncol, 1, LANE), jnp.float32), pltpu.VMEM((nrow // 2, 1, LANE), jnp.float32)]
            + [pltpu.VMEM((nrow * ncol, 1, LANE), jnp.float32), pltpu.VMEM((1, 1, LANE), jnp.float32)]
            + [
                pltpu.SemaphoreType.DMA((4, tiles)),
                pltpu.SemaphoreType.DMA((12,)),
                pltpu.SemaphoreType.DMA((12,)),
                pltpu.SemaphoreType.DMA((4,)),
                pltpu.SemaphoreType.DMA((4,)),
                pltpu.SemaphoreType.REGULAR((2,)),
            ],
            compiler_params=pltpu.CompilerParams(
                collective_id=0, has_side_effects=True, vmem_limit_bytes=55200000
            ),
        )(running_cost, control_x, control_y, prior_density)
        value, density = pl.pallas_call(
            store_kernel,
            out_shape=(jax.ShapeDtypeStruct((rows, cols), jnp.float32),) * 2,
            in_specs=[pl.BlockSpec(memory_space=pltpu.VMEM)] * 2,
            out_specs=(pl.BlockSpec(memory_space=pltpu.HBM),) * 2,
            scratch_shapes=[pltpu.SemaphoreType.DMA((2,))],
            compiler_params=pltpu.CompilerParams(vmem_limit_bytes=4 * 1024 * 1024),
        )(value, density)
        return value, density, ergodic[0, 0]

    spec = P("row", "col")
    return jax.shard_map(
        body,
        mesh=mesh,
        in_specs=(spec, spec, spec, spec),
        out_specs=(spec, spec, P()),
        check_vma=False,
    )
```

```python
import functools

import jax
import jax.numpy as jnp
from jax import lax
from jax.experimental import pallas as pl
from jax.experimental.pallas import tpu as pltpu
from jax.sharding import PartitionSpec as P

MESH = pl.DeviceIdType.MESH

SCALE = 1.0 / 64.0
FACE = 0.25 * 0.5 * SCALE
DISCOUNT = 0.05

LANE = 128
TOP = 16
HALO = 8


def solve(nu):
    shift = DISCOUNT * SCALE
    m = [nu[k + 1] + shift * nu[k] for k in range(5)]
    l1 = m[1] / m[0]
    l2 = m[2] / m[0]
    d1 = m[2] - l1 * m[1]
    e = m[3] - l2 * m[1]
    l3 = e / d1
    d2 = (m[4] - l2 * m[2]) - l3 * e
    y0 = nu[0]
    y1 = nu[1] - l1 * y0
    y2 = (nu[2] - l2 * y0) - l3 * y1
    c2 = y2 / d2
    c1 = y1 / d1 - l3 * c2
    c0 = y0 / m[0] - l1 * c1 - l2 * c2
    return c0 * SCALE, c1 * SCALE, c2 * SCALE


def kernel(
    nrow, ncol, nx, rows, tiles, step_rows,
    rc_hbm, cx_hbm, cy_hbm, pr_hbm,
    val_ref, den_ref, erg_ref,
    cx, cy, rc, C, B, Q, WE, WW, WS, CE, V1, V2, X, LP, U1, U2,
    pack_e, pack_w, from_w, from_e, SC, SB, S1, S2, ga, gb, gc,
    in_sem, hs_sem, hr_sem, as_sem, ar_sem, near_sem,
):
    me_r = lax.axis_index("row")
    me_c = lax.axis_index("col")
    up, down = lax.rem(me_r + nrow - 1, nrow), lax.rem(me_r + 1, nrow)
    west, east = lax.rem(me_c + ncol - 1, ncol), lax.rem(me_c + 1, ncol)
    ext = tiles + 1
    END = TOP + rows

    def tile_of(ref, j):
        return ref.at[:, pl.ds(j * LANE, LANE)]

    loads = {}
    outer_tiles = tuple(sorted({0, tiles - 1}))
    inner_tiles = tuple(range(1, tiles - 1))
    fields = ((cx_hbm, cx, 0), (cy_hbm, cy, 0), (rc_hbm, rc, 0), (pr_hbm, Q, TOP))
    for n, (src, dst, top), js in [(n, f, js) for js in (outer_tiles, inner_tiles) for n, f in enumerate(fields)]:
        for j in js:
            copy = pltpu.make_async_copy(tile_of(src, j), dst.at[j, pl.ds(top, rows), :], in_sem.at[n, j])
            copy.start()
            loads[n, j] = copy

    nz, ny = nrow // 2, ncol // nx
    core, z = lax.rem(me_r, 2), me_r // 2
    x, y = me_c // ny, lax.rem(me_c, ny)

    def at_offset(dz, dc, dx, dy):
        r = 2 * lax.rem(z + dz, nz) + lax.rem(core + dc, 2)
        return r, ny * lax.rem(x + dx, nx) + lax.rem(y + dy, ny)

    def offsets(zs, cs, xs, ys):
        every = {(a % nz, b, c % nx, d % ny) for a in zs for b in cs for c in xs for d in ys}
        return sorted(every - {(0, 0, 0, 0)})

    def tell(sem, to):
        pl.semaphore_signal(sem, inc=1, device_id=to, device_id_type=MESH)

    not_first, not_last = me_r > 0, me_r < nrow - 1
    not_west, not_east = me_c > 0, me_c < ncol - 1
    beyond = me_r + 2 * core - 1
    far_row = lax.rem(beyond + nrow, nrow)

    def when(*conditions):
        def run(fn):
            for c in conditions[::-1]:
                fn = functools.partial(lambda c, f: pl.when(c)(f) and None, c, fn)
            fn()
        return run

    far_there = (beyond >= 0, beyond < nrow)

    barrier = pltpu.get_barrier_semaphore()
    around = (-1, 0, 1)
    near = offsets((0,), (0, 1), around, around) + offsets(around, (0,), (0,), (0,))
    for o in near:
        tell(barrier, at_offset(*o))
    when(*far_there)(lambda: tell(barrier, (far_row, me_c)))
    when(*far_there, not_west)(lambda: tell(barrier, (far_row, west)))
    when(*far_there, not_east)(lambda: tell(barrier, (far_row, east)))

    zero = jnp.zeros((8, LANE), jnp.float32)
    for ref in (C, B, Q, WS, V1, V2, X, U1, U2):
        for j in range(ext):
            ref[j, pl.ds(0, 8), :] = zero
            ref[j, pl.ds(END + HALO, 8), :] = zero

    low, high = pl.ds(0, 8), pl.ds(rows // 8 - 8, 8)
    sw_at, nw_at = pl.ds(rows // 8, 8), pl.ds(rows // 8 + 8, 8)

    @pl.when(me_c == 0)
    def _():
        from_w[...] = jnp.zeros_like(from_w)

    @pl.when(me_c == ncol - 1)
    def _():
        from_e[...] = jnp.zeros_like(from_e)

    def no_row(top, corner):
        for f in (C, B, Q):
            for j in range(tiles):
                f[j, pl.ds(top, HALO), :] = zero
        from_w[corner, :] = zero
        from_e[corner, :] = zero

    @pl.when(me_r == 0)
    def _():
        no_row(TOP - HALO, nw_at)

    @pl.when(me_r == nrow - 1)
    def _():
        no_row(END, sw_at)

    def fold(acc, v):
        while v.shape[0] > 8:
            n = v.shape[0]
            if n % 16 == 0:
                v = v[: n // 2, :] + v[n // 2 :, :]
            else:
                acc, v = acc + v[n - 8 :, :], v[: n - 8, :]
        return acc + v

    def blank(k):
        return tuple(zero for _ in range(k))

    def prepare(js, accs):
        for n in range(len(fields)):
            for j in js:
                loads[n, j].wait()

        def first(i, accs):
            r = pl.multiple_of(i * step_rows, step_rows)
            at = pl.ds(TOP + r, step_rows)
            terms = [None] * 4
            for j in js:
                a, b = cx[j, pl.ds(r, step_rows), :], cy[j, pl.ds(r, step_rows), :]
                cost = 0.5 * (a * a + b * b)
                force = rc[j, pl.ds(r, step_rows), :] + cost
                C[j, at, :] = (1.0 + cost) * FACE
                B[j, at, :] = force
                q = Q[j, at, :]
                for k, t in enumerate((force * force, q, q * force, q * q)):
                    terms[k] = t if terms[k] is None else terms[k] + t
            return tuple(fold(acc, t) for acc, t in zip(accs, terms))

        return lax.fori_loop(0, rows // step_rows, first, accs)

    sums0 = prepare(outer_tiles, blank(4))

    parts = LANE // 16
    pile = rows // parts
    lane = lax.broadcasted_iota(jnp.int32, (pile, LANE), 1)
    slot = lane & 15
    is_c, is_b = slot < 6, slot < 11
    acc_e = jnp.zeros((pile, LANE), jnp.float32)
    acc_w = jnp.zeros((pile, LANE), jnp.float32)
    for k in range(parts):
        at = pl.ds(TOP + pile * k, pile)
        here = (lane >> 4) == k
        got = []
        for j, firsts in ((tiles - 1, (122, 123, 125)), (0, (0, 0, 0))):
            rolled = [
                pltpu.roll(f[j, at, :], (16 * k + o - s) % LANE, 1)
                for f, o, s in zip((C, B, Q), (0, 6, 11), firsts)
            ]
            got.append(jnp.where(is_c, rolled[0], jnp.where(is_b, rolled[1], rolled[2])))
        acc_e = jnp.where(here, got[0], acc_e)
        acc_w = jnp.where(here, got[1], acc_w)
    pack_e[...] = acc_e
    pack_w[...] = acc_w

    any_west, any_east = (me_c + ncol - 1) // ncol, (2 * ncol - 2 - me_c) // ncol
    any_far = core * ((2 * nrow - 2 - me_r) // nrow) + (1 - core) * ((me_r + nrow - 1) // nrow)
    pl.semaphore_wait(barrier, len(near) + any_far * (1 + any_west + any_east))

    sends = []

    def send(src, dst, to, there, here):
        n = len(sends)
        copy = pltpu.make_async_remote_copy(
            src_ref=src, dst_ref=dst, send_sem=hs_sem.at[n], recv_sem=hr_sem.at[n],
            device_id=to, device_id_type=MESH,
        )
        when(*there)(copy.start)
        sends.append((copy, there, here))

    send(pack_e.at[high, :], from_w.at[nw_at, :], (down, east), (not_last, not_east), (not_first, not_west))
    send(pack_e.at[low, :], from_w.at[sw_at, :], (up, east), (not_first, not_east), (not_last, not_west))
    send(pack_w.at[high, :], from_e.at[nw_at, :], (down, west), (not_last, not_west), (not_first, not_east))
    send(pack_w.at[low, :], from_e.at[sw_at, :], (up, west), (not_first, not_west), (not_last, not_east))
    send(pack_e, from_w.at[pl.ds(0, pile), :], (me_r, east), (not_east,), (not_west,))
    send(pack_w, from_e.at[pl.ds(0, pile), :], (me_r, west), (not_west,), (not_east,))
    if inner_tiles:
        sums0 = prepare(inner_tiles, sums0)
    nu0, s_q, s_qb, mu0 = sums0

    body = pl.ds(0, tiles)
    for f in (C, B, Q):
        send(f.at[body, pl.ds(TOP, HALO), :], f.at[body, pl.ds(END, HALO), :], (up, me_c), (not_first,), (not_last,))
        send(f.at[body, pl.ds(END - HALO, HALO), :], f.at[body, pl.ds(TOP - HALO, HALO), :], (down, me_c), (not_last,), (not_first,))

    first_ring = offsets((0,), (0,), around, around) + offsets(around, (0,), (0,), (0,))
    second_ring = offsets((-2, 2), (0,), (0,), (0,))
    for o in first_ring:
        tell(near_sem.at[0], at_offset(*o))

    fone, fnil = jnp.float32(1.0), jnp.float32(0.0)
    has_n, has_s = jnp.where(not_first, fone, fnil), jnp.where(not_last, fone, fnil)
    has_w, has_e = jnp.where(not_west, fone, fnil), jnp.where(not_east, fone, fnil)
    lane1 = lax.broadcasted_iota(jnp.int32, (1, LANE), 1)
    inside = jnp.where(lane1 < LANE // 2, has_e, has_w)

    def masks(n):
        l = lax.broadcasted_iota(jnp.int32, (n, LANE), 1)
        return l == LANE - 1, l == 0

    def to_east(vs, last):
        r = [pltpu.roll(v, LANE - 1, 1) for v in vs]
        return [jnp.where(last, r[(j + 1) % len(vs)], r[j]) for j in range(len(vs))]

    def to_west(vs, start):
        r = [pltpu.roll(v, 1, 1) for v in vs]
        return [jnp.where(start, r[(j - 1) % len(vs)], r[j]) for j in range(len(vs))]

    def rows_of(ref, r, n, count=ext):
        return [ref[j, pl.ds(r, n), :] for j in range(count)]

    def keep_in(vs, keep):
        if len(vs) == ext:
            vs = vs[:tiles] + [vs[tiles] * inside]
        return vs if keep is None else [v * keep for v in vs]

    def put(ref, r, n, vs):
        for j, v in enumerate(vs):
            ref[j, pl.ds(r, n), :] = v

    def add(accs, lists, weigh=None):
        out = []
        for acc, (p, q) in zip(accs, lists):
            total = None
            for j in range(tiles):
                t = p[j] * q[j]
                if weigh is not None and weigh[j] is not None:
                    t = t * weigh[j]
                total = t if total is None else total + t
            out.append(fold(acc, total))
        return tuple(out)

    def apply_from(vs, ref, r, n, center, we, ww, ws, wn, keep):
        count = len(vs)
        last, start = masks(n)
        ve, vw = to_east(vs, last), to_west(vs, start)
        vs_, vn = rows_of(ref, r + 1, n, count), rows_of(ref, r - 1, n, count)
        return keep_in(
            [
                center[j] * vs[j] - ((ws[j] * vs_[j] + wn[j] * vn[j]) + (we[j] * ve[j] + ww[j] * vw[j]))
                for j in range(count)
            ],
            keep,
        )

    def over_rows(step, accs, above=True, unrolled=False):
        if above:
            step(TOP - HALO, HALO, None, has_n)
        step(END, HALO, None, has_s)

        def loop(i, accs):
            return step(pl.multiple_of(TOP + i * step_rows, TOP), step_rows, accs, None)

        if unrolled:
            for i in range(rows // step_rows):
                accs = step(TOP + i * step_rows, step_rows, accs, None)
            return accs
        return lax.fori_loop(0, rows // step_rows, loop, accs)

    def weights_and_v1(r, n, count, keep):
        last, start = masks(n)
        c0 = rows_of(C, r, n, count)
        cs, cn = rows_of(C, r + 1, n, count), rows_of(C, r - 1, n, count)
        ce, cw = to_east(c0, last), to_west(c0, start)
        we = [c0[j] + ce[j] for j in range(count)]
        ww = [c0[j] + cw[j] for j in range(count)]
        ws = [c0[j] + cs[j] for j in range(count)]
        wn = [c0[j] + cn[j] for j in range(count)]
        center = [(ws[j] + wn[j]) + (we[j] + ww[j]) for j in range(count)]
        put(WE, r, n, we)
        put(WW, r, n, ww)
        put(WS, r, n, ws)
        put(CE, r, n, center)
        v1 = apply_from(rows_of(B, r, n, count), B, r, n, center, we, ww, ws, wn, keep)
        put(V1, r, n, v1)
        return v1

    def weights_of(r, n, count=ext):
        return rows_of(WE, r, n, count), rows_of(WW, r, n, count), rows_of(WS, r, n, count), rows_of(WS, r - 1, n, count)

    def second(r, n, count, keep):
        v1 = rows_of(V1, r, n, count)
        v2 = apply_from(v1, V1, r, n, rows_of(CE, r, n, count), *weights_of(r, n, count), keep)
        put(V2, r, n, v2)
        return v1, v2

    def face_terms(V, r, n, count, weigh=None):
        last, _ = masks(n)
        v = rows_of(V, r, n, count)
        ve = to_east(v, last)
        total = None
        for j in range(tiles):
            out = WE[j, pl.ds(r, n), :] * ve[j] + WS[j, pl.ds(r, n), :] * V[j, pl.ds(r + 1, n), :]
            t = v[j] * (CE[j, pl.ds(r, n), :] * v[j] - (out + out))
            if weigh is not None and weigh[j] is not None:
                t = t * weigh[j]
            total = t if total is None else total + t
        return total

    in_west = jnp.where(lane1 >= 6, jnp.ones((1, LANE), jnp.float32), jnp.zeros((1, LANE), jnp.float32))
    in_east = jnp.where(lane1 < LANE - 6, jnp.ones((1, LANE), jnp.float32), jnp.zeros((1, LANE), jnp.float32))
    weigh = [None] * tiles
    weigh[0] = in_west
    weigh[tiles - 1] = in_east if tiles > 1 else in_west * in_east
    INNER = 16
    pieces = 2
    part = (rows - 2 * INNER) // pieces

    def over_center(step, accs):
        step(TOP + 8, 8, None)
        step(END - 16, 8, None)

        for i in range(pieces):
            accs = step(TOP + INNER + i * part, part, accs)
        return accs

    def center1(r, n, accs):
        v1 = weights_and_v1(r, n, tiles, None)
        if accs is None:
            return None
        return add(accs, ((rows_of(B, r, n, tiles), v1), (v1, v1), (rows_of(Q, r, n, tiles), v1)), weigh)

    def center2(r, n, accs):
        v1, v2 = second(r, n, tiles, None)
        if accs is None:
            return None
        return add(accs, ((v1, v2), (v2, v2), (rows_of(Q, r, n, tiles), v2)), weigh)

    nu1, nu2, s_q1 = over_center(center1, blank(3))
    nu3, nu4, s_q2 = over_center(center2, blank(3))
    nu5 = zero
    for i in range(pieces):
        nu5 = fold(nu5, face_terms(V2, TOP + INNER + i * part, part, tiles, weigh))

    def own_columns(f, j, shift):
        acc = jnp.zeros((pile, LANE), jnp.float32)
        for k in range(parts):
            acc = jnp.where((lane >> 4) == k, pltpu.roll(f[j, pl.ds(TOP + pile * k, pile), :], (16 * k + shift) % LANE, 1), acc)
        return acc

    own_w = [own_columns(f, 0, 6) for f in (C, B, Q)]
    own_e = [own_columns(f, tiles - 1, 10 - LANE) for f in (C, B, Q)]

    for copy, _, here in sends[:10]:
        when(*here)(copy.wait_recv)

    pl.semaphore_wait(near_sem.at[0], len(first_ring))
    for o in second_ring:
        tell(near_sem.at[1], at_offset(*o))

    def unpack(at, src, k, n, fields):
        w, e = from_w[src, :], from_e[src, :]
        l = lax.broadcasted_iota(jnp.int32, (n, LANE), 1)
        none = jnp.zeros((n, LANE), jnp.float32)
        for f, o, s, wide in zip((C, B, Q)[:fields], (0, 6, 11), (122, 123, 125), (6, 5, 3)):
            rw = pltpu.roll(w, (s - 16 * k - o) % LANE, 1)
            re = pltpu.roll(e, (-16 * k - o) % LANE, 1)
            f[tiles, at, :] = jnp.where(l >= s, rw, jnp.where(l < wide, re, none))

    top_at, end_at = pl.ds(TOP - HALO, HALO), pl.ds(END, HALO)
    for k in range(parts):
        if pile * k < 32 or pile * (k + 1) > rows - 32:
            unpack(pl.ds(TOP + pile * k, pile), pl.ds(0, pile), k, pile, 2)
    unpack(top_at, nw_at, parts - 1, HALO, 2)
    unpack(end_at, sw_at, 0, HALO, 2)

    rows32 = lax.broadcasted_iota(jnp.int32, (32, LANE), 0)
    ones32 = jnp.ones((32, LANE), jnp.float32)
    tops = ((TOP - HALO, jnp.where(rows32 < HALO, has_n * ones32, ones32), HALO), (END - 24, jnp.where(rows32 >= 24, has_s * ones32, ones32), HALO))
    def own_16(vs, skip):
        return [v[skip : skip + 16, :] for v in vs]

    for r, keep, skip in tops:
        v1 = own_16(weights_and_v1(r, 32, ext, keep), skip)
        b, q = rows_of(B, r + skip, 16, tiles), rows_of(Q, r + skip, 16, tiles)
        nu1, nu2, s_q1 = add((nu1, nu2, s_q1), ((b, v1), (v1, v1), (q, v1)))
    for r, keep, skip in tops:
        v1, v2 = [own_16(v, skip) for v in second(r, 32, ext, keep)]
        q = rows_of(Q, r + skip, 16, tiles)
        nu3, nu4, s_q2 = add((nu3, nu4, s_q2), ((v1, v2), (v2, v2), (q, v2)))
    for r, keep, skip in tops:
        nu5 = fold(nu5, face_terms(V2, r + skip, 16, ext))

    def put_strip(ref, n, v):
        ref[n, pl.ds(8, pile), :] = v
        ref[n, pl.ds(7, 1), :] = pltpu.roll(v[pile - 1 :, :], 16, 1)
        ref[n, pl.ds(8 + pile, 1), :] = pltpu.roll(v[:1, :], LANE - 16, 1)

    def below_above(ref, n):
        return ref[n, pl.ds(9, pile), :], ref[n, pl.ds(7, pile), :]

    sides = ((own_w, from_w, (0, -5), slot < 6, has_w, 6), (own_e, from_e, (10, 4), slot >= 10, has_e, 4))
    row_at = lax.broadcasted_iota(jnp.int32, (pile, LANE), 0) + pile * (lane >> 4)
    for n, (own, come, shifts, outer, there, begin) in enumerate(sides):
        got = come[pl.ds(0, pile), :]
        keep = jnp.where(outer, there * jnp.ones((pile, LANE), jnp.float32), jnp.ones((pile, LANE), jnp.float32))
        middle = (row_at >= INNER) & (row_at < rows - INNER) & (slot >= begin) & (slot < begin + 6)
        mine = jnp.where(middle, jnp.ones((pile, LANE), jnp.float32), jnp.zeros((pile, LANE), jnp.float32))
        c, b = [jnp.where(outer, pltpu.roll(got, h % LANE, 1), o) for h, o in zip(shifts, own)]
        q = own[2] * mine
        put_strip(SC, n, c)
        put_strip(SB, n, b)
        c_s, c_n = below_above(SC, n)
        we, ww, ws, wn = c + pltpu.roll(c, LANE - 1, 1), c + pltpu.roll(c, 1, 1), c + c_s, c + c_n
        mid = (ws + wn) + (we + ww)

        def strip_apply(ref, v):
            put_strip(ref, n, v)
            v_s, v_n = below_above(ref, n)
            beside = we * pltpu.roll(v, LANE - 1, 1) + ww * pltpu.roll(v, 1, 1)
            return (mid * v - ((ws * v_s + wn * v_n) + beside)) * keep

        v1 = strip_apply(SB, b)
        v2 = strip_apply(S1, v1)
        put_strip(S2, n, v2)
        out = we * pltpu.roll(v2, LANE - 1, 1) + ws * S2[n, pl.ds(9, pile), :]
        m1, m2 = v1 * mine, v2 * mine
        nu1, nu2, nu3 = fold(nu1, b * m1), fold(nu2, v1 * m1), fold(nu3, v1 * m2)
        nu4, nu5 = fold(nu4, v2 * m2), fold(nu5, m2 * (mid * v2 - (out + out)))
        s_q1, s_q2 = fold(s_q1, q * v1), fold(s_q2, q * v2)

    lane8 = lax.broadcasted_iota(jnp.int32, (8, LANE), 1)

    def add_up(buf, count):
        terms = [buf[k] for k in range(count)]
        while len(terms) > 1:
            terms = [terms[k] + terms[k + 1] if k + 1 < len(terms) else terms[k] for k in range(0, len(terms), 2)]
        return terms[0]

    def start_sum(part, ga, gb, stage):
        slot = core * ncol + me_c
        ga[slot] = part
        for d in sorted(range(ncol), key=lambda d: -min(d, ncol - d)):
            copy = pltpu.make_async_remote_copy(
                src_ref=ga.at[slot], dst_ref=ga.at[slot], send_sem=as_sem.at[stage], recv_sem=ar_sem.at[stage],
                device_id=(2 * z + 1, lax.rem(me_c + d, ncol)), device_id_type=MESH,
            )
            if d == 0:
                pl.when(core == 0)(copy.start)
            else:
                copy.start()

    def wait_bytes(buf, count, sem):
        some = buf.at[pl.ds(0, count)]
        pltpu.make_async_copy(some, some, sem).wait()

    def finish_sum(ga, gb, stage):
        @pl.when(core == 1)
        def _():
            wait_bytes(ga, 2 * ncol - 1, ar_sem.at[stage])
            if stage == 0:
                pl.semaphore_wait(near_sem.at[1], len(second_ring))
            gb[z] = add_up(ga, 2 * ncol)
            for dz in sorted(range(nz), key=lambda d: -min(d, nz - d)):
                for to_core in (0, 1):
                    if dz or to_core == 0:
                        pltpu.make_async_remote_copy(
                            src_ref=gb.at[z], dst_ref=gb.at[z],
                            send_sem=as_sem.at[stage + 1], recv_sem=ar_sem.at[stage + 1],
                            device_id=(2 * lax.rem(z + dz, nz) + to_core, me_c), device_id_type=MESH,
                        ).start()
            wait_bytes(ga, ncol - 1, as_sem.at[stage])
            wait_bytes(gb, nz - 1, ar_sem.at[stage + 1])

        @pl.when(core == 0)
        def _():
            if stage == 0:
                pl.semaphore_wait(near_sem.at[1], len(second_ring))
            wait_bytes(ga, ncol, as_sem.at[stage])
            wait_bytes(gb, nz, ar_sem.at[stage + 1])

        return add_up(gb, nz)

    def settle(stage):
        @pl.when(core == 1)
        def _():
            wait_bytes(ga, 2 * nz - 1, as_sem.at[stage])

    others = nrow * ncol - 1

    def start_direct(part):
        slot = me_r * ncol + me_c
        gc[slot] = part
        zs = [2 * lax.rem(z + d, nz) for d in range(nz)]
        cs = [[ny * lax.rem(x + a, nx) + lax.rem(y + b, ny) for b in range(ny)] for a in range(nx)]

        def hops(o):
            return min(o[0], nz - o[0]) + min(o[1], nx - o[1]) + min(o[2], ny - o[2])

        every = [(d, a, b) for d in range(nz) for a in range(nx) for b in range(ny)]
        for to_core in (1, 0):
            for o in sorted(every, key=lambda o: -hops(o)):
                copy = pltpu.make_async_remote_copy(
                    src_ref=gc.at[slot], dst_ref=gc.at[slot], send_sem=as_sem.at[2], recv_sem=ar_sem.at[2],
                    device_id=(zs[o[0]] + to_core, cs[o[1]][o[2]]), device_id_type=MESH,
                )
                if hops(o) == 0:
                    pl.when(core == 1 - to_core)(copy.start)
                else:
                    copy.start()

    def finish_direct():
        wait_bytes(gc, others, ar_sem.at[2])
        return jnp.sum(gc[...], axis=0)

    def gather(accs):
        packed = jnp.zeros((8, LANE), jnp.float32)
        for k, acc in enumerate(accs):
            packed = jnp.where(lane8 == k, jnp.sum(acc, axis=1, keepdims=True), packed)
        return jnp.sum(packed, axis=0, keepdims=True)

    def spread(row, k):
        return jnp.broadcast_to(row[:, k : k + 1], (1, LANE))

    start_sum(gather((nu0, nu1, nu2, nu3, nu4, nu5, s_q, s_qb, s_q1, s_q2)), ga, gb, 0)

    for copy, _, here in sends[10:]:
        when(*here)(copy.wait_recv)
    for k in range(parts):
        unpack(pl.ds(TOP + pile * k, pile), pl.ds(0, pile), k, pile, 3)
    unpack(top_at, nw_at, parts - 1, HALO, 3)
    unpack(end_at, sw_at, 0, HALO, 3)

    def all1(r, n, accs, keep):
        weights_and_v1(r, n, ext, keep)
        return accs

    def all2(r, n, accs, keep):
        second(r, n, ext, keep)
        return accs

    def pass_q(r, n, accs, keep):
        put(LP, r, n, apply_from(rows_of(Q, r, n), Q, r, n, rows_of(CE, r, n), *weights_of(r, n), keep))
        return accs

    over_rows(all1, 0)
    over_rows(all2, 0)
    over_rows(pass_q, 0)

    for copy, there, _ in sends:
        when(*there)(copy.wait_send)
    sums = finish_sum(ga, gb, 0)

    c0, c1, c2 = solve([spread(sums, k) for k in range(6)])
    t_q, t_qb, t_q1, t_q2 = [spread(sums, k) for k in range(6, 10)]

    def pass_x(r, n, accs, keep):
        b, v1, v2 = rows_of(B, r, n), rows_of(V1, r, n), rows_of(V2, r, n)
        value = [c0 * b[j] + (c1 * v1[j] + c2 * v2[j]) for j in range(ext)]
        put(X, r, n, value)
        if keep is None:
            for j in range(tiles):
                val_ref[pl.ds(r - TOP, n), pl.ds(j * LANE, LANE)] = value[j]
        return accs

    over_rows(pass_x, 0, unrolled=True)

    def pass3(r, n, accs, keep):
        last, start = masks(n)
        x = rows_of(X, r, n)
        xe, xw = to_east(x, last), to_west(x, start)
        xs, xn = rows_of(X, r + 1, n), rows_of(X, r - 1, n)
        q, lp, center = rows_of(Q, r, n), rows_of(LP, r, n), rows_of(CE, r, n)
        u1, full = [], []
        for j in range(ext):
            dr, dc = xs[j] - xn[j], xe[j] - xw[j]
            g = (0.25 / (2.0 * 0.25) * SCALE) * (dr * dr + dc * dc)
            full.append(center[j] + g)
            u1.append(lp[j] + g * q[j])
        u1 = keep_in(u1, keep)
        put(CE, r, n, full)
        put(U1, r, n, u1)
        if accs is None:
            return None
        return add(accs, ((q, u1), (u1, u1)))

    mu1, mu2 = over_rows(pass3, blank(2), unrolled=True)

    def pass4(r, n, accs, keep):
        u1 = rows_of(U1, r, n)
        u2 = apply_from(u1, U1, r, n, rows_of(CE, r, n), *weights_of(r, n), keep)
        put(U2, r, n, u2)
        return None if accs is None else add(accs, ((u1, u2), (u2, u2)))

    mu3, mu4 = over_rows(pass4, blank(2), False, True)

    mu5 = zero
    for i in range(rows // step_rows):
        mu5 = fold(mu5, face_terms(U2, TOP + i * step_rows, step_rows, ext))


    start_direct(gather((mu0, mu1, mu2, mu3, mu4, mu5)))
    erg_ref[...] = (t_qb - DISCOUNT * (c0 * t_qb + (c1 * t_q1 + c2 * t_q2))) / t_q
    settle(1)
    sums = finish_direct()
    d0, d1, d2 = solve([spread(sums, k) for k in range(6)])

    def last_pass(i, carry):
        r = pl.multiple_of(i * step_rows, step_rows)
        at = pl.ds(TOP + r, step_rows)
        for j in range(tiles):
            den_ref[pl.ds(r, step_rows), pl.ds(j * LANE, LANE)] = d0 * Q[j, at, :] + (d1 * U1[j, at, :] + d2 * U2[j, at, :])
        return carry

    lax.fori_loop(0, rows // step_rows, last_pass, 0)
    wait_bytes(gc, others, as_sem.at[2])


def store_kernel(val_ref, den_ref, val_hbm, den_hbm, sem):
    copies = [pltpu.make_async_copy(val_ref, val_hbm, sem.at[0]), pltpu.make_async_copy(den_ref, den_hbm, sem.at[1])]
    for copy in copies:
        copy.start()
    for copy in copies:
        copy.wait()


def solution(mesh):
    nrow, ncol = mesh.shape["row"], mesh.shape["col"]

    def body(running_cost, control_x, control_y, prior_density):
        rows, cols = running_cost.shape
        tiles = cols // LANE
        ext = tiles + 1
        pile = rows // 8
        big = pltpu.VMEM((ext, rows + 2 * TOP, LANE), jnp.float32)
        plain = pltpu.VMEM((tiles, rows, LANE), jnp.float32)
        value, density, ergodic = pl.pallas_call(
            functools.partial(kernel, nrow, ncol, 4 if ncol % 4 == 0 else 1, rows, tiles, min(rows, 128)),
            out_shape=(
                jax.ShapeDtypeStruct((rows, cols), jnp.float32),
                jax.ShapeDtypeStruct((rows, cols), jnp.float32),
                jax.ShapeDtypeStruct((1, LANE), jnp.float32),
            ),
            in_specs=[pl.BlockSpec(memory_space=pltpu.HBM)] * 4,
            out_specs=(pl.BlockSpec(memory_space=pltpu.VMEM),) * 3,
            scratch_shapes=[plain] * 3
            + [big] * 13
            + [pltpu.VMEM((pile, LANE), jnp.float32)] * 2
            + [pltpu.VMEM((pile + 16, LANE), jnp.float32)] * 2
            + [pltpu.VMEM((2, pile + 16, LANE), jnp.float32)] * 4
            + [pltpu.VMEM((2 * ncol, 1, LANE), jnp.float32), pltpu.VMEM((nrow // 2, 1, LANE), jnp.float32)]
            + [pltpu.VMEM((nrow * ncol, 1, LANE), jnp.float32)]
            + [
                pltpu.SemaphoreType.DMA((4, tiles)),
                pltpu.SemaphoreType.DMA((12,)),
                pltpu.SemaphoreType.DMA((12,)),
                pltpu.SemaphoreType.DMA((4,)),
                pltpu.SemaphoreType.DMA((4,)),
                pltpu.SemaphoreType.REGULAR((2,)),
            ],
            compiler_params=pltpu.CompilerParams(
                collective_id=0, has_side_effects=True, vmem_limit_bytes=55200000
            ),
        )(running_cost, control_x, control_y, prior_density)
        value, density = pl.pallas_call(
            store_kernel,
            out_shape=(jax.ShapeDtypeStruct((rows, cols), jnp.float32),) * 2,
            in_specs=[pl.BlockSpec(memory_space=pltpu.VMEM)] * 2,
            out_specs=(pl.BlockSpec(memory_space=pltpu.HBM),) * 2,
            scratch_shapes=[pltpu.SemaphoreType.DMA((2,))],
            compiler_params=pltpu.CompilerParams(vmem_limit_bytes=4 * 1024 * 1024),
        )(value, density)
        return value, density, ergodic[0, 0]

    spec = P("row", "col")
    return jax.shard_map(
        body,
        mesh=mesh,
        in_specs=(spec, spec, spec, spec),
        out_specs=(spec, spec, P()),
        check_vma=False,
    )
```

```python
import functools

import jax
import jax.numpy as jnp
from jax import lax
from jax.experimental import pallas as pl
from jax.experimental.pallas import tpu as pltpu
from jax.sharding import PartitionSpec as P

MESH = pl.DeviceIdType.MESH

SCALE = 1.0 / 64.0
FACE = 0.25 * 0.5 * SCALE
DISCOUNT = 0.05

LANE = 128
TOP = 16
HALO = 8


def solve(nu):
    shift = DISCOUNT * SCALE
    m = [nu[k + 1] + shift * nu[k] for k in range(5)]
    l1 = m[1] / m[0]
    l2 = m[2] / m[0]
    d1 = m[2] - l1 * m[1]
    e = m[3] - l2 * m[1]
    l3 = e / d1
    d2 = (m[4] - l2 * m[2]) - l3 * e
    y0 = nu[0]
    y1 = nu[1] - l1 * y0
    y2 = (nu[2] - l2 * y0) - l3 * y1
    c2 = y2 / d2
    c1 = y1 / d1 - l3 * c2
    c0 = y0 / m[0] - l1 * c1 - l2 * c2
    return c0 * SCALE, c1 * SCALE, c2 * SCALE


def kernel(
    nrow, ncol, nx, rows, tiles, step_rows,
    rc_hbm, cx_hbm, cy_hbm, pr_hbm,
    val_ref, den_ref, erg_ref,
    cx, cy, rc, C, B, Q, WE, WW, WS, CE, V1, V2, X, LP, U1, U2,
    pack_e, pack_w, from_w, from_e, SC, SB, S1, S2, ga, gb, gc,
    in_sem, hs_sem, hr_sem, as_sem, ar_sem, near_sem,
):
    me_r = lax.axis_index("row")
    me_c = lax.axis_index("col")
    up, down = lax.rem(me_r + nrow - 1, nrow), lax.rem(me_r + 1, nrow)
    west, east = lax.rem(me_c + ncol - 1, ncol), lax.rem(me_c + 1, ncol)
    ext = tiles + 1
    END = TOP + rows

    def tile_of(ref, j):
        return ref.at[:, pl.ds(j * LANE, LANE)]

    loads = {}
    outer_tiles = tuple(sorted({0, tiles - 1}))
    inner_tiles = tuple(range(1, tiles - 1))
    fields = ((cx_hbm, cx, 0), (cy_hbm, cy, 0), (rc_hbm, rc, 0), (pr_hbm, Q, TOP))
    for n, (src, dst, top), js in [(n, f, js) for js in (outer_tiles, inner_tiles) for n, f in enumerate(fields)]:
        for j in js:
            copy = pltpu.make_async_copy(tile_of(src, j), dst.at[j, pl.ds(top, rows), :], in_sem.at[n, j])
            copy.start()
            loads[n, j] = copy

    nz, ny = nrow // 2, ncol // nx
    core, z = lax.rem(me_r, 2), me_r // 2
    x, y = me_c // ny, lax.rem(me_c, ny)

    def at_offset(dz, dc, dx, dy):
        r = 2 * lax.rem(z + dz, nz) + lax.rem(core + dc, 2)
        return r, ny * lax.rem(x + dx, nx) + lax.rem(y + dy, ny)

    def offsets(zs, cs, xs, ys):
        every = {(a % nz, b, c % nx, d % ny) for a in zs for b in cs for c in xs for d in ys}
        return sorted(every - {(0, 0, 0, 0)})

    def tell(sem, to):
        pl.semaphore_signal(sem, inc=1, device_id=to, device_id_type=MESH)

    not_first, not_last = me_r > 0, me_r < nrow - 1
    not_west, not_east = me_c > 0, me_c < ncol - 1
    beyond = me_r + 2 * core - 1
    far_row = lax.rem(beyond + nrow, nrow)

    def when(*conditions):
        def run(fn):
            for c in conditions[::-1]:
                fn = functools.partial(lambda c, f: pl.when(c)(f) and None, c, fn)
            fn()
        return run

    far_there = (beyond >= 0, beyond < nrow)

    barrier = pltpu.get_barrier_semaphore()
    around = (-1, 0, 1)
    near = offsets((0,), (0, 1), around, around) + offsets(around, (0,), (0,), (0,))
    for o in near:
        tell(barrier, at_offset(*o))
    when(*far_there)(lambda: tell(barrier, (far_row, me_c)))
    when(*far_there, not_west)(lambda: tell(barrier, (far_row, west)))
    when(*far_there, not_east)(lambda: tell(barrier, (far_row, east)))

    zero = jnp.zeros((8, LANE), jnp.float32)
    for ref in (C, B, Q, WS, V1, V2, X, U1, U2):
        for j in range(ext):
            ref[j, pl.ds(0, 8), :] = zero
            ref[j, pl.ds(END + HALO, 8), :] = zero

    low, high = pl.ds(0, 8), pl.ds(rows // 8 - 8, 8)
    sw_at, nw_at = pl.ds(rows // 8, 8), pl.ds(rows // 8 + 8, 8)

    @pl.when(me_c == 0)
    def _():
        from_w[...] = jnp.zeros_like(from_w)

    @pl.when(me_c == ncol - 1)
    def _():
        from_e[...] = jnp.zeros_like(from_e)

    def no_row(top, corner):
        for f in (C, B, Q):
            for j in range(tiles):
                f[j, pl.ds(top, HALO), :] = zero
        from_w[corner, :] = zero
        from_e[corner, :] = zero

    @pl.when(me_r == 0)
    def _():
        no_row(TOP - HALO, nw_at)

    @pl.when(me_r == nrow - 1)
    def _():
        no_row(END, sw_at)

    def fold(acc, v):
        while v.shape[0] > 8:
            n = v.shape[0]
            if n % 16 == 0:
                v = v[: n // 2, :] + v[n // 2 :, :]
            else:
                acc, v = acc + v[n - 8 :, :], v[: n - 8, :]
        return acc + v

    def blank(k):
        return tuple(zero for _ in range(k))

    def prepare(js, accs):
        for n in range(len(fields)):
            for j in js:
                loads[n, j].wait()

        def first(i, accs):
            r = i * step_rows
            at = pl.ds(TOP + r, step_rows)
            terms = [None] * 4
            for j in js:
                a, b = cx[j, pl.ds(r, step_rows), :], cy[j, pl.ds(r, step_rows), :]
                cost = 0.5 * (a * a + b * b)
                force = rc[j, pl.ds(r, step_rows), :] + cost
                C[j, at, :] = (1.0 + cost) * FACE
                B[j, at, :] = force
                q = Q[j, at, :]
                for k, t in enumerate((force * force, q, q * force, q * q)):
                    terms[k] = t if terms[k] is None else terms[k] + t
            return tuple(fold(acc, t) for acc, t in zip(accs, terms))

        for i in range(rows // step_rows):
            accs = first(i, accs)
        return accs

    sums0 = prepare(outer_tiles, blank(4))

    parts = LANE // 16
    pile = rows // parts
    lane = lax.broadcasted_iota(jnp.int32, (pile, LANE), 1)
    slot = lane & 15
    is_c, is_b = slot < 6, slot < 11
    acc_e = jnp.zeros((pile, LANE), jnp.float32)
    acc_w = jnp.zeros((pile, LANE), jnp.float32)
    for k in range(parts):
        at = pl.ds(TOP + pile * k, pile)
        here = (lane >> 4) == k
        got = []
        for j, firsts in ((tiles - 1, (122, 123, 125)), (0, (0, 0, 0))):
            rolled = [
                pltpu.roll(f[j, at, :], (16 * k + o - s) % LANE, 1)
                for f, o, s in zip((C, B, Q), (0, 6, 11), firsts)
            ]
            got.append(jnp.where(is_c, rolled[0], jnp.where(is_b, rolled[1], rolled[2])))
        acc_e = jnp.where(here, got[0], acc_e)
        acc_w = jnp.where(here, got[1], acc_w)
    pack_e[...] = acc_e
    pack_w[...] = acc_w

    any_west, any_east = (me_c + ncol - 1) // ncol, (2 * ncol - 2 - me_c) // ncol
    any_far = core * ((2 * nrow - 2 - me_r) // nrow) + (1 - core) * ((me_r + nrow - 1) // nrow)
    pl.semaphore_wait(barrier, len(near) + any_far * (1 + any_west + any_east))

    sends = []

    def send(src, dst, to, there, here):
        n = len(sends)
        copy = pltpu.make_async_remote_copy(
            src_ref=src, dst_ref=dst, send_sem=hs_sem.at[n], recv_sem=hr_sem.at[n],
            device_id=to, device_id_type=MESH,
        )
        when(*there)(copy.start)
        sends.append((copy, there, here))

    send(pack_e.at[high, :], from_w.at[nw_at, :], (down, east), (not_last, not_east), (not_first, not_west))
    send(pack_e.at[low, :], from_w.at[sw_at, :], (up, east), (not_first, not_east), (not_last, not_west))
    send(pack_w.at[high, :], from_e.at[nw_at, :], (down, west), (not_last, not_west), (not_first, not_east))
    send(pack_w.at[low, :], from_e.at[sw_at, :], (up, west), (not_first, not_west), (not_last, not_east))
    send(pack_e, from_w.at[pl.ds(0, pile), :], (me_r, east), (not_east,), (not_west,))
    send(pack_w, from_e.at[pl.ds(0, pile), :], (me_r, west), (not_west,), (not_east,))
    if inner_tiles:
        sums0 = prepare(inner_tiles, sums0)
    nu0, s_q, s_qb, mu0 = sums0

    body = pl.ds(0, tiles)
    for f in (C, B, Q):
        send(f.at[body, pl.ds(TOP, HALO), :], f.at[body, pl.ds(END, HALO), :], (up, me_c), (not_first,), (not_last,))
        send(f.at[body, pl.ds(END - HALO, HALO), :], f.at[body, pl.ds(TOP - HALO, HALO), :], (down, me_c), (not_last,), (not_first,))

    first_ring = offsets((0,), (0,), around, around) + offsets(around, (0,), (0,), (0,))
    second_ring = offsets((-2, 2), (0,), (0,), (0,))
    for o in first_ring:
        tell(near_sem.at[0], at_offset(*o))

    fone, fnil = jnp.float32(1.0), jnp.float32(0.0)
    has_n, has_s = jnp.where(not_first, fone, fnil), jnp.where(not_last, fone, fnil)
    has_w, has_e = jnp.where(not_west, fone, fnil), jnp.where(not_east, fone, fnil)
    lane1 = lax.broadcasted_iota(jnp.int32, (1, LANE), 1)
    inside = jnp.where(lane1 < LANE // 2, has_e, has_w)

    def masks(n):
        l = lax.broadcasted_iota(jnp.int32, (n, LANE), 1)
        return l == LANE - 1, l == 0

    def to_east(vs, last):
        r = [pltpu.roll(v, LANE - 1, 1) for v in vs]
        return [jnp.where(last, r[(j + 1) % len(vs)], r[j]) for j in range(len(vs))]

    def to_west(vs, start):
        r = [pltpu.roll(v, 1, 1) for v in vs]
        return [jnp.where(start, r[(j - 1) % len(vs)], r[j]) for j in range(len(vs))]

    def rows_of(ref, r, n, count=ext):
        return [ref[j, pl.ds(r, n), :] for j in range(count)]

    def keep_in(vs, keep):
        if len(vs) == ext:
            vs = vs[:tiles] + [vs[tiles] * inside]
        return vs if keep is None else [v * keep for v in vs]

    def put(ref, r, n, vs):
        for j, v in enumerate(vs):
            ref[j, pl.ds(r, n), :] = v

    def add(accs, lists, weigh=None):
        out = []
        for acc, (p, q) in zip(accs, lists):
            total = None
            for j in range(tiles):
                t = p[j] * q[j]
                if weigh is not None and weigh[j] is not None:
                    t = t * weigh[j]
                total = t if total is None else total + t
            out.append(fold(acc, total))
        return tuple(out)

    def apply_from(vs, ref, r, n, center, we, ww, ws, wn, keep):
        count = len(vs)
        last, start = masks(n)
        ve, vw = to_east(vs, last), to_west(vs, start)
        vs_, vn = rows_of(ref, r + 1, n, count), rows_of(ref, r - 1, n, count)
        return keep_in(
            [
                center[j] * vs[j] - ((ws[j] * vs_[j] + wn[j] * vn[j]) + (we[j] * ve[j] + ww[j] * vw[j]))
                for j in range(count)
            ],
            keep,
        )

    def over_rows(step, accs, above=True, unrolled=False):
        if above:
            step(TOP - HALO, HALO, None, has_n)
        step(END, HALO, None, has_s)

        def loop(i, accs):
            return step(pl.multiple_of(TOP + i * step_rows, TOP), step_rows, accs, None)

        if unrolled:
            for i in range(rows // step_rows):
                accs = step(TOP + i * step_rows, step_rows, accs, None)
            return accs
        return lax.fori_loop(0, rows // step_rows, loop, accs)

    def weights_and_v1(r, n, count, keep):
        last, start = masks(n)
        c0 = rows_of(C, r, n, count)
        cs, cn = rows_of(C, r + 1, n, count), rows_of(C, r - 1, n, count)
        ce, cw = to_east(c0, last), to_west(c0, start)
        we = [c0[j] + ce[j] for j in range(count)]
        ww = [c0[j] + cw[j] for j in range(count)]
        ws = [c0[j] + cs[j] for j in range(count)]
        wn = [c0[j] + cn[j] for j in range(count)]
        center = [(ws[j] + wn[j]) + (we[j] + ww[j]) for j in range(count)]
        put(WE, r, n, we)
        put(WW, r, n, ww)
        put(WS, r, n, ws)
        put(CE, r, n, center)
        v1 = apply_from(rows_of(B, r, n, count), B, r, n, center, we, ww, ws, wn, keep)
        put(V1, r, n, v1)
        return v1

    def weights_of(r, n, count=ext):
        return rows_of(WE, r, n, count), rows_of(WW, r, n, count), rows_of(WS, r, n, count), rows_of(WS, r - 1, n, count)

    def second(r, n, count, keep):
        v1 = rows_of(V1, r, n, count)
        v2 = apply_from(v1, V1, r, n, rows_of(CE, r, n, count), *weights_of(r, n, count), keep)
        put(V2, r, n, v2)
        return v1, v2

    def face_terms(V, r, n, count, weigh=None):
        last, _ = masks(n)
        v = rows_of(V, r, n, count)
        ve = to_east(v, last)
        total = None
        for j in range(tiles):
            out = WE[j, pl.ds(r, n), :] * ve[j] + WS[j, pl.ds(r, n), :] * V[j, pl.ds(r + 1, n), :]
            t = v[j] * (CE[j, pl.ds(r, n), :] * v[j] - (out + out))
            if weigh is not None and weigh[j] is not None:
                t = t * weigh[j]
            total = t if total is None else total + t
        return total

    in_west = jnp.where(lane1 >= 6, jnp.ones((1, LANE), jnp.float32), jnp.zeros((1, LANE), jnp.float32))
    in_east = jnp.where(lane1 < LANE - 6, jnp.ones((1, LANE), jnp.float32), jnp.zeros((1, LANE), jnp.float32))
    weigh = [None] * tiles
    weigh[0] = in_west
    weigh[tiles - 1] = in_east if tiles > 1 else in_west * in_east
    INNER = 16
    pieces = 2
    part = (rows - 2 * INNER) // pieces

    def over_center(step, accs):
        step(TOP + 8, 8, None)
        step(END - 16, 8, None)

        for i in range(pieces):
            accs = step(TOP + INNER + i * part, part, accs)
        return accs

    def center1(r, n, accs):
        v1 = weights_and_v1(r, n, tiles, None)
        if accs is None:
            return None
        return add(accs, ((rows_of(B, r, n, tiles), v1), (v1, v1), (rows_of(Q, r, n, tiles), v1)), weigh)

    def center2(r, n, accs):
        v1, v2 = second(r, n, tiles, None)
        if accs is None:
            return None
        return add(accs, ((v1, v2), (v2, v2), (rows_of(Q, r, n, tiles), v2)), weigh)

    nu1, nu2, s_q1 = over_center(center1, blank(3))
    nu3, nu4, s_q2 = over_center(center2, blank(3))
    nu5 = zero
    for i in range(pieces):
        nu5 = fold(nu5, face_terms(V2, TOP + INNER + i * part, part, tiles, weigh))

    def own_columns(f, j, shift):
        acc = jnp.zeros((pile, LANE), jnp.float32)
        for k in range(parts):
            acc = jnp.where((lane >> 4) == k, pltpu.roll(f[j, pl.ds(TOP + pile * k, pile), :], (16 * k + shift) % LANE, 1), acc)
        return acc

    own_w = [own_columns(f, 0, 6) for f in (C, B, Q)]
    own_e = [own_columns(f, tiles - 1, 10 - LANE) for f in (C, B, Q)]

    for copy, _, here in sends[:10]:
        when(*here)(copy.wait_recv)

    pl.semaphore_wait(near_sem.at[0], len(first_ring))
    for o in second_ring:
        tell(near_sem.at[1], at_offset(*o))

    def unpack(at, src, k, n, fields):
        w, e = from_w[src, :], from_e[src, :]
        l = lax.broadcasted_iota(jnp.int32, (n, LANE), 1)
        none = jnp.zeros((n, LANE), jnp.float32)
        for f, o, s, wide in zip((C, B, Q)[:fields], (0, 6, 11), (122, 123, 125), (6, 5, 3)):
            rw = pltpu.roll(w, (s - 16 * k - o) % LANE, 1)
            re = pltpu.roll(e, (-16 * k - o) % LANE, 1)
            f[tiles, at, :] = jnp.where(l >= s, rw, jnp.where(l < wide, re, none))

    top_at, end_at = pl.ds(TOP - HALO, HALO), pl.ds(END, HALO)
    for k in range(parts):
        if pile * k < 32 or pile * (k + 1) > rows - 32:
            unpack(pl.ds(TOP + pile * k, pile), pl.ds(0, pile), k, pile, 2)
    unpack(top_at, nw_at, parts - 1, HALO, 2)
    unpack(end_at, sw_at, 0, HALO, 2)

    rows32 = lax.broadcasted_iota(jnp.int32, (32, LANE), 0)
    ones32 = jnp.ones((32, LANE), jnp.float32)
    tops = ((TOP - HALO, jnp.where(rows32 < HALO, has_n * ones32, ones32), HALO), (END - 24, jnp.where(rows32 >= 24, has_s * ones32, ones32), HALO))
    def own_16(vs, skip):
        return [v[skip : skip + 16, :] for v in vs]

    for r, keep, skip in tops:
        v1 = own_16(weights_and_v1(r, 32, ext, keep), skip)
        b, q = rows_of(B, r + skip, 16, tiles), rows_of(Q, r + skip, 16, tiles)
        nu1, nu2, s_q1 = add((nu1, nu2, s_q1), ((b, v1), (v1, v1), (q, v1)))
    for r, keep, skip in tops:
        v1, v2 = [own_16(v, skip) for v in second(r, 32, ext, keep)]
        q = rows_of(Q, r + skip, 16, tiles)
        nu3, nu4, s_q2 = add((nu3, nu4, s_q2), ((v1, v2), (v2, v2), (q, v2)))
    for r, keep, skip in tops:
        nu5 = fold(nu5, face_terms(V2, r + skip, 16, ext))

    def put_strip(ref, n, v):
        ref[n, pl.ds(8, pile), :] = v
        ref[n, pl.ds(7, 1), :] = pltpu.roll(v[pile - 1 :, :], 16, 1)
        ref[n, pl.ds(8 + pile, 1), :] = pltpu.roll(v[:1, :], LANE - 16, 1)

    def below_above(ref, n):
        return ref[n, pl.ds(9, pile), :], ref[n, pl.ds(7, pile), :]

    sides = ((own_w, from_w, (0, -5), slot < 6, has_w, 6), (own_e, from_e, (10, 4), slot >= 10, has_e, 4))
    row_at = lax.broadcasted_iota(jnp.int32, (pile, LANE), 0) + pile * (lane >> 4)
    for n, (own, come, shifts, outer, there, begin) in enumerate(sides):
        got = come[pl.ds(0, pile), :]
        keep = jnp.where(outer, there * jnp.ones((pile, LANE), jnp.float32), jnp.ones((pile, LANE), jnp.float32))
        middle = (row_at >= INNER) & (row_at < rows - INNER) & (slot >= begin) & (slot < begin + 6)
        mine = jnp.where(middle, jnp.ones((pile, LANE), jnp.float32), jnp.zeros((pile, LANE), jnp.float32))
        c, b = [jnp.where(outer, pltpu.roll(got, h % LANE, 1), o) for h, o in zip(shifts, own)]
        q = own[2] * mine
        put_strip(SC, n, c)
        put_strip(SB, n, b)
        c_s, c_n = below_above(SC, n)
        we, ww, ws, wn = c + pltpu.roll(c, LANE - 1, 1), c + pltpu.roll(c, 1, 1), c + c_s, c + c_n
        mid = (ws + wn) + (we + ww)

        def strip_apply(ref, v):
            put_strip(ref, n, v)
            v_s, v_n = below_above(ref, n)
            beside = we * pltpu.roll(v, LANE - 1, 1) + ww * pltpu.roll(v, 1, 1)
            return (mid * v - ((ws * v_s + wn * v_n) + beside)) * keep

        v1 = strip_apply(SB, b)
        v2 = strip_apply(S1, v1)
        put_strip(S2, n, v2)
        out = we * pltpu.roll(v2, LANE - 1, 1) + ws * S2[n, pl.ds(9, pile), :]
        m1, m2 = v1 * mine, v2 * mine
        nu1, nu2, nu3 = fold(nu1, b * m1), fold(nu2, v1 * m1), fold(nu3, v1 * m2)
        nu4, nu5 = fold(nu4, v2 * m2), fold(nu5, m2 * (mid * v2 - (out + out)))
        s_q1, s_q2 = fold(s_q1, q * v1), fold(s_q2, q * v2)

    lane8 = lax.broadcasted_iota(jnp.int32, (8, LANE), 1)

    def add_up(buf, count):
        terms = [buf[k] for k in range(count)]
        while len(terms) > 1:
            terms = [terms[k] + terms[k + 1] if k + 1 < len(terms) else terms[k] for k in range(0, len(terms), 2)]
        return terms[0]

    def start_sum(part, ga, gb, stage):
        slot = core * ncol + me_c
        ga[slot] = part
        for d in sorted(range(ncol), key=lambda d: -min(d, ncol - d)):
            copy = pltpu.make_async_remote_copy(
                src_ref=ga.at[slot], dst_ref=ga.at[slot], send_sem=as_sem.at[stage], recv_sem=ar_sem.at[stage],
                device_id=(2 * z + 1, lax.rem(me_c + d, ncol)), device_id_type=MESH,
            )
            if d == 0:
                pl.when(core == 0)(copy.start)
            else:
                copy.start()

    def wait_bytes(buf, count, sem):
        some = buf.at[pl.ds(0, count)]
        pltpu.make_async_copy(some, some, sem).wait()

    def finish_sum(ga, gb, stage):
        @pl.when(core == 1)
        def _():
            wait_bytes(ga, 2 * ncol - 1, ar_sem.at[stage])
            if stage == 0:
                pl.semaphore_wait(near_sem.at[1], len(second_ring))
            gb[z] = add_up(ga, 2 * ncol)
            for dz in sorted(range(nz), key=lambda d: -min(d, nz - d)):
                for to_core in (0, 1):
                    if dz or to_core == 0:
                        pltpu.make_async_remote_copy(
                            src_ref=gb.at[z], dst_ref=gb.at[z],
                            send_sem=as_sem.at[stage + 1], recv_sem=ar_sem.at[stage + 1],
                            device_id=(2 * lax.rem(z + dz, nz) + to_core, me_c), device_id_type=MESH,
                        ).start()
            wait_bytes(ga, ncol - 1, as_sem.at[stage])
            wait_bytes(gb, nz - 1, ar_sem.at[stage + 1])

        @pl.when(core == 0)
        def _():
            if stage == 0:
                pl.semaphore_wait(near_sem.at[1], len(second_ring))
            wait_bytes(ga, ncol, as_sem.at[stage])
            wait_bytes(gb, nz, ar_sem.at[stage + 1])

        return add_up(gb, nz)

    def settle(stage):
        @pl.when(core == 1)
        def _():
            wait_bytes(ga, 2 * nz - 1, as_sem.at[stage])

    others = nrow * ncol - 1

    def start_direct(part):
        slot = me_r * ncol + me_c
        gc[slot] = part
        zs = [2 * lax.rem(z + d, nz) for d in range(nz)]
        cs = [[ny * lax.rem(x + a, nx) + lax.rem(y + b, ny) for b in range(ny)] for a in range(nx)]

        def hops(o):
            return min(o[0], nz - o[0]) + min(o[1], nx - o[1]) + min(o[2], ny - o[2])

        every = [(d, a, b) for d in range(nz) for a in range(nx) for b in range(ny)]
        for to_core in (1, 0):
            for o in sorted(every, key=lambda o: -hops(o)):
                copy = pltpu.make_async_remote_copy(
                    src_ref=gc.at[slot], dst_ref=gc.at[slot], send_sem=as_sem.at[2], recv_sem=ar_sem.at[2],
                    device_id=(zs[o[0]] + to_core, cs[o[1]][o[2]]), device_id_type=MESH,
                )
                if hops(o) == 0:
                    pl.when(core == 1 - to_core)(copy.start)
                else:
                    copy.start()

    def finish_direct():
        wait_bytes(gc, others, ar_sem.at[2])
        return jnp.sum(gc[...], axis=0)

    def gather(accs):
        packed = jnp.zeros((8, LANE), jnp.float32)
        for k, acc in enumerate(accs):
            packed = jnp.where(lane8 == k, jnp.sum(acc, axis=1, keepdims=True), packed)
        return jnp.sum(packed, axis=0, keepdims=True)

    def spread(row, k):
        return jnp.broadcast_to(row[:, k : k + 1], (1, LANE))

    start_sum(gather((nu0, nu1, nu2, nu3, nu4, nu5, s_q, s_qb, s_q1, s_q2)), ga, gb, 0)

    for copy, _, here in sends[10:]:
        when(*here)(copy.wait_recv)
    for k in range(parts):
        unpack(pl.ds(TOP + pile * k, pile), pl.ds(0, pile), k, pile, 3)
    unpack(top_at, nw_at, parts - 1, HALO, 3)
    unpack(end_at, sw_at, 0, HALO, 3)

    def all1(r, n, accs, keep):
        weights_and_v1(r, n, ext, keep)
        return accs

    def all2(r, n, accs, keep):
        second(r, n, ext, keep)
        return accs

    def pass_q(r, n, accs, keep):
        put(LP, r, n, apply_from(rows_of(Q, r, n), Q, r, n, rows_of(CE, r, n), *weights_of(r, n), keep))
        return accs

    over_rows(all1, 0)
    over_rows(all2, 0)
    over_rows(pass_q, 0)

    for copy, there, _ in sends:
        when(*there)(copy.wait_send)
    sums = finish_sum(ga, gb, 0)

    c0, c1, c2 = solve([spread(sums, k) for k in range(6)])
    t_q, t_qb, t_q1, t_q2 = [spread(sums, k) for k in range(6, 10)]

    def pass_x(r, n, accs, keep):
        b, v1, v2 = rows_of(B, r, n), rows_of(V1, r, n), rows_of(V2, r, n)
        value = [c0 * b[j] + (c1 * v1[j] + c2 * v2[j]) for j in range(ext)]
        put(X, r, n, value)
        if keep is None:
            for j in range(tiles):
                val_ref[pl.ds(r - TOP, n), pl.ds(j * LANE, LANE)] = value[j]
        return accs

    over_rows(pass_x, 0, unrolled=True)

    def pass3(r, n, accs, keep):
        last, start = masks(n)
        x = rows_of(X, r, n)
        xe, xw = to_east(x, last), to_west(x, start)
        xs, xn = rows_of(X, r + 1, n), rows_of(X, r - 1, n)
        q, lp, center = rows_of(Q, r, n), rows_of(LP, r, n), rows_of(CE, r, n)
        u1, full = [], []
        for j in range(ext):
            dr, dc = xs[j] - xn[j], xe[j] - xw[j]
            g = (0.25 / (2.0 * 0.25) * SCALE) * (dr * dr + dc * dc)
            full.append(center[j] + g)
            u1.append(lp[j] + g * q[j])
        u1 = keep_in(u1, keep)
        put(CE, r, n, full)
        put(U1, r, n, u1)
        if accs is None:
            return None
        return add(accs, ((q, u1), (u1, u1)))

    mu1, mu2 = over_rows(pass3, blank(2), unrolled=True)

    def pass4(r, n, accs, keep):
        u1 = rows_of(U1, r, n)
        u2 = apply_from(u1, U1, r, n, rows_of(CE, r, n), *weights_of(r, n), keep)
        put(U2, r, n, u2)
        return None if accs is None else add(accs, ((u1, u2), (u2, u2)))

    mu3, mu4 = over_rows(pass4, blank(2), False, True)

    mu5 = zero
    for i in range(rows // step_rows):
        mu5 = fold(mu5, face_terms(U2, TOP + i * step_rows, step_rows, ext))


    start_direct(gather((mu0, mu1, mu2, mu3, mu4, mu5)))
    erg_ref[...] = (t_qb - DISCOUNT * (c0 * t_qb + (c1 * t_q1 + c2 * t_q2))) / t_q
    settle(1)
    sums = finish_direct()
    d0, d1, d2 = solve([spread(sums, k) for k in range(6)])

    def last_pass(i, carry):
        r = i * step_rows
        at = pl.ds(TOP + r, step_rows)
        for j in range(tiles):
            den_ref[pl.ds(r, step_rows), pl.ds(j * LANE, LANE)] = d0 * Q[j, at, :] + (d1 * U1[j, at, :] + d2 * U2[j, at, :])
        return carry

    for i in range(rows // step_rows):
        last_pass(i, 0)
    wait_bytes(gc, others, as_sem.at[2])


def store_kernel(val_ref, den_ref, val_hbm, den_hbm, sem):
    copies = [pltpu.make_async_copy(val_ref, val_hbm, sem.at[0]), pltpu.make_async_copy(den_ref, den_hbm, sem.at[1])]
    for copy in copies:
        copy.start()
    for copy in copies:
        copy.wait()


def solution(mesh):
    nrow, ncol = mesh.shape["row"], mesh.shape["col"]

    def body(running_cost, control_x, control_y, prior_density):
        rows, cols = running_cost.shape
        tiles = cols // LANE
        ext = tiles + 1
        pile = rows // 8
        big = pltpu.VMEM((ext, rows + 2 * TOP, LANE), jnp.float32)
        plain = pltpu.VMEM((tiles, rows, LANE), jnp.float32)
        value, density, ergodic = pl.pallas_call(
            functools.partial(kernel, nrow, ncol, 4 if ncol % 4 == 0 else 1, rows, tiles, min(rows, 128)),
            out_shape=(
                jax.ShapeDtypeStruct((rows, cols), jnp.float32),
                jax.ShapeDtypeStruct((rows, cols), jnp.float32),
                jax.ShapeDtypeStruct((1, LANE), jnp.float32),
            ),
            in_specs=[pl.BlockSpec(memory_space=pltpu.HBM)] * 4,
            out_specs=(pl.BlockSpec(memory_space=pltpu.VMEM),) * 3,
            scratch_shapes=[plain] * 3
            + [big] * 13
            + [pltpu.VMEM((pile, LANE), jnp.float32)] * 2
            + [pltpu.VMEM((pile + 16, LANE), jnp.float32)] * 2
            + [pltpu.VMEM((2, pile + 16, LANE), jnp.float32)] * 4
            + [pltpu.VMEM((2 * ncol, 1, LANE), jnp.float32), pltpu.VMEM((nrow // 2, 1, LANE), jnp.float32)]
            + [pltpu.VMEM((nrow * ncol, 1, LANE), jnp.float32)]
            + [
                pltpu.SemaphoreType.DMA((4, tiles)),
                pltpu.SemaphoreType.DMA((12,)),
                pltpu.SemaphoreType.DMA((12,)),
                pltpu.SemaphoreType.DMA((4,)),
                pltpu.SemaphoreType.DMA((4,)),
                pltpu.SemaphoreType.REGULAR((2,)),
            ],
            compiler_params=pltpu.CompilerParams(
                collective_id=0, has_side_effects=True, vmem_limit_bytes=55200000
            ),
        )(running_cost, control_x, control_y, prior_density)
        value, density = pl.pallas_call(
            store_kernel,
            out_shape=(jax.ShapeDtypeStruct((rows, cols), jnp.float32),) * 2,
            in_specs=[pl.BlockSpec(memory_space=pltpu.VMEM)] * 2,
            out_specs=(pl.BlockSpec(memory_space=pltpu.HBM),) * 2,
            scratch_shapes=[pltpu.SemaphoreType.DMA((2,))],
            compiler_params=pltpu.CompilerParams(vmem_limit_bytes=4 * 1024 * 1024),
        )(value, density)
        return value, density, ergodic[0, 0]

    spec = P("row", "col")
    return jax.shard_map(
        body,
        mesh=mesh,
        in_specs=(spec, spec, spec, spec),
        out_specs=(spec, spec, P()),
        check_vma=False,
    )
```
